32 devices in a mesh: rep: 1 (over z), data: 4 (over y), model: 8 (over x, core).
Axes of the slice: x: 4, y: 4, z: 1, core: 2. Of those that a mesh axis runs over, the one named last changes fastest.
The devices are a block of a 4x4x8 slice.
Arguments:
- x: bfloat16 [32, 1024, 2048], P(('rep', 'data'), 'model')
- lengths: int32 [32], P(('rep', 'data'))
- gamma: bfloat16 [2, 2048], P(None, 'data')
- w_in: bfloat16 [2, 2048, 18432], P(None, 'data', 'model')
- w_kv: bfloat16 [2, 2048, 256], P(None, 'data')
- w_out: bfloat16 [2, 10240, 2048], P(None, 'model', 'data')
Outputs:
- output: bfloat16 [32, 1024, 2048], P(('rep', 'data'), 'model')
All inputs are finite; a program needn't handle non-finite values.
Results may differ from the reference program's by a relative error of at most 0.0158209.
Values are sent between devices in bfloat16 or wider.
A program may use at most 768 MiB of HBM per device.

```python
import jax
import jax.numpy as jnp
from jax import lax

BATCH_SIZE = 32
SEQ_LEN = 1024
D_MODEL = 2048
N_HEADS = 16
HEAD_DIM = 128
D_FF = 8192
N_SHARDS = 8

EPSILON = 1e-6
LOCAL_HEADS = N_HEADS // N_SHARDS
FF_LOCAL = D_FF // N_SHARDS
ATTN_COLS = LOCAL_HEADS * HEAD_DIM
IN_LOCAL = ATTN_COLS + 2 * FF_LOCAL
OUT_LOCAL = ATTN_COLS + FF_LOCAL
QUERY_BLOCK = SEQ_LEN // N_SHARDS


def setup_inputs(seed: int = 0, part: int = 0) -> dict:
    part_key = jax.random.fold_in(jax.random.key(seed), part)
    key_x, key_len_a, key_len_b = jax.random.split(part_key, 3)
    key_gain, key_in, key_kv, key_out = jax.random.split(jax.random.key(seed + 1), 4)
    x = jax.random.normal(key_x, (BATCH_SIZE, SEQ_LEN, D_MODEL), jnp.float32).astype(jnp.bfloat16)
    len_min = SEQ_LEN // 8
    len_a = jax.random.randint(key_len_a, (BATCH_SIZE,), len_min, SEQ_LEN + 1, jnp.int32)
    len_b = jax.random.randint(key_len_b, (BATCH_SIZE,), len_min, SEQ_LEN + 1, jnp.int32)
    lengths = jnp.maximum(len_a, len_b).at[0].set(SEQ_LEN).at[BATCH_SIZE - 1].set(len_min)
    gamma = (1.0 + 0.3 * jax.random.normal(key_gain, (2, D_MODEL), jnp.float32)).astype(jnp.bfloat16)
    w_in = (jax.random.normal(key_in, (2, D_MODEL, N_SHARDS * IN_LOCAL), jnp.float32) * D_MODEL ** -0.5).astype(jnp.bfloat16)
    w_kv = (jax.random.normal(key_kv, (2, D_MODEL, 2 * HEAD_DIM), jnp.float32) * (2.0 * D_MODEL ** -0.5)).astype(jnp.bfloat16)
    w_out = (jax.random.normal(key_out, (2, N_SHARDS * OUT_LOCAL, D_MODEL), jnp.float32) * (N_SHARDS * OUT_LOCAL) ** -0.5).astype(jnp.bfloat16)
    return {"x": x, "lengths": lengths, "gamma": gamma, "w_in": w_in, "w_kv": w_kv, "w_out": w_out}


def rms_norm(x_in, gain):
    x_f32 = x_in.astype(jnp.float32)
    inv_rms = lax.rsqrt(jnp.mean(x_f32 * x_f32, axis=-1, keepdims=True) + EPSILON)
    return (x_f32 * inv_rms * gain.astype(jnp.float32)).astype(jnp.bfloat16)


def attend_one(q_seq, k_seq, v_seq, seq_len):
    key_pos = jnp.arange(SEQ_LEN)
    q_blocks = q_seq.reshape(N_SHARDS, QUERY_BLOCK, N_HEADS, HEAD_DIM)
    k_f32 = k_seq.astype(jnp.float32)
    v_f32 = v_seq.astype(jnp.float32)

    def one_block(block_in):
        q_blk, blk_idx = block_in
        scores = jnp.einsum("qhd,kd->hqk", q_blk.astype(jnp.float32), k_f32) * (HEAD_DIM ** -0.5)
        q_pos = blk_idx * QUERY_BLOCK + jnp.arange(QUERY_BLOCK)
        visible = (key_pos[None, :] <= q_pos[:, None]) & (key_pos[None, :] < seq_len)
        scores = jnp.where(visible[None], scores, -1e30)
        attn_probs = jax.nn.softmax(scores, axis=-1).astype(jnp.bfloat16)
        blk_out = jnp.einsum("hqk,kd->qhd", attn_probs.astype(jnp.float32), v_f32)
        return blk_out.astype(jnp.bfloat16)

    blocks_out = lax.map(one_block, (q_blocks, jnp.arange(N_SHARDS)))
    return blocks_out.reshape(SEQ_LEN, N_SHARDS, ATTN_COLS)


def layer_one(x_seq, seq_len, gain, w_in_l, w_kv_l, w_out_l):
    normed = rms_norm(x_seq, gain)
    projected = jnp.dot(normed, w_in_l, preferred_element_type=jnp.float32).astype(jnp.bfloat16)
    projected = projected.reshape(SEQ_LEN, N_SHARDS, IN_LOCAL)
    queries = projected[:, :, :ATTN_COLS].reshape(SEQ_LEN, N_HEADS, HEAD_DIM)
    gate = projected[:, :, ATTN_COLS:ATTN_COLS + FF_LOCAL].astype(jnp.float32)
    up_proj = projected[:, :, ATTN_COLS + FF_LOCAL:].astype(jnp.float32)
    key_value = jnp.dot(normed, w_kv_l, preferred_element_type=jnp.float32).astype(jnp.bfloat16)
    attn_out = attend_one(queries, key_value[:, :HEAD_DIM], key_value[:, HEAD_DIM:], seq_len)
    mlp_out = (jax.nn.silu(gate) * up_proj).astype(jnp.bfloat16)
    mixed = jnp.moveaxis(jnp.concatenate([attn_out, mlp_out], axis=-1), 1, 0)
    w_out_groups = w_out_l.reshape(N_SHARDS, OUT_LOCAL, D_MODEL)

    def add_group(z_acc, group_in):
        rows, weights = group_in
        part_z = jnp.dot(rows, weights, preferred_element_type=jnp.float32).astype(jnp.bfloat16)
        return z_acc + part_z.astype(jnp.float32), None

    z_sum, _ = lax.scan(add_group, jnp.zeros((SEQ_LEN, D_MODEL), jnp.float32), (mixed, w_out_groups))
    return (x_seq.astype(jnp.float32) + z_sum).astype(jnp.bfloat16)


def reference(x, lengths, gamma, w_in, w_kv, w_out):
    def one_layer(hidden, params):
        gain, w_in_l, w_kv_l, w_out_l = params
        new_hidden = lax.map(lambda seq_in: layer_one(seq_in[0], seq_in[1], gain, w_in_l, w_kv_l, w_out_l), (hidden, lengths))
        return new_hidden, None

    result, _ = lax.scan(one_layer, x, (gamma, w_in, w_kv, w_out))
    return result
```

```python
import functools

import jax
import jax.numpy as jnp
from jax import lax
from jax.experimental import pallas as pl
from jax.experimental.pallas import tpu as pltpu
from jax.sharding import PartitionSpec as P

EPSILON = 1e-6
MIB = 1 << 20


def rms_norm(x_in, gain):
    x_f32 = x_in.astype(jnp.float32)
    inv_rms = lax.rsqrt(jnp.mean(x_f32 * x_f32, axis=-1, keepdims=True) + EPSILON)
    return (x_f32 * inv_rms * gain.astype(jnp.float32)).astype(jnp.bfloat16)


def assemble(slots, pieces, n_slots, axis):
    own, below, above, far_a, far_b = pieces
    rows, cols = own.shape
    tile = rows // 2
    far = n_slots // 2
    order = [(0, 0, 0), (0, 1, 0), (1, 0, n_slots - 1), (1, 1, n_slots - 1), (2, 0, 1), (2, 1, 1), (3, 0, far), (4, 1, far)]
    starts = {0: 0, 1: 2, 2: 4, 3: 6, 4: 7}
    lasts = {0: 1, 1: 1, 2: 1, 3: 0, 4: 0}

    def out_map(step, table):
        half = step % 2
        slot = table[n_slots + step]
        if axis == 0:
            return (2 * slot + half, 0)
        return (half, slot)

    def body(table, *refs):
        out = refs[-1]
        step = pl.program_id(0)
        for piece in range(5):
            first = starts[piece]

            @pl.when((step >= first) & (step <= first + lasts[piece]))
            def _(piece=piece):
                out[...] = refs[piece][...]

    table = jnp.concatenate([slots, jnp.stack([slots[entry] for _, _, entry in order])])
    in_specs = [
        pl.BlockSpec((tile, cols), functools.partial(lambda step, table, first, last: (jnp.clip(step - first, 0, last), 0), first=starts[k], last=lasts[k]))
        for k in range(5)
    ]
    out_shape = (rows * n_slots, cols) if axis == 0 else (rows, cols * n_slots)
    return pl.pallas_call(
        body,
        out_shape=jax.ShapeDtypeStruct(out_shape, own.dtype),
        grid_spec=pltpu.PrefetchScalarGridSpec(
            num_scalar_prefetch=1, grid=(len(order),), in_specs=in_specs, out_specs=pl.BlockSpec((tile, cols), out_map)
        ),
        compiler_params=pltpu.CompilerParams(dimension_semantics=("arbitrary",), vmem_limit_bytes=24 * MIB),
        cost_estimate=pl.CostEstimate(flops=rows * cols * 400, bytes_accessed=rows * cols * n_slots * 4, transcendentals=0),
        name="assemble",
    )(table, *pieces)


def norm_pair(own, par, gain, tile):
    rows, d_model = own.shape

    def body(own_ref, par_ref, gain_ref, h_ref):
        h_ref[0] = rms_norm(own_ref[...], gain_ref[...])
        h_ref[1] = rms_norm(par_ref[...], gain_ref[...])

    row_spec = pl.BlockSpec((tile, d_model), lambda i: (i, 0))
    return pl.pallas_call(
        body,
        out_shape=jax.ShapeDtypeStruct((2, rows, d_model), jnp.bfloat16),
        grid=(rows // tile,),
        in_specs=[row_spec, row_spec, pl.BlockSpec((1, d_model), lambda i: (0, 0))],
        out_specs=pl.BlockSpec((2, tile, d_model), lambda i: (0, i, 0)),
        compiler_params=pltpu.CompilerParams(dimension_semantics=("arbitrary",), vmem_limit_bytes=24 * MIB),
        cost_estimate=pl.CostEstimate(flops=rows * d_model * 800, bytes_accessed=rows * d_model * 8, transcendentals=0),
        name="norm_pair",
    )(own, par, gain)


def keys_values_of(x_in, gain, w_kv, tile):
    rows, d_model = x_in.shape

    def body(x_ref, gain_ref, w_ref, kv_ref):
        h = rms_norm(x_ref[...], gain_ref[...])
        kv_ref[...] = jnp.dot(h, w_ref[...], preferred_element_type=jnp.float32).astype(jnp.bfloat16)

    return pl.pallas_call(
        body,
        out_shape=jax.ShapeDtypeStruct((rows, w_kv.shape[1]), jnp.bfloat16),
        grid=(rows // tile,),
        in_specs=[
            pl.BlockSpec((tile, d_model), lambda i: (i, 0)),
            pl.BlockSpec((1, d_model), lambda i: (0, 0)),
            pl.BlockSpec(w_kv.shape, lambda i: (0, 0)),
        ],
        out_specs=pl.BlockSpec((tile, w_kv.shape[1]), lambda i: (i, 0)),
        compiler_params=pltpu.CompilerParams(dimension_semantics=("arbitrary",), vmem_limit_bytes=24 * MIB),
        cost_estimate=pl.CostEstimate(flops=rows * d_model * 1200, bytes_accessed=rows * d_model * 2, transcendentals=0),
        name="keys_values",
    )(x_in, gain, w_kv)


def finish_layer(x_in, z_own, z_got, gain, w_kv, tile):
    rows, d_model = x_in.shape

    def body(x_ref, own_ref, got_ref, gain_ref, w_ref, y_ref, kv_ref):
        z = own_ref[...].astype(jnp.float32) + got_ref[...].astype(jnp.float32)
        y = (x_ref[...].astype(jnp.float32) + z).astype(jnp.bfloat16)
        y_ref[...] = y
        h = rms_norm(y, gain_ref[...])
        kv_ref[...] = jnp.dot(h, w_ref[...], preferred_element_type=jnp.float32).astype(jnp.bfloat16)

    row_spec = pl.BlockSpec((tile, d_model), lambda i: (i, 0))
    return pl.pallas_call(
        body,
        out_shape=(jax.ShapeDtypeStruct((rows, d_model), jnp.bfloat16), jax.ShapeDtypeStruct((rows, w_kv.shape[1]), jnp.bfloat16)),
        grid=(rows // tile,),
        in_specs=[row_spec, row_spec, row_spec, pl.BlockSpec((1, d_model), lambda i: (0, 0)), pl.BlockSpec(w_kv.shape, lambda i: (0, 0))],
        out_specs=(row_spec, pl.BlockSpec((tile, w_kv.shape[1]), lambda i: (i, 0))),
        compiler_params=pltpu.CompilerParams(dimension_semantics=("arbitrary",), vmem_limit_bytes=24 * MIB),
        cost_estimate=pl.CostEstimate(flops=rows * d_model * 1200, bytes_accessed=rows * d_model * 8, transcendentals=0),
        name="finish_layer",
    )(x_in, z_own, z_got, gain, w_kv)


def finish_last(x_in, z_own, z_got, so_far, chunk, total_rows, tile):
    rows, d_model = x_in.shape
    steps = rows // tile

    def body(x_ref, own_ref, got_ref, *refs):
        y_ref = refs[-1]
        z = own_ref[...].astype(jnp.float32) + got_ref[...].astype(jnp.float32)
        y_ref[...] = (x_ref[...].astype(jnp.float32) + z).astype(jnp.bfloat16)

    row_spec = pl.BlockSpec((tile, d_model), lambda i: (i, 0))
    args, in_specs, aliases = [x_in, z_own, z_got], [row_spec] * 3, {}
    if so_far is not None:
        args.append(so_far)
        in_specs.append(pl.BlockSpec(memory_space=pl.ANY))
        aliases = {3: 0}
    return pl.pallas_call(
        body,
        out_shape=jax.ShapeDtypeStruct((total_rows, d_model), jnp.bfloat16),
        grid=(steps,),
        in_specs=in_specs,
        out_specs=pl.BlockSpec((tile, d_model), lambda i: (chunk * steps + i, 0)),
        input_output_aliases=aliases,
        compiler_params=pltpu.CompilerParams(dimension_semantics=("arbitrary",), vmem_limit_bytes=24 * MIB),
        cost_estimate=pl.CostEstimate(flops=rows * d_model * 400, bytes_accessed=rows * d_model * 8, transcendentals=0),
        name="finish_last",
    )(*args)


def in_proj(h, weights, attn_cols, ff, tile_rows):
    sides, rows, d_model = h.shape
    n_blocks = len(weights)
    cols = attn_cols
    per_block = 1 + ff // cols

    def body(*refs):
        h_ref = refs[0]
        q_ref, m_ref = refs[-2:]
        step = pl.program_id(1)
        h_val = h_ref[...].reshape(sides * tile_rows, d_model)
        for blk in range(n_blocks):
            g_ref, u_ref = refs[1 + 2 * blk], refs[2 + 2 * blk]
            base = blk * per_block

            @pl.when(step == base)
            def _(g_ref=g_ref):
                q = jnp.dot(h_val, g_ref[...], preferred_element_type=jnp.float32)
                q_ref[...] = q.astype(q_ref.dtype).reshape(q_ref.shape)

            @pl.when((step > base) & (step < base + per_block))
            def _(g_ref=g_ref, u_ref=u_ref):
                gate = jnp.dot(h_val, g_ref[...], preferred_element_type=jnp.float32).astype(jnp.bfloat16).astype(jnp.float32)
                up = jnp.dot(h_val, u_ref[...], preferred_element_type=jnp.float32).astype(jnp.bfloat16).astype(jnp.float32)
                mid = gate * jax.nn.sigmoid(gate) * up
                m_ref[...] = mid.astype(m_ref.dtype).reshape(m_ref.shape)

    in_specs = [pl.BlockSpec((sides, tile_rows, d_model), lambda i, s: (0, i, 0))]
    args = [h]
    for blk, weight in enumerate(weights):
        base = blk * per_block

        def g_map(i, s, base=base):
            return (0, jnp.clip(s - base, 0, per_block - 1))

        def u_map(i, s, base=base):
            return (0, per_block + jnp.clip(s - base - 1, 0, per_block - 2))

        in_specs += [pl.BlockSpec((d_model, cols), g_map), pl.BlockSpec((d_model, cols), u_map)]
        args += [weight, weight]
    q_spec = pl.BlockSpec((1, sides, tile_rows, attn_cols), lambda i, s: (s // per_block, 0, i, 0))
    m_spec = pl.BlockSpec(
        (1, sides, tile_rows, cols), lambda i, s: (s // per_block, 0, i, jnp.maximum(s % per_block - 1, 0))
    )
    total = sides * rows
    flops = 2 * total * d_model * (attn_cols + 2 * ff) * n_blocks
    return pl.pallas_call(
        body,
        out_shape=(
            jax.ShapeDtypeStruct((n_blocks, sides, rows, attn_cols), jnp.bfloat16),
            jax.ShapeDtypeStruct((n_blocks, sides, rows, ff), jnp.bfloat16),
        ),
        grid=(rows // tile_rows, n_blocks * per_block),
        in_specs=in_specs,
        out_specs=(q_spec, m_spec),
        compiler_params=pltpu.CompilerParams(dimension_semantics=("arbitrary", "arbitrary"), vmem_limit_bytes=60 * MIB),
        cost_estimate=pl.CostEstimate(flops=flops, bytes_accessed=2 * total * d_model + 2 * d_model * (attn_cols + 2 * ff) * n_blocks, transcendentals=0),
        name="in_proj",
    )(*args)


def attend(lens, slabs, queries, keys_values, chunk, n_chunk):
    n_slab, _, slab_len, two_hd = keys_values.shape
    head_dim = two_hd // 2
    cols = queries[0].shape[3]
    per_block = cols // head_dim
    n_blocks = sum(q.shape[0] for q in queries)
    heads = n_blocks * per_block
    rows = heads * slab_len
    key_rows = 2 * slab_len
    log2e = 1.4426950408889634
    scale = head_dim ** -0.5 * log2e
    q_chunks = [q.shape[2] // (n_chunk * slab_len) for q in queries]
    offset = [chunk * n_chunk if n > 1 else 0 for n in q_chunks]
    kv_offset = chunk * n_chunk if keys_values.shape[1] > n_chunk else 0

    def body(lens_ref, slab_ref, *refs):
        q_refs = refs[: len(queries)]
        kv_ref, o_ref, s_ref, mx_ref, sum_ref, acc_ref = refs[len(queries):]
        batch, side = pl.program_id(0), pl.program_id(1)
        slab = slab_ref[side]
        length = lens_ref[chunk * n_chunk + batch]
        n_key = jnp.minimum(slab // 2 + 1, (length + key_rows - 1) // key_rows)
        parts = []
        for q_ref in q_refs:
            for blk in range(q_ref.shape[0]):
                for head in range(per_block):
                    parts.append(q_ref[blk, 0, :, head * head_dim:(head + 1) * head_dim])
        q = jnp.concatenate(parts, axis=0)
        row_pos = slab * slab_len + lax.rem(lax.broadcasted_iota(jnp.int32, (rows, key_rows), 0), slab_len)
        key_pos = lax.broadcasted_iota(jnp.int32, (rows, key_rows), 1)
        room = jnp.minimum(row_pos + 1, length) - key_pos
        mx_ref[...] = jnp.full_like(mx_ref, -1e30)

        def score(kb, carry):
            k = kv_ref[pl.ds(2 * kb, 2), 0, :, :head_dim].reshape(key_rows, head_dim)
            s = lax.dot_general(q, k, (((1,), (1,)), ((), ())), preferred_element_type=jnp.float32) * scale
            s = jnp.where(room > kb * key_rows, s, -1e30)
            s_ref[kb] = s
            mx_ref[...] = jnp.maximum(mx_ref[...], jnp.maximum(s[:, :slab_len], s[:, slab_len:]))
            return carry

        lax.fori_loop(0, n_key, score, 0)
        top = jnp.max(mx_ref[...], axis=-1, keepdims=True)
        mx_ref[...] = jnp.broadcast_to(top, mx_ref.shape)
        sum_ref[...] = jnp.zeros_like(sum_ref)
        acc_ref[...] = jnp.zeros_like(acc_ref)

        def weigh(kb, carry):
            v = kv_ref[pl.ds(2 * kb, 2), 0, :, head_dim:].reshape(key_rows, head_dim)
            top_b = mx_ref[...]
            e_lo = jnp.exp2(s_ref[kb, :, :slab_len] - top_b)
            e_hi = jnp.exp2(s_ref[kb, :, slab_len:] - top_b)
            sum_ref[...] += e_lo + e_hi
            e = jnp.concatenate([e_lo, e_hi], axis=1).astype(jnp.bfloat16)
            acc_ref[...] += jnp.dot(e, v, preferred_element_type=jnp.float32)
            return carry

        lax.fori_loop(0, n_key, weigh, 0)
        out = (acc_ref[...] / jnp.sum(sum_ref[...], axis=-1, keepdims=True)).astype(jnp.bfloat16)
        for blk in range(n_blocks):
            for head in range(per_block):
                at = (blk * per_block + head) * slab_len
                o_ref[blk, 0, :, head * head_dim:(head + 1) * head_dim] = out[at:at + slab_len]

    in_specs = [
        pl.BlockSpec((q.shape[0], 1, slab_len, cols), functools.partial(lambda b, s, lens, slabs, off: (0, s, off + b, 0), off=off))
        for q, off in zip(queries, offset)
    ]
    in_specs.append(pl.BlockSpec((n_slab, 1, slab_len, two_hd), lambda b, s, lens, slabs: (0, kv_offset + b, 0, 0)))
    return pl.pallas_call(
        body,
        out_shape=jax.ShapeDtypeStruct((n_blocks, 2, n_chunk * slab_len, cols), jnp.bfloat16),
        grid_spec=pltpu.PrefetchScalarGridSpec(
            num_scalar_prefetch=2,
            grid=(n_chunk, 2),
            in_specs=in_specs,
            out_specs=pl.BlockSpec((n_blocks, 1, slab_len, cols), lambda b, s, lens, slabs: (0, s, b, 0)),
            scratch_shapes=[
                pltpu.VMEM((n_slab // 2, rows, key_rows), jnp.float32),
                pltpu.VMEM((rows, slab_len), jnp.float32),
                pltpu.VMEM((rows, slab_len), jnp.float32),
                pltpu.VMEM((rows, head_dim), jnp.float32),
            ],
        ),
        compiler_params=pltpu.CompilerParams(dimension_semantics=("arbitrary", "arbitrary"), vmem_limit_bytes=40 * MIB),
        cost_estimate=pl.CostEstimate(flops=n_chunk * 2 * rows * n_slab * slab_len * head_dim * 6, bytes_accessed=n_chunk * 2 * rows * cols * 4, transcendentals=0),
        name="attend",
    )(lens, slabs, *queries, keys_values)


def out_proj(attn, mids, weights, chunk, rows, cols):
    n_blocks, _, _, attn_cols = attn.shape
    ff = mids[0].shape[3]
    depth, d_model = weights[0].shape

    def body(*refs):
        o_ref = refs[0]
        m_refs = refs[1:1 + len(mids)]
        w_refs = refs[1 + len(mids):1 + len(mids) + n_blocks]
        own_ref, par_ref = refs[-2:]
        total = None
        blk = 0
        for m_ref in m_refs:
            for inner in range(m_ref.shape[0]):
                w_ref = w_refs[blk]
                part = jnp.dot(m_ref[inner].reshape(2 * rows, ff), w_ref[attn_cols:, :], preferred_element_type=jnp.float32)
                total = part if total is None else total + part
                total = total + jnp.dot(o_ref[blk].reshape(2 * rows, attn_cols), w_ref[:attn_cols, :], preferred_element_type=jnp.float32)
                blk += 1
        z = total.astype(jnp.bfloat16)
        own_ref[...] = z[:rows]
        par_ref[...] = z[rows:]

    in_specs = [pl.BlockSpec((n_blocks, 2, rows, attn_cols), lambda n: (0, 0, 0, 0))]
    for mid in mids:
        at = chunk if mid.shape[2] > rows else 0
        in_specs.append(pl.BlockSpec((mid.shape[0], 2, rows, ff), functools.partial(lambda n, at: (0, 0, at, 0), at=at)))
    in_specs += [pl.BlockSpec((depth, cols), lambda n: (0, n)) for _ in weights]
    out = jax.ShapeDtypeStruct((rows, d_model), jnp.bfloat16)
    return pl.pallas_call(
        body,
        out_shape=(out, out),
        grid=(d_model // cols,),
        in_specs=in_specs,
        out_specs=(pl.BlockSpec((rows, cols), lambda n: (0, n)),) * 2,
        compiler_params=pltpu.CompilerParams(dimension_semantics=("arbitrary",), vmem_limit_bytes=60 * MIB),
        cost_estimate=pl.CostEstimate(flops=2 * 2 * rows * n_blocks * depth * d_model, bytes_accessed=n_blocks * 2 * (depth * d_model + 2 * rows * depth), transcendentals=0),
        name="out_proj",
    )(attn, *mids, *weights)


def solution(mesh):
    batch_axes = ("rep", "data")
    n_data, n_model = mesh.shape["data"], mesh.shape["model"]
    n_chip = n_model // 2

    def chip_pairs(other):
        return [(2 * x + c, 2 * other(x) + c) for x in range(n_chip) for c in range(2)]

    def near(x):
        return x ^ 1

    def across(x):
        return n_chip - 1 - x

    mates = [(m, m ^ 1) for m in range(n_model)]
    up = [(y, (y + 1) % n_data) for y in range(n_data)]
    down = [(y, (y - 1) % n_data) for y in range(n_data)]

    def after(values, *others):
        return lax.optimization_barrier((values,) + others)[0]

    def local_step(x_loc, lens_loc, gamma_loc, w_in_loc, w_kv_loc, w_out_loc):
        n_batch, slab_len, d_model = x_loc.shape
        head_dim = w_kv_loc.shape[2] // 2
        in_local = w_in_loc.shape[2]
        out_local = w_out_loc.shape[1]
        ff = in_local - out_local
        attn_cols = out_local - ff
        n_layers = gamma_loc.shape[0]
        n_chunk = 2
        chunks = n_batch // n_chunk
        rows = n_chunk * slab_len

        me_y = lax.axis_index("data")
        me_m = lax.axis_index("model")
        slots = lax.rem(me_y + jnp.arange(n_data, dtype=jnp.int32), n_data)
        token_pair = [near if layer % 2 == 0 else across for layer in range(n_layers)]
        weight_pair = [across if layer % 2 == 0 else near for layer in range(n_layers)]

        def partner_slab(other):
            table = jnp.array([2 * other(m // 2) + m % 2 for m in range(n_model)], jnp.int32)
            return jnp.stack([me_m, table[me_m]]).astype(jnp.int32)

        gains = [gamma_loc]
        for k in range(1, n_data):
            gains.append(lax.ppermute(gamma_loc, "data", [(y, (y - k) % n_data) for y in range(n_data)]))
        ring = jnp.concatenate(gains + gains[:-1], axis=1)
        width = gamma_loc.shape[1]
        gamma = lax.dynamic_slice_in_dim(ring, lax.rem(n_data - me_y, n_data) * width, n_data * width, axis=1)
        w_kv = lax.all_gather(w_kv_loc, "data", axis=1, tiled=True)

        def pieces_of(own):
            half = own.shape[0] // 2
            below = lax.ppermute(own, "data", up)
            above = lax.ppermute(own, "data", down)
            far_a = lax.ppermute(below[:half], "data", up)
            far_b = lax.ppermute(above[half:], "data", down)
            return own, below, above, far_a, far_b

        def neighbour_pieces(own, far_a, far_b, pairs):
            first = lax.ppermute(own, "model", pairs)
            below = lax.ppermute(first, "data", up)
            above = lax.ppermute(first, "data", down)
            return first, below, above, lax.ppermute(far_a, "model", pairs), lax.ppermute(far_b, "model", pairs)

        def gather_layer(own_in, own_out, pairs):
            blocks = {}
            for name, own, axis in (("in", own_in, 0), ("out", own_out, 1)):
                mine = pieces_of(own)
                theirs = neighbour_pieces(own, mine[3], mine[4], pairs)
                block_a = assemble(slots, mine, n_data, axis)
                block_c = assemble(slots, theirs, n_data, axis)
                block_b = lax.ppermute(block_a, "model", mates)
                block_d = lax.ppermute(block_c, "model", mates)
                blocks[name] = (block_a, block_b, block_c, block_d)
            return blocks

        blocks = []
        order = ()
        for layer in range(n_layers):
            own_in, own_out = w_in_loc[layer], w_out_loc[layer]
            if order:
                own_in, own_out = after((own_in, own_out), *order)
            got = gather_layer(own_in, own_out, chip_pairs(weight_pair[layer]))
            order = (got["out"][0],)
            blocks.append(got)

        own = [x_loc[c * n_chunk:(c + 1) * n_chunk].reshape(rows, d_model) for c in range(chunks)]
        kv_parts, result = None, None
        for layer in range(n_layers):
            pairs = chip_pairs(token_pair[layer])
            slabs = partner_slab(token_pair[layer])
            gain = gamma[layer:layer + 1]
            w_in, w_out = blocks[layer]["in"], blocks[layer]["out"]
            if layer == 0:
                x_all = x_loc.reshape(n_batch * slab_len, d_model)
                other = lax.ppermute(x_all, "model", pairs)
                kv = keys_values_of(x_all, gain, w_kv[layer], rows)
                kv_all = lax.all_gather(kv.reshape(n_batch, slab_len, 2 * head_dim), "model", axis=0)
                h = norm_pair(x_all, other, gain, rows)
                results = [in_proj(h, [w], attn_cols, ff, 512) for w in w_in]
                q_list = [[q for q, _ in results]] * chunks
                m_list = [[m for _, m in results]] * chunks
                kv_list = [kv_all] * chunks
            else:
                q_list, m_list, kv_list = [], [], []
                for c in range(chunks):
                    other = lax.ppermute(own[c], "model", pairs)
                    kv_list.append(lax.all_gather(kv_parts[c].reshape(n_chunk, slab_len, 2 * head_dim), "model", axis=0))
                    h = norm_pair(own[c], other, gain, slab_len)
                    q, m = in_proj(h, list(w_in), attn_cols, ff, rows)
                    q_list.append([q])
                    m_list.append([m])
            new, kv_parts = [], []
            for c in range(chunks):
                attn = attend(lens_loc, slabs, q_list[c], kv_list[c], c, n_chunk)
                z_own, z_par = out_proj(attn, m_list[c], w_out, c, rows, 512)
                z_got = lax.ppermute(z_par, "model", pairs)
                if layer + 1 < n_layers:
                    y, kv = finish_layer(own[c], z_own, z_got, gamma[layer + 1:layer + 2], w_kv[layer + 1], slab_len)
                    new.append(y)
                    kv_parts.append(kv)
                else:
                    result = finish_last(own[c], z_own, z_got, result, c, n_batch * slab_len, slab_len)
            own = new
        return result.reshape(n_batch, slab_len, d_model)

    in_specs = (
        P(batch_axes, "model", None),
        P(batch_axes),
        P(None, "data"),
        P(None, "data", "model"),
        P(None, "data", None),
        P(None, "model", "data"),
    )
    return jax.shard_map(local_step, mesh=mesh, in_specs=in_specs, out_specs=P(batch_axes, "model", None), check_vma=False)
```

```python
import functools

import jax
import jax.numpy as jnp
from jax import lax
from jax.experimental import pallas as pl
from jax.experimental.pallas import tpu as pltpu
from jax.sharding import PartitionSpec as P

EPSILON = 1e-6
VMEM_LIMIT = 66_000_000
MESH = pl.DeviceIdType.MESH
BF16, F32 = jnp.bfloat16, jnp.float32

UP, DOWN, FORWARD, FIRST, SIDE_UP, SIDE_DOWN, FAR, MATE, SIDE_MATE, KINDS = 0, 1, 2, 3, 4, 5, 6, 7, 11, 15


def rms_norm(x_in, gain):
    x_f32 = x_in.astype(F32)
    inv_rms = lax.rsqrt(jnp.mean(x_f32 * x_f32, axis=-1, keepdims=True) + EPSILON)
    return (x_f32 * inv_rms * gain.astype(F32)).astype(BF16)


class Place:
    def __init__(self, n_data, n_model, partner, neighbour):
        self.n_data, self.n_model = n_data, n_model
        self.y = lax.axis_index("data")
        self.me = lax.axis_index("model")
        self.up = lax.rem(self.y + 1, n_data)
        self.down = lax.rem(self.y + n_data - 1, n_data)
        self.far = lax.rem(self.y + 2, n_data)
        self.slots = (self.y, self.down, self.up, self.far)
        self.mate = self.me + 1 - 2 * lax.rem(self.me, 2)
        self.partner, self.neighbour = partner(self.me), neighbour(self.me)
        n_other = n_model // 2 - 1
        self.ahead = [lax.rem(self.me + 2 * k, n_model) for k in range(1, n_other + 1)]
        self.behind = [lax.rem(self.me + n_model - 2 * k, n_model) for k in range(1, n_other + 1)]

    def meet(self):
        barrier = pltpu.get_barrier_semaphore()
        targets = [{"data": self.up}, {"data": self.down}, {"data": self.far}, {"model": self.mate}]
        targets += [{"model": m} for m in self.ahead]
        for target in targets:
            pl.semaphore_signal(barrier, inc=1, device_id=target, device_id_type=MESH)
        pl.semaphore_wait(barrier, len(targets))


def remote(src, dst, send, recv, target):
    return pltpu.make_async_remote_copy(
        src_ref=src, dst_ref=dst, send_sem=send, recv_sem=recv, device_id=target, device_id_type=MESH
    )


class Gather:
    def __init__(self, place, buf, own, send, recv, local, first=None, column=None):
        self.place, self.buf, self.own, self.first, self.column = place, buf, own, first, column
        self.send, self.recv, self.local = send, recv, local

    def at(self, block, p, slot):
        return self.buf.at[block, p, slot]

    def _copy(self, src, dst, kind, p, target):
        return remote(src, dst, self.send.at[kind, p], self.recv.at[kind, p], target)

    def up(self, p):
        y = self.place.y
        return self._copy(self.own(p), self.at(0, p, y), UP, p, {"data": self.place.up})

    def down(self, p):
        y = self.place.y
        return self._copy(self.own(p), self.at(0, p, y), DOWN, p, {"data": self.place.down})

    def forward(self, p):
        even = lax.rem(p, 2) == 0
        slot = jnp.where(even, self.place.down, self.place.up)
        target = jnp.where(even, self.place.up, self.place.down)
        return self._copy(self.at(0, p, slot), self.at(0, p, slot), FORWARD, p, {"data": target})

    def neighbour_first(self, p):
        return self._copy(self.own(p), self.at(2, p, self.place.y), FIRST, p, {"model": self.place.neighbour})

    def _first(self, p):
        return self.at(2, p, self.place.y) if self.first is None else self.first.at[p]

    def side_up(self, p):
        return self._copy(self._first(p), self.at(2, p, self.place.y), SIDE_UP, p, {"data": self.place.up})

    def side_down(self, p):
        return self._copy(self._first(p), self.at(2, p, self.place.y), SIDE_DOWN, p, {"data": self.place.down})

    def neighbour_far(self, p):
        far = self.place.far
        src = self.at(0, p, far) if self.column is None else self.column.at[p, far]
        return self._copy(src, self.at(2, p, far), FAR, p, {"model": self.place.neighbour})

    def mate(self, p, which):
        slot = self.place.slots[which]
        if which == 0:
            src = self.own(p)
        else:
            src = self.at(0, p, slot) if self.column is None else self.column.at[p, slot]
        return self._copy(src, self.at(1, p, slot), MATE + which, p, {"model": self.place.mate})

    def side_mate(self, p, which):
        slot = self.place.slots[which]
        src = self._first(p) if which == 0 else self.at(2, p, slot)
        return self._copy(src, self.at(3, p, slot), SIDE_MATE + which, p, {"model": self.place.mate})

    def load_own(self, p):
        return pltpu.make_async_copy(self.own(p), self.at(0, p, self.place.y), self.local.at[0, p])

    def load_column(self, p, which):
        slot = self.place.slots[which]
        return pltpu.make_async_copy(self.column.at[p, slot], self.at(0, p, slot), self.local.at[which, p])

    def load_first(self, p):
        return pltpu.make_async_copy(self.first.at[p], self.at(2, p, self.place.y), self.local.at[4, p])

    def pass_side(self, p):
        self.side_up(p).wait_recv()
        self.side_mate(p, 1).start()
        self.side_down(p).wait_recv()
        self.side_mate(p, 2).start()
        self.neighbour_far(p).wait_recv()
        self.side_mate(p, 3).start()

    def wait_sends(self, p):
        made = [self.side_up(p), self.side_down(p), self.neighbour_far(p)]
        if self.column is None:
            made += [self.up(p), self.down(p), self.forward(p)]
        if self.first is None:
            made.append(self.neighbour_first(p))
        made += [self.mate(p, which) for which in range(4)] + [self.side_mate(p, which) for which in range(4)]
        for copy in made:
            copy.wait_send()


class Prefetch:
    def __init__(self, place, own, send, recv, neighbour=None, first=None, column=None):
        self.place, self.own, self.send, self.recv = place, own, send, recv
        self.neighbour, self.first, self.column = neighbour, first, column

    def up(self, p):
        dst = self.column.at[p, self.place.y]
        return remote(self.own(p), dst, self.send.at[0, p], self.recv.at[0, p], {"data": self.place.up})

    def down(self, p):
        dst = self.column.at[p, self.place.y]
        return remote(self.own(p), dst, self.send.at[1, p], self.recv.at[1, p], {"data": self.place.down})

    def forward(self, p):
        even = lax.rem(p, 2) == 0
        slot = jnp.where(even, self.place.down, self.place.up)
        target = jnp.where(even, self.place.up, self.place.down)
        ref = self.column.at[p, slot]
        return remote(ref, ref, self.send.at[2, p], self.recv.at[2, p], {"data": target})

    def neighbour_first(self, p):
        return remote(self.own(p), self.first.at[p], self.send.at[3, p], self.recv.at[3, p], {"model": self.neighbour})


def in_pieces(layer, head_ref, w_ref, c, ff):
    def own(p):
        if isinstance(p, int) and p < 2:
            return head_ref.at[layer, :, pl.ds(p * c, c)]
        column = (p // 2) * c + lax.rem(p, 2) * ff
        return w_ref.at[layer, :, pl.ds(pl.multiple_of(column, c), c)]

    return own


def out_pieces(layer, w_ref, width):
    def own(p):
        return w_ref.at[layer, :, pl.ds(pl.multiple_of(p * width, width), width)]

    return own


def project(layer, n_data, n_model, partner, neighbour, next_neighbour, x_own, head, w_in, w_out, extra):
    start_layer = layer == 0
    rows, d_model = x_own.shape
    part, two_c = head.shape[1:]
    c = two_c // 2
    depth, out_part = w_out.shape[1:]
    ff = depth - c
    n_group = 1 + ff // c
    pieces = 2 * n_group
    width = out_part // 2
    n_units = 8 * n_group
    row_parts = 4
    row_part = rows // row_parts
    n_other = n_model // 2 - 1
    gain_shape = (n_data, 8, part)

    def kernel(*refs):
        x_ref, head_ref, w_ref, wo_ref = refs[:4]
        if start_layer:
            gain_ref = refs[4]
            q_ref, m_ref, kv_ref, gains_ref, out_first_ref, in_first_ref = refs[5:11]
            first_ref = column_ref = None
            rest = refs[11:]
        else:
            par_ref, gain_ref, first_ref, column_ref = refs[4:8]
            q_ref, m_ref, kv_ref, out_first_ref, out_column_ref = refs[8:13]
            rest = refs[13:]
        wbuf, h_ref, gbuf, stage, kv_stage, send, recv, w_local, next_send, next_recv, late_send, late_recv = rest[:12]
        x_send, x_recv, g_send, g_recv, kv_send, kv_recv, local, out_sem = rest[12:]

        place = Place(n_data, n_model, partner, neighbour)
        place.meet()
        w = Gather(place, wbuf, in_pieces(layer, head_ref, w_ref, c, ff), send, recv, w_local, first_ref, column_ref)
        out_own = out_pieces(layer, wo_ref, width)
        if start_layer:
            out_next = Prefetch(place, out_own, next_send, next_recv, place.neighbour, out_first_ref)
            in_own = in_pieces(layer + 1, head_ref, w_ref, c, ff)
            in_next = Prefetch(place, in_own, late_send, late_recv, next_neighbour(place.me), in_first_ref)
        else:
            out_next = Prefetch(place, out_own, next_send, next_recv, place.neighbour, out_first_ref, out_column_ref)

        def c_x(part_no):
            piece = pl.ds(part_no * row_part, row_part)
            return remote(
                x_ref.at[piece], h_ref.at[1, piece], x_send.at[part_no], x_recv.at[part_no], {"model": place.partner}
            )

        def c_gain(which):
            target = {"data": (place.up, place.down, place.far)[which]}
            return remote(gain_ref, gbuf.at[place.y], g_send.at[which], g_recv.at[which], target)

        def c_kv(which):
            ref = kv_ref.at[place.me]
            return remote(ref, ref, kv_send.at[which], kv_recv.at[which], {"model": place.ahead[which]})

        def c_kv_mate(which):
            ref = kv_ref.at[place.me if which == 0 else place.behind[which - 1]]
            at = n_other + which
            return remote(ref, ref, kv_send.at[at], kv_recv.at[at], {"model": place.mate})

        save_kv = pltpu.make_async_copy(kv_stage, kv_ref.at[place.me], local.at[0])
        load_x = pltpu.make_async_copy(x_ref, h_ref.at[0], local.at[0])

        if start_layer:
            load_gain = pltpu.make_async_copy(gain_ref, gbuf.at[place.y], local.at[1])
            for which in range(3):
                c_gain(which).start()
        else:
            load_gain = pltpu.make_async_copy(gain_ref, gbuf, local.at[1])
            load_par = pltpu.make_async_copy(par_ref, h_ref.at[1], local.at[2])
        load_gain.start()
        load_x.start()
        if start_layer:
            for p in range(4):
                w.up(p).start()
                w.down(p).start()
            for p in range(pieces):
                w.neighbour_first(p).start()
                w.load_own(p).start()
            for part_no in range(row_parts):
                c_x(part_no).start()
            for p in range(pieces):
                w.mate(p, 0).start()
        else:
            load_par.start()
            for p in range(pieces):
                w.load_own(p).start()
                for which in range(1, 4):
                    w.load_column(p, which).start()
                w.mate(p, 0).start()
                w.side_up(p).start()
                w.side_down(p).start()
                w.neighbour_far(p).start()
                for which in range(1, 4):
                    w.mate(p, which).start()
            for p in range(pieces):
                w.load_first(p).start()
                w.side_mate(p, 0).start()
            for p in range(2):
                out_next.neighbour_first(p).start()
                out_next.up(p).start()
                out_next.down(p).start()

        def ring_stage(g):
            for p in (2 * g, 2 * g + 1):
                w.up(p).wait_recv()
                w.down(p).wait_recv()
                w.forward(p).start()

            @pl.when(g + 2 < n_group)
            def _():
                for p in (2 * g + 4, 2 * g + 5):
                    w.up(p).start()
                    w.down(p).start()

            for p in (2 * g, 2 * g + 1):
                w.mate(p, 1).start()
                w.mate(p, 2).start()

        if start_layer:
            for which in range(3):
                c_gain(which).wait_recv()
        load_gain.wait()
        gain = jnp.concatenate([gbuf[k, layer:layer + 1, :] for k in range(n_data)], axis=1)
        if start_layer:
            save_gain = pltpu.make_async_copy(gbuf, gains_ref, local.at[1])
            save_gain.start()
        load_x.wait()

        def norm_rows(side, part_no):
            piece = pl.ds(part_no * row_part, row_part)
            h_ref[side, piece] = rms_norm(h_ref[side, piece], gain)

        @pl.loop(0, row_parts)
        def _(part_no):
            norm_rows(0, part_no)

        if start_layer:
            ring_stage(0)
        else:
            load_par.wait()

            @pl.loop(0, row_parts)
            def _(part_no):
                norm_rows(1, part_no)

        half, quarter = n_units // 2, n_units // 4

        def out_copy(slot, blk, side, g):
            def to_q():
                return pltpu.make_async_copy(stage.at[slot], q_ref.at[blk, side], out_sem.at[slot])

            def to_m():
                column = pl.ds(pl.multiple_of((g - 1) * c, c), c)
                return pltpu.make_async_copy(stage.at[slot], m_ref.at[blk, side, :, column], out_sem.at[slot])

            return to_q, to_m

        @pl.loop(0, n_units)
        def _(step):
            late = step - half
            if start_layer:
                opening, second = step < quarter, (step >= quarter) & (step < half)
                g = jnp.where(opening, step // 2, jnp.where(second, (step - quarter) // 2, late // 4))
                blk = jnp.where(step < half, lax.rem(step, 2), 2 + lax.rem(late, 4) // 2)
                side = jnp.where(opening, 0, jnp.where(second, 1, lax.rem(late, 2)))

                @pl.when(opening & (blk == 0))
                def _():
                    @pl.when(g + 1 < n_group)
                    def _():
                        ring_stage(g + 1)

                    @pl.when(g + 2 == n_group)
                    def _():
                        @pl.loop(0, pieces)
                        def _(p):
                            w.neighbour_first(p).wait_recv()
                            w.side_up(p).start()
                            w.side_down(p).start()
                            w.side_mate(p, 0).start()

                    for p in (2 * g, 2 * g + 1):
                        w.forward(p).wait_recv()
                        w.mate(p, 3).start()
                        w.neighbour_far(p).start()
                        w.load_own(p).wait()

                @pl.when(opening & (blk == 1))
                def _():
                    for p in (2 * g, 2 * g + 1):
                        for which in range(4):
                            w.mate(p, which).wait_recv()

                @pl.when(step == quarter)
                def _():
                    @pl.loop(0, row_parts)
                    def _(part_no):
                        c_x(part_no).wait_recv()
                        norm_rows(1, part_no)

                    for p in range(2):
                        out_next.neighbour_first(p).start()
                    for p in range(pieces):
                        in_next.neighbour_first(p).start()
            else:
                g = jnp.where(late < 0, step, late) // 4
                blk = jnp.where(late < 0, 0, 2) + lax.rem(step, 4) // 2
                side = lax.rem(step, 2)

                @pl.when((late < 0) & (lax.rem(step, 4) == 0))
                def _():
                    for p in (2 * g, 2 * g + 1):
                        w.load_own(p).wait()
                        for which in range(1, 4):
                            w.load_column(p, which).wait()

                @pl.when((late < 0) & (lax.rem(step, 4) == 2))
                def _():
                    for p in (2 * g, 2 * g + 1):
                        for which in range(4):
                            w.mate(p, which).wait_recv()

                @pl.when(step == half - 2)
                def _():
                    @pl.loop(0, pieces)
                    def _(p):
                        w.load_first(p).wait()

                @pl.when(step == n_units - 4)
                def _():
                    for p in range(2):
                        out_next.up(p).wait_recv()
                        out_next.down(p).wait_recv()
                        out_next.forward(p).start()

            @pl.when(step == half - 2)
            def _():
                for p in range(2):
                    w.pass_side(p)

            @pl.when((late >= 0) & (lax.rem(late, 4) == 2))
            def _():
                @pl.when(g + 1 < n_group)
                def _():
                    for p in (2 * g + 2, 2 * g + 3):
                        w.pass_side(p)

                for p in (2 * g, 2 * g + 1):
                    for which in range(4):
                        w.side_mate(p, which).wait_recv()

            slot = lax.rem(step, 2)
            to_q, to_m = out_copy(slot, blk, side, g)

            @pl.when(step >= 2)
            def _():
                to_q().wait()

            def columns(p):
                return wbuf[blk, p].reshape(d_model, c)

            @pl.when(g == 0)
            def _():
                q = jnp.dot(h_ref[side], columns(0), preferred_element_type=F32)
                stage[slot] = q.astype(BF16)
                to_q().start()

            @pl.when(g > 0)
            def _():
                h_val = h_ref[side]
                gate = jnp.dot(h_val, columns(2 * g), preferred_element_type=F32).astype(BF16).astype(F32)
                raised = jnp.dot(h_val, columns(2 * g + 1), preferred_element_type=F32).astype(BF16).astype(F32)
                stage[slot] = (gate * jax.nn.sigmoid(gate) * raised).astype(BF16)
                to_m().start()

            @pl.when(step == 0)
            def _():
                kv_stage[...] = jnp.dot(h_ref[0], columns(1), preferred_element_type=F32).astype(BF16)
                save_kv.start()

            @pl.when(step == 1)
            def _():
                save_kv.wait()
                for which in range(n_other):
                    c_kv(which).start()
                c_kv_mate(0).start()

            @pl.when(step == quarter)
            def _():
                for which in range(n_other):
                    c_kv(which).wait_recv()
                    c_kv_mate(1 + which).start()

        for which in range(n_other + 1):
            c_kv_mate(which).wait()
        for which in range(n_other):
            c_kv(which).wait_send()
        if start_layer:
            save_gain.wait()
            for which in range(3):
                c_gain(which).wait_send()
            for part_no in range(row_parts):
                c_x(part_no).wait_send()
            for p in range(pieces):
                in_next.neighbour_first(p).wait()
        else:
            for p in range(2):
                out_next.forward(p).wait()
                out_next.up(p).wait_send()
                out_next.down(p).wait_send()
        for p in range(2):
            out_next.neighbour_first(p).wait()
        for slot in range(2):
            pltpu.make_async_copy(stage.at[slot], q_ref.at[0, 0], out_sem.at[slot]).wait()

        @pl.loop(0, pieces)
        def _(p):
            w.wait_sends(p)

    anywhere = pl.BlockSpec(memory_space=pl.ANY)
    out_shape = [
        jax.ShapeDtypeStruct((4, 2, rows, c), BF16),
        jax.ShapeDtypeStruct((4, 2, rows, ff), BF16),
        jax.ShapeDtypeStruct((n_model, rows, c), BF16),
    ]
    if start_layer:
        out_shape += [
            jax.ShapeDtypeStruct(gain_shape, F32),
            jax.ShapeDtypeStruct((2, depth, width), BF16),
            jax.ShapeDtypeStruct((pieces, part, c), BF16),
        ]
    else:
        out_shape += [
            jax.ShapeDtypeStruct((2, depth, width), BF16),
            jax.ShapeDtypeStruct((2, n_data, depth, width), BF16),
        ]
    dma = pltpu.SemaphoreType.DMA
    args = (x_own, head, w_in, w_out) + tuple(extra)
    return pl.pallas_call(
        kernel,
        out_shape=out_shape,
        in_specs=[anywhere] * len(args),
        out_specs=[anywhere] * len(out_shape),
        scratch_shapes=[
            pltpu.VMEM((4, pieces, n_data, part, c), BF16),
            pltpu.VMEM((2, rows, d_model), BF16),
            pltpu.VMEM(gain_shape, F32),
            pltpu.VMEM((2, rows, c), BF16),
            pltpu.VMEM((rows, c), BF16),
            dma((KINDS, pieces)), dma((KINDS, pieces)), dma((5, pieces)),
            dma((4, 2)), dma((4, 2)), dma((4, pieces)), dma((4, pieces)),
            dma((row_parts,)), dma((row_parts,)), dma((3,)), dma((3,)),
            dma((n_model - 1,)), dma((n_model - 1,)), dma((3,)), dma((2,)),
        ],
        compiler_params=pltpu.CompilerParams(collective_id=2 * layer, has_side_effects=True, vmem_limit_bytes=VMEM_LIMIT),
        cost_estimate=pl.CostEstimate(flops=4 * rows * d_model * 4 * (c + 2 * ff), bytes_accessed=16 * rows * d_model, transcendentals=0),
        name=f"project_{layer}",
    )(*args)


def attend_and_sum(layer, last, n_data, n_model, partner, neighbour, next_partner, lens, q, m, kv, x_own, w_in, w_out, head, first, column):
    n_blocks, _, rows, c = q.shape
    ff = m.shape[3]
    d_model = x_own.shape[1]
    depth, out_part = w_out.shape[1:]
    width = out_part // 2
    head_dim = c // 2
    n_batch = lens.shape[0]
    slab_len = rows // n_batch
    chunks = 4
    n_seq = n_batch // chunks
    crow = rows // chunks
    tiles = chunks * n_data
    heads = n_blocks * 2
    qrows = heads * slab_len
    key_rows = 2 * slab_len
    scale = head_dim ** -0.5 * 1.4426950408889634
    part = head.shape[1]
    in_count = 2 * (1 + ff // c)
    ready = column is not None
    held = tiles // 2

    def kernel(*refs):
        lens_ref, q_ref, m_ref, kv_ref, x_ref, wo_ref, first_ref = refs[:7]
        at = 7
        column_ref = None
        if ready:
            column_ref = refs[at]
            at += 1
        if not last:
            head_ref, wi_ref = refs[at:at + 2]
            at += 2
        y_ref = refs[at]
        at += 1
        if not last:
            par_ref, in_column_ref = refs[at:at + 2]
            at += 2
        (wbuf, obuf, kvb, mbuf, xb, zb, zr, z_stage, s_ref, mx_ref, sum_ref, acc_ref,
         send, recv, w_local, in_send, in_recv, z_send, z_recv, y_send, y_recv, y_save, x_sem, m_sem, local) = refs[at:]

        place = Place(n_data, n_model, partner, neighbour)
        place.meet()
        w = Gather(place, wbuf, out_pieces(layer, wo_ref, width), send, recv, w_local, first_ref, column_ref)

        def tile_of(k):
            which = k // chunks
            slot = jnp.where(which == 0, place.y, jnp.where(which == 1, place.down, jnp.where(which == 2, place.up, place.far)))
            return lax.rem(k, chunks), which, slot

        def whole(ref, chunk, slot):
            return ref.at[pl.ds(pl.multiple_of(chunk * crow, crow), crow), pl.ds(pl.multiple_of(slot * out_part, out_part), out_part)]

        load_q = pltpu.make_async_copy(q_ref, obuf, local.at[0])
        load_kv = pltpu.make_async_copy(kv_ref, kvb, local.at[1])

        def load_m(k):
            chunk, _, _ = tile_of(k)
            slot = lax.rem(k, 2)
            return pltpu.make_async_copy(
                m_ref.at[:, :, pl.ds(pl.multiple_of(chunk * crow, crow), crow)], mbuf.at[slot], m_sem.at[slot]
            )

        def load_x(k):
            chunk, _, slot = tile_of(k)
            return pltpu.make_async_copy(whole(x_ref, chunk, slot), xb.at[chunk, slot], x_sem.at[k])

        def c_z(k):
            chunk, _, slot = tile_of(k)
            return remote(z_stage.at[lax.rem(k, 4)], zr.at[chunk, slot], z_send.at[k], z_recv.at[k], {"model": place.partner})

        def c_y(k):
            chunk, _, slot = tile_of(k)
            target = {"model": next_partner(place.me)}
            return remote(xb.at[chunk, slot], whole(par_ref, chunk, slot), y_send.at[k], y_recv.at[k], target)

        def save_y(k):
            chunk, _, slot = tile_of(k)
            return pltpu.make_async_copy(xb.at[chunk, slot], whole(y_ref, chunk, slot), y_save.at[k])

        load_q.start()
        load_kv.start()
        load_m(0).start()
        for p in range(2):
            w.load_own(p).start()
            w.load_first(p).start()
            w.mate(p, 0).start()
            w.side_mate(p, 0).start()
        for p in range(2):
            if ready:
                for which in range(1, 4):
                    w.load_column(p, which).start()
                    w.mate(p, which).start()
                w.neighbour_far(p).start()
            else:
                w.up(p).start()
                w.down(p).start()
        for p in range(2):
            w.side_up(p).start()
            w.side_down(p).start()
        if not last:
            in_next = Prefetch(place, in_pieces(layer + 1, head_ref, wi_ref, c, ff), in_send, in_recv, column=in_column_ref)

        @pl.loop(0, tiles)
        def _(k):
            load_x(k).start()

        load_q.wait()
        load_kv.wait()

        def attend_one(batch, side):
            slab = jnp.where(side == 0, place.me, place.partner)
            length = lens_ref[batch]
            n_key = slab // 2 + 1
            at_row = pl.ds(pl.multiple_of(batch * slab_len, slab_len), slab_len)
            parts = []
            for blk in range(n_blocks):
                for one in range(2):
                    parts.append(obuf[blk, side, at_row, one * head_dim:(one + 1) * head_dim])
            q_val = jnp.concatenate(parts, axis=0)
            row_pos = slab * slab_len + lax.rem(lax.broadcasted_iota(jnp.int32, (qrows, key_rows), 0), slab_len)
            key_pos = lax.broadcasted_iota(jnp.int32, (qrows, key_rows), 1)
            room = jnp.minimum(row_pos + 1, length) - key_pos
            mx_ref[...] = jnp.full_like(mx_ref, -1e30)

            def score(kb, carry):
                k = kvb[pl.ds(2 * kb, 2), at_row, :head_dim].reshape(key_rows, head_dim)
                s = lax.dot_general(q_val, k, (((1,), (1,)), ((), ())), preferred_element_type=F32) * scale
                s = jnp.where(room > kb * key_rows, s, -1e30)
                s_ref[kb] = s
                mx_ref[...] = jnp.maximum(mx_ref[...], jnp.maximum(s[:, :slab_len], s[:, slab_len:]))
                return carry

            lax.fori_loop(0, n_key, score, 0)
            top = jnp.max(mx_ref[...], axis=-1, keepdims=True)
            mx_ref[...] = jnp.broadcast_to(top, mx_ref.shape)
            sum_ref[...] = jnp.zeros_like(sum_ref)
            acc_ref[...] = jnp.zeros_like(acc_ref)

            def weigh(kb, carry):
                v = kvb[pl.ds(2 * kb, 2), at_row, head_dim:].reshape(key_rows, head_dim)
                top_b = mx_ref[...]
                e_lo = jnp.exp2(s_ref[kb, :, :slab_len] - top_b)
                e_hi = jnp.exp2(s_ref[kb, :, slab_len:] - top_b)
                sum_ref[...] += e_lo + e_hi
                e = jnp.concatenate([e_lo, e_hi], axis=1).astype(BF16)
                acc_ref[...] += jnp.dot(e, v, preferred_element_type=F32)
                return carry

            lax.fori_loop(0, n_key, weigh, 0)
            out = (acc_ref[...] / jnp.sum(sum_ref[...], axis=-1, keepdims=True)).astype(BF16)
            for blk in range(n_blocks):
                for one in range(2):
                    first_row = (blk * 2 + one) * slab_len
                    obuf[blk, side, at_row, one * head_dim:(one + 1) * head_dim] = out[first_row:first_row + slab_len]

        def settle(k):
            chunk, _, slot = tile_of(k)
            load_x(k).wait()
            c_z(k).wait_recv()
            z = zb[chunk, slot].astype(F32) + zr[chunk, slot].astype(F32)
            xb[chunk, slot] = (xb[chunk, slot].astype(F32) + z).astype(BF16)
            save_y(k).start()
            if not last:
                c_y(k).start()

        @pl.loop(0, tiles)
        def _(step):
            chunk, which, slot = tile_of(step)

            @pl.when(step + 1 < tiles)
            def _():
                load_m(step + 1).start()

            @pl.when(step < chunks)
            def _():
                @pl.loop(0, 2 * n_seq)
                def _(unit):
                    attend_one(step * n_seq + unit // 2, lax.rem(unit, 2))

            @pl.when(step == 0)
            def _():
                for p in range(2):
                    w.load_own(p).wait()
                    w.load_first(p).wait()
                    w.mate(p, 0).wait_recv()
                    w.side_mate(p, 0).wait_recv()

            if not ready:

                @pl.when(step == 2)
                def _():
                    for p in range(2):
                        w.up(p).wait_recv()
                        w.down(p).wait_recv()
                        w.forward(p).start()
                        w.mate(p, 1).start()
                        w.mate(p, 2).start()
                    if not last:
                        for p in range(4):
                            in_next.up(p).start()
                            in_next.down(p).start()

                @pl.when(step == chunks + 2)
                def _():
                    for p in range(2):
                        w.forward(p).wait_recv()
                        w.mate(p, 3).start()
                        w.neighbour_far(p).start()

            @pl.when(step == chunks)
            def _():
                for p in range(2):
                    w.side_up(p).wait_recv()
                    w.side_mate(p, 1).start()
                    w.side_down(p).wait_recv()
                    w.side_mate(p, 2).start()
                for p in range(2):
                    for one in (1, 2):
                        if ready:
                            w.load_column(p, one).wait()
                        w.mate(p, one).wait_recv()
                        w.side_mate(p, one).wait_recv()

            @pl.when(step == 3 * chunks)
            def _():
                for p in range(2):
                    w.neighbour_far(p).wait_recv()
                    w.side_mate(p, 3).start()
                for p in range(2):
                    if ready:
                        w.load_column(p, 3).wait()
                    w.mate(p, 3).wait_recv()
                    w.side_mate(p, 3).wait_recv()

            if not last:
                @pl.when((step >= chunks + 3) & (lax.rem(step, 2) == 1))
                def _():
                    g = (step - chunks - 3) // 2

                    @pl.when(g < in_count // 2 - 2)
                    def _():
                        for p in (2 * g + 4, 2 * g + 5):
                            in_next.up(p).start()
                            in_next.down(p).start()

            @pl.when(step >= 4)
            def _():
                c_z(step - 4).wait_send()

            load_m(step).wait()
            here = lax.rem(step, 2)
            rows_c = pl.ds(pl.multiple_of(chunk * crow, crow), crow)
            for p in range(2):
                total = None
                for blk in range(n_blocks):
                    mid = mbuf[here, blk].reshape(2 * crow, ff)
                    attn = obuf[blk, :, rows_c, :].reshape(2 * crow, c)
                    one = jnp.dot(mid, wbuf[blk, p, slot, c:, :], preferred_element_type=F32)
                    one = one + jnp.dot(attn, wbuf[blk, p, slot, :c, :], preferred_element_type=F32)
                    total = one if total is None else total + one
                z = total.astype(BF16)
                zb[chunk, slot, :, p * width:(p + 1) * width] = z[:crow]
                z_stage[lax.rem(step, 4), :, p * width:(p + 1) * width] = z[crow:]
            c_z(step).start()

            early = (step >= 1) & (step <= chunks)
            paced = (step >= 2 * chunks) & (lax.rem(step, 2) == 0)

            @pl.when(early | paced)
            def _():
                settle(jnp.where(early, step - 1, step // 2))

        if not last:

            @pl.loop(0, in_count)
            def _(p):
                in_next.up(p).wait_recv()
                in_next.down(p).wait_recv()
                in_next.forward(p).start()

        @pl.loop(held, tiles)
        def _(k):
            settle(k)

        @pl.loop(0, tiles)
        def _(k):
            save_y(k).wait()
            if not last:
                c_y(k).wait()

        @pl.loop(tiles - 4, tiles)
        def _(k):
            c_z(k).wait_send()

        for p in range(2):
            w.wait_sends(p)
        if not last:

            @pl.loop(0, in_count)
            def _(p):
                in_next.forward(p).wait()
                in_next.up(p).wait_send()
                in_next.down(p).wait_send()

    anywhere = pl.BlockSpec(memory_space=pl.ANY)
    args = [lens, q, m, kv, x_own, w_out, first]
    if ready:
        args.append(column)
    if not last:
        args += [head, w_in]
    out_shape = [jax.ShapeDtypeStruct((rows, d_model), BF16)]
    if not last:
        out_shape += [
            jax.ShapeDtypeStruct((rows, d_model), BF16),
            jax.ShapeDtypeStruct((in_count, n_data, part, c), BF16),
        ]
    dma = pltpu.SemaphoreType.DMA
    tile = (chunks, n_data, crow, out_part)
    return pl.pallas_call(
        kernel,
        out_shape=out_shape,
        in_specs=[pl.BlockSpec(memory_space=pltpu.SMEM)] + [anywhere] * (len(args) - 1),
        out_specs=[anywhere] * len(out_shape),
        scratch_shapes=[
            pltpu.VMEM((n_blocks, 2, n_data, depth, width), BF16),
            pltpu.VMEM(q.shape, BF16),
            pltpu.VMEM(kv.shape, BF16),
            pltpu.VMEM((2, n_blocks, 2, crow, ff), BF16),
            pltpu.VMEM(tile, BF16),
            pltpu.VMEM(tile, BF16),
            pltpu.VMEM(tile, BF16),
            pltpu.VMEM((4, crow, out_part), BF16),
            pltpu.VMEM((n_model // 2, qrows, key_rows), F32),
            pltpu.VMEM((qrows, slab_len), F32),
            pltpu.VMEM((qrows, slab_len), F32),
            pltpu.VMEM((qrows, head_dim), F32),
            dma((KINDS, 2)), dma((KINDS, 2)), dma((5, 2)), dma((4, in_count)), dma((4, in_count)),
            dma((tiles,)), dma((tiles,)), dma((tiles,)), dma((tiles,)), dma((tiles,)), dma((tiles,)), dma((2,)), dma((2,)),
        ],
        compiler_params=pltpu.CompilerParams(collective_id=2 * layer + 1, has_side_effects=True, vmem_limit_bytes=VMEM_LIMIT),
        cost_estimate=pl.CostEstimate(flops=4 * rows * n_blocks * depth * d_model, bytes_accessed=16 * rows * d_model, transcendentals=0),
        name=f"attend_and_sum_{layer}",
    )(*args)


def solution(mesh):
    batch_axes = ("rep", "data")
    n_data, n_model = mesh.shape["data"], mesh.shape["model"]
    n_chip = n_model // 2

    def near(x):
        return x + 1 - 2 * (x % 2)

    def across(x):
        return n_chip - 1 - x

    def on_chip(other):
        return lambda m: 2 * other(m // 2) + m % 2

    def local_step(x_loc, lens_loc, gamma_loc, w_in_loc, w_kv_loc, w_out_loc):
        n_batch, slab_len, d_model = x_loc.shape
        n_layers, part = gamma_loc.shape
        attn_cols = w_kv_loc.shape[2]
        partners = [on_chip(near if layer % 2 == 0 else across) for layer in range(n_layers)]
        neighbours = [on_chip(across if layer % 2 == 0 else near) for layer in range(n_layers)]

        head = jnp.concatenate([w_in_loc[:, :, :attn_cols], w_kv_loc], axis=2)
        gain_rows = jnp.zeros((8, part), F32).at[:n_layers].set(gamma_loc.astype(F32))
        own = x_loc.reshape(n_batch * slab_len, d_model)
        for layer in range(n_layers):
            last = layer + 1 == n_layers
            following = min(layer + 1, n_layers - 1)
            if layer == 0:
                extra = (gain_rows,)
                q, m, kv, gains, out_first, in_first = project(
                    layer, n_data, n_model, partners[layer], neighbours[layer], neighbours[following],
                    own, head, w_in_loc, w_out_loc, extra,
                )
                out_column = None
            else:
                extra = (other, gains, in_first, in_column)
                q, m, kv, out_first, out_column = project(
                    layer, n_data, n_model, partners[layer], neighbours[layer], neighbours[following],
                    own, head, w_in_loc, w_out_loc, extra,
                )
            outs = attend_and_sum(
                layer, last, n_data, n_model, partners[layer], neighbours[layer], partners[following],
                lens_loc, q, m, kv, own, w_in_loc, w_out_loc, head, out_first, out_column,
            )
            own = outs[0]
            if not last:
                other, in_column = outs[1:]
        return own.reshape(n_batch, slab_len, d_model)

    in_specs = (
        P(batch_axes, "model", None),
        P(batch_axes),
        P(None, "data"),
        P(None, "data", "model"),
        P(None, "data", None),
        P(None, "model", "data"),
    )
    return jax.shard_map(local_step, mesh=mesh, in_specs=in_specs, out_specs=P(batch_axes, "model", None), check_vma=False)
```

```python
import functools

import jax
import jax.numpy as jnp
from jax import lax
from jax.experimental import pallas as pl
from jax.experimental.pallas import tpu as pltpu
from jax.sharding import PartitionSpec as P

EPSILON = 1e-6
VMEM_LIMIT = 66_000_000
MESH = pl.DeviceIdType.MESH
BF16, F32 = jnp.bfloat16, jnp.float32

UP, DOWN, FORWARD, FORWARD_B, FIRST, SIDE_UP, SIDE_DOWN, FAR, MATE, SIDE_MATE = range(10)


def rms_norm(x_in, gain):
    x_f32 = x_in.astype(F32)
    inv_rms = lax.rsqrt(jnp.mean(x_f32 * x_f32, axis=-1, keepdims=True) + EPSILON)
    return (x_f32 * inv_rms * gain.astype(F32)).astype(BF16)


class Place:
    def __init__(self, n_data, n_model, partner, neighbour):
        self.n_data, self.n_model = n_data, n_model
        self.y = lax.axis_index("data")
        self.me = lax.axis_index("model")
        self.up = lax.rem(self.y + 1, n_data)
        self.down = lax.rem(self.y + n_data - 1, n_data)
        self.far = lax.rem(self.y + 2, n_data)
        self.slots = (self.y, self.down, self.up, self.far)
        self.mate = self.me + 1 - 2 * lax.rem(self.me, 2)
        self.partner, self.neighbour = partner(self.me), neighbour(self.me)
        n_other = n_model // 2 - 1
        self.ahead = [lax.rem(self.me + 2 * k, n_model) for k in range(1, n_other + 1)]
        self.behind = [lax.rem(self.me + n_model - 2 * k, n_model) for k in range(1, n_other + 1)]

    def meet(self):
        barrier = pltpu.get_barrier_semaphore()
        targets = [{"data": self.up}, {"data": self.down}, {"data": self.far}, {"model": self.mate}]
        targets += [{"model": m} for m in self.ahead]
        for target in targets:
            pl.semaphore_signal(barrier, inc=1, device_id=target, device_id_type=MESH)
        pl.semaphore_wait(barrier, len(targets))


def remote(src, dst, send, recv, target):
    return pltpu.make_async_remote_copy(
        src_ref=src, dst_ref=dst, send_sem=send, recv_sem=recv, device_id=target, device_id_type=MESH
    )


class GatherIn:
    def __init__(self, place, buf, own, send, recv, local, first=None, column=None):
        self.place, self.buf, self.own, self.first, self.column = place, buf, own, first, column
        self.send, self.recv, self.local = send, recv, local

    def at(self, block, g, slot):
        return self.buf.at[block, g, slot]

    def _copy(self, src, dst, kind, at, target):
        return remote(src, dst, self.send.at[kind, at], self.recv.at[kind, at], target)

    def up(self, g, half):
        dst = self.at(0, g, self.place.y).at[half]
        return self._copy(self.own(g, half), dst, UP, 2 * g + half, {"data": self.place.up})

    def down(self, g, half):
        dst = self.at(0, g, self.place.y).at[half]
        return self._copy(self.own(g, half), dst, DOWN, 2 * g + half, {"data": self.place.down})

    def neighbour_first(self, g, half):
        dst = self.at(2, g, self.place.y).at[half]
        return self._copy(self.own(g, half), dst, FIRST, 2 * g + half, {"model": self.place.neighbour})

    def forward(self, g):
        even = lax.rem(g, 2) == 0
        ref = self.at(0, g, jnp.where(even, self.place.down, self.place.up))
        target = jnp.where(even, self.place.up, self.place.down)
        return self._copy(ref, ref, FORWARD, g, {"data": target})

    def _side(self, g):
        return self.at(2, g, self.place.y) if self.first is None else self.first.at[g]

    def side_up(self, g):
        return self._copy(self._side(g), self.at(2, g, self.place.y), SIDE_UP, g, {"data": self.place.up})

    def side_down(self, g):
        return self._copy(self._side(g), self.at(2, g, self.place.y), SIDE_DOWN, g, {"data": self.place.down})

    def far(self, g):
        slot = self.place.far
        src = self.at(0, g, slot) if self.column is None else self.column.at[g, slot]
        return self._copy(src, self.at(2, g, slot), FAR, g, {"model": self.place.neighbour})

    def mate(self, g):
        return self._copy(self.buf.at[0, g], self.buf.at[1, g], MATE, g, {"model": self.place.mate})

    def side_mate(self, g):
        return self._copy(self.buf.at[2, g], self.buf.at[3, g], SIDE_MATE, g, {"model": self.place.mate})

    def load_own(self, g, half):
        dst = self.at(0, g, self.place.y).at[half]
        return pltpu.make_async_copy(self.own(g, half), dst, self.local.at[half, g])

    def load_column(self, g, which):
        slot = self.place.slots[which]
        return pltpu.make_async_copy(self.column.at[g, slot], self.at(0, g, slot), self.local.at[1 + which, g])

    def load_first(self, g):
        return pltpu.make_async_copy(self.first.at[g], self.at(2, g, self.place.y), self.local.at[5, g])

    def pass_side(self, g):
        if self.first is not None:
            self.load_first(g).wait()
        self.side_up(g).wait_recv()
        self.side_down(g).wait_recv()
        self.far(g).wait_recv()
        self.side_mate(g).start()

    def wait_sends(self, g):
        made = [self.side_up(g), self.side_down(g), self.far(g), self.mate(g), self.side_mate(g)]
        if self.column is None:
            made += [self.forward(g)] + [copy(g, half) for copy in (self.up, self.down) for half in range(2)]
        if self.first is None:
            made += [self.neighbour_first(g, half) for half in range(2)]
        for copy in made:
            copy.wait_send()


class FetchIn:
    def __init__(self, place, own, send, recv, neighbour=None, first=None, column=None):
        self.place, self.own, self.send, self.recv = place, own, send, recv
        self.neighbour, self.first, self.column = neighbour, first, column

    def _ring(self, g, half, kind, target):
        at = 2 * g + half
        dst = self.column.at[g, self.place.y, half]
        return remote(self.own(g, half), dst, self.send.at[kind, at], self.recv.at[kind, at], {"data": target})

    def up(self, g, half):
        return self._ring(g, half, 0, self.place.up)

    def down(self, g, half):
        return self._ring(g, half, 1, self.place.down)

    def forward(self, g):
        even = lax.rem(g, 2) == 0
        ref = self.column.at[g, jnp.where(even, self.place.down, self.place.up)]
        target = jnp.where(even, self.place.up, self.place.down)
        return remote(ref, ref, self.send.at[2, g], self.recv.at[2, g], {"data": target})

    def neighbour_first(self, g, half):
        at = 2 * g + half
        dst = self.first.at[g, half]
        return remote(self.own(g, half), dst, self.send.at[3, at], self.recv.at[3, at], {"model": self.neighbour})


class GatherOut:
    def __init__(self, place, buf, own, send, recv, local=None, first=None, column=None):
        self.place, self.buf, self.own, self.first, self.column = place, buf, own, first, column
        self.send, self.recv, self.local = send, recv, local

    def _copy(self, src, dst, kind, target):
        return remote(src, dst, self.send.at[kind], self.recv.at[kind], target)

    def up(self):
        return self._copy(self.own, self.buf.at[0, self.place.y], UP, {"data": self.place.up})

    def down(self):
        return self._copy(self.own, self.buf.at[0, self.place.y], DOWN, {"data": self.place.down})

    def _half(self, ref, second):
        size = ref.shape[0] // 2
        return ref.at[pl.ds(second * size, size)]

    def forward(self):
        ref = self._half(self.buf.at[0, self.place.down], 0)
        return self._copy(ref, ref, FORWARD, {"data": self.place.up})

    def forward_b(self):
        ref = self._half(self.buf.at[0, self.place.up], 1)
        return self._copy(ref, ref, FORWARD_B, {"data": self.place.down})

    def neighbour_first(self, dst):
        return self._copy(self.own, dst, FIRST, {"model": self.place.neighbour})

    def side_up(self):
        return self._copy(self.first, self.buf.at[2, self.place.y], SIDE_UP, {"data": self.place.up})

    def side_down(self):
        return self._copy(self.first, self.buf.at[2, self.place.y], SIDE_DOWN, {"data": self.place.down})

    def far(self):
        slot = self.place.far
        src = self.buf.at[0, slot] if self.column is None else self.column.at[0, slot]
        return self._copy(src, self.buf.at[2, slot], FAR, {"model": self.place.neighbour})

    def mate(self, which):
        slot = self.place.slots[which]
        if which == 0:
            src = self.own
        else:
            src = self.buf.at[0, slot] if self.column is None else self.column.at[0, slot]
        return self._copy(src, self.buf.at[1, slot], MATE + 2 * which, {"model": self.place.mate})

    def side_mate(self, which):
        slot = self.place.slots[which]
        src = self.first if which == 0 else self.buf.at[2, slot]
        return self._copy(src, self.buf.at[3, slot], SIDE_MATE + 2 * which, {"model": self.place.mate})

    def load_own(self):
        return pltpu.make_async_copy(self.own, self.buf.at[0, self.place.y], self.local.at[0])

    def load_column(self, which):
        slot = self.place.slots[which]
        return pltpu.make_async_copy(self.column.at[0, slot], self.buf.at[0, slot], self.local.at[which])

    def load_first(self):
        return pltpu.make_async_copy(self.first, self.buf.at[2, self.place.y], self.local.at[4])


def in_halves(layer, head_ref, w_ref, c, ff):
    def own(g, half):
        if isinstance(g, int) and g == 0:
            return head_ref.at[layer, :, pl.ds(half * c, c)]
        return w_ref.at[layer, :, pl.ds(pl.multiple_of(g * c + half * ff, c), c)]

    return own


def project(layer, n_data, n_model, partner, neighbour, next_neighbour, x_own, head, w_in, w_out, extra):
    start_layer = layer == 0
    rows, d_model = x_own.shape
    part, two_c = head.shape[1:]
    c = two_c // 2
    depth, out_part = w_out.shape[1:]
    ff = depth - c
    n_group = 1 + ff // c
    n_units = 8 * n_group
    row_parts = 4
    row_part = rows // row_parts
    n_other = n_model // 2 - 1
    gain_shape = (n_data, 8, part)

    def kernel(*refs):
        x_ref, head_ref, w_ref, wo_ref = refs[:4]
        if start_layer:
            gain_ref = refs[4]
            q_ref, m_ref, kv_ref, gains_ref, out_first_ref, in_first_ref = refs[5:11]
            first_ref = column_ref = None
            rest = refs[11:]
        else:
            par_ref, gain_ref, first_ref, column_ref = refs[4:8]
            q_ref, m_ref, kv_ref, out_first_ref, out_column_ref = refs[8:13]
            rest = refs[13:]
        wbuf, h_ref, gbuf, stage, kv_stage, send, recv, w_local, next_send, next_recv, late_send, late_recv = rest[:12]
        x_send, x_recv, g_send, g_recv, kv_send, kv_recv, local, out_sem = rest[12:]

        place = Place(n_data, n_model, partner, neighbour)
        place.meet()
        w = GatherIn(place, wbuf, in_halves(layer, head_ref, w_ref, c, ff), send, recv, w_local, first_ref, column_ref)
        out_column = None if start_layer else out_column_ref
        out_next = GatherOut(place, out_column, wo_ref.at[layer], next_send, next_recv)
        if start_layer:
            in_own = in_halves(layer + 1, head_ref, w_ref, c, ff)
            in_next = FetchIn(place, in_own, late_send, late_recv, next_neighbour(place.me), in_first_ref)

        def c_x(part_no):
            piece = pl.ds(part_no * row_part, row_part)
            return remote(
                x_ref.at[piece], h_ref.at[1, piece], x_send.at[part_no], x_recv.at[part_no], {"model": place.partner}
            )

        def c_gain(which):
            target = {"data": (place.up, place.down, place.far)[which]}
            return remote(gain_ref, gbuf.at[place.y], g_send.at[which], g_recv.at[which], target)

        def c_kv(which):
            ref = kv_ref.at[place.me]
            return remote(ref, ref, kv_send.at[which], kv_recv.at[which], {"model": place.ahead[which]})

        def c_kv_mate(which):
            ref = kv_ref.at[place.me if which == 0 else place.behind[which - 1]]
            at = n_other + which
            return remote(ref, ref, kv_send.at[at], kv_recv.at[at], {"model": place.mate})

        save_kv = pltpu.make_async_copy(kv_stage, kv_ref.at[place.me], local.at[0])
        load_x = pltpu.make_async_copy(x_ref, h_ref.at[0], local.at[0])

        if start_layer:
            load_gain = pltpu.make_async_copy(gain_ref, gbuf.at[place.y], local.at[1])
            for which in range(3):
                c_gain(which).start()
        else:
            load_gain = pltpu.make_async_copy(gain_ref, gbuf, local.at[1])
            load_par = pltpu.make_async_copy(par_ref, h_ref.at[1], local.at[2])
        load_gain.start()
        load_x.start()
        if start_layer:
            for g in range(2):
                for half in range(2):
                    w.up(g, half).start()
                    w.down(g, half).start()
            for g in range(n_group):
                for half in range(2):
                    w.neighbour_first(g, half).start()
                    w.load_own(g, half).start()
            for part_no in range(row_parts):
                c_x(part_no).start()
        else:
            load_par.start()
            for g in range(n_group):
                for half in range(2):
                    w.load_own(g, half).start()
                for which in range(1, 4):
                    w.load_column(g, which).start()
                w.side_up(g).start()
                w.side_down(g).start()
                w.far(g).start()
            for g in range(n_group):
                w.load_first(g).start()
            out_next.neighbour_first(out_first_ref).start()
            out_next.up().start()
            out_next.down().start()

        def ring_stage(g):
            for half in range(2):
                w.up(g, half).wait_recv()
                w.down(g, half).wait_recv()
            w.forward(g).start()

            @pl.when(g + 2 < n_group)
            def _():
                for half in range(2):
                    w.up(g + 2, half).start()
                    w.down(g + 2, half).start()

        if start_layer:
            for which in range(3):
                c_gain(which).wait_recv()
        load_gain.wait()
        gain = jnp.concatenate([gbuf[k, layer:layer + 1, :] for k in range(n_data)], axis=1)
        if start_layer:
            save_gain = pltpu.make_async_copy(gbuf, gains_ref, local.at[1])
            save_gain.start()
        load_x.wait()

        def norm_rows(side, part_no):
            piece = pl.ds(part_no * row_part, row_part)
            h_ref[side, piece] = rms_norm(h_ref[side, piece], gain)

        @pl.loop(0, row_parts)
        def _(part_no):
            norm_rows(0, part_no)

        if start_layer:
            ring_stage(0)
        else:
            for g in range(n_group):
                for half in range(2):
                    w.load_own(g, half).wait()
                for which in range(1, 4):
                    w.load_column(g, which).wait()
                w.mate(g).start()
            load_par.wait()

            @pl.loop(0, row_parts)
            def _(part_no):
                norm_rows(1, part_no)

        halfway, quarter = n_units // 2, n_units // 4

        def out_copy(slot, blk, side, g):
            def to_q():
                return pltpu.make_async_copy(stage.at[slot], q_ref.at[blk, side], out_sem.at[slot])

            def to_m():
                column = pl.ds(pl.multiple_of((g - 1) * c, c), c)
                return pltpu.make_async_copy(stage.at[slot], m_ref.at[blk, side, :, column], out_sem.at[slot])

            return to_q, to_m

        @pl.loop(0, n_units)
        def _(step):
            late = step - halfway
            if start_layer:
                opening, second = step < quarter, (step >= quarter) & (step < halfway)
                g = jnp.where(opening, step // 2, jnp.where(second, (step - quarter) // 2, late // 4))
                blk = jnp.where(step < halfway, lax.rem(step, 2), 2 + lax.rem(late, 4) // 2)
                side = jnp.where(opening, 0, jnp.where(second, 1, lax.rem(late, 2)))

                @pl.when(opening & (blk == 0))
                def _():
                    @pl.when(g + 1 < n_group)
                    def _():
                        ring_stage(g + 1)

                    @pl.when(g + 2 == n_group)
                    def _():
                        @pl.loop(0, n_group)
                        def _(k):
                            for half in range(2):
                                w.neighbour_first(k, half).wait_recv()
                            w.side_up(k).start()
                            w.side_down(k).start()

                    w.forward(g).wait_recv()
                    w.far(g).start()
                    for half in range(2):
                        w.load_own(g, half).wait()
                    w.mate(g).start()

                @pl.when(opening & (blk == 1))
                def _():
                    w.mate(g).wait_recv()

                @pl.when(step == quarter)
                def _():
                    @pl.loop(0, row_parts)
                    def _(part_no):
                        c_x(part_no).wait_recv()
                        norm_rows(1, part_no)

                    out_next.neighbour_first(out_first_ref).start()
                    for k in range(n_group):
                        for half in range(2):
                            in_next.neighbour_first(k, half).start()
            else:
                g = jnp.where(late < 0, step, late) // 4
                blk = jnp.where(late < 0, 0, 2) + lax.rem(step, 4) // 2
                side = lax.rem(step, 2)

                @pl.when((late < 0) & (lax.rem(step, 4) == 2))
                def _():
                    w.mate(g).wait_recv()

                @pl.when(step == n_units - 6)
                def _():
                    out_next.up().wait_recv()
                    out_next.down().wait_recv()
                    out_next.forward().start()
                    out_next.forward_b().start()

            @pl.when(step == halfway - 2)
            def _():
                w.pass_side(0)

            @pl.when((late >= 0) & (lax.rem(late, 4) == 2))
            def _():
                @pl.when(g + 1 < n_group)
                def _():
                    w.pass_side(g + 1)

                w.side_mate(g).wait_recv()

            slot = lax.rem(step, 2)
            to_q, to_m = out_copy(slot, blk, side, g)

            @pl.when(step >= 2)
            def _():
                to_q().wait()

            def columns(half):
                return wbuf[blk, g, :, half].reshape(d_model, c)

            @pl.when(g == 0)
            def _():
                q = jnp.dot(h_ref[side], columns(0), preferred_element_type=F32)
                stage[slot] = q.astype(BF16)
                to_q().start()

            @pl.when(g > 0)
            def _():
                h_val = h_ref[side]
                gate = jnp.dot(h_val, columns(0), preferred_element_type=F32).astype(BF16).astype(F32)
                raised = jnp.dot(h_val, columns(1), preferred_element_type=F32).astype(BF16).astype(F32)
                stage[slot] = (gate * jax.nn.sigmoid(gate) * raised).astype(BF16)
                to_m().start()

            @pl.when(step == 0)
            def _():
                kv_stage[...] = jnp.dot(h_ref[0], columns(1), preferred_element_type=F32).astype(BF16)
                save_kv.start()

            @pl.when(step == 1)
            def _():
                save_kv.wait()
                for which in range(n_other):
                    c_kv(which).start()
                c_kv_mate(0).start()

            @pl.when(step == quarter)
            def _():
                for which in range(n_other):
                    c_kv(which).wait_recv()
                    c_kv_mate(1 + which).start()

        for which in range(n_other + 1):
            c_kv_mate(which).wait()
        for which in range(n_other):
            c_kv(which).wait_send()
        if start_layer:
            save_gain.wait()
            for which in range(3):
                c_gain(which).wait_send()
            for part_no in range(row_parts):
                c_x(part_no).wait_send()
            for g in range(n_group):
                for half in range(2):
                    in_next.neighbour_first(g, half).wait()
        else:
            for copy in (out_next.forward(), out_next.forward_b()):
                copy.wait()
            for copy in (out_next.up(), out_next.down()):
                copy.wait_send()
        out_next.neighbour_first(out_first_ref).wait()
        for slot in range(2):
            pltpu.make_async_copy(stage.at[slot], q_ref.at[0, 0], out_sem.at[slot]).wait()

        @pl.loop(0, n_group)
        def _(g):
            w.wait_sends(g)

    anywhere = pl.BlockSpec(memory_space=pl.ANY)
    out_shape = [
        jax.ShapeDtypeStruct((4, 2, rows, c), BF16),
        jax.ShapeDtypeStruct((4, 2, rows, ff), BF16),
        jax.ShapeDtypeStruct((n_model, rows, c), BF16),
    ]
    if start_layer:
        out_shape += [
            jax.ShapeDtypeStruct(gain_shape, F32),
            jax.ShapeDtypeStruct((depth, out_part), BF16),
            jax.ShapeDtypeStruct((n_group, 2, part, c), BF16),
        ]
    else:
        out_shape += [
            jax.ShapeDtypeStruct((depth, out_part), BF16),
            jax.ShapeDtypeStruct((1, n_data, depth, out_part), BF16),
        ]
    dma = pltpu.SemaphoreType.DMA
    args = (x_own, head, w_in, w_out) + tuple(extra)
    return pl.pallas_call(
        kernel,
        out_shape=out_shape,
        in_specs=[anywhere] * len(args),
        out_specs=[anywhere] * len(out_shape),
        scratch_shapes=[
            pltpu.VMEM((4, n_group, n_data, 2, part, c), BF16),
            pltpu.VMEM((2, rows, d_model), BF16),
            pltpu.VMEM(gain_shape, F32),
            pltpu.VMEM((2, rows, c), BF16),
            pltpu.VMEM((rows, c), BF16),
            dma((SIDE_MATE + 1, 2 * n_group)), dma((SIDE_MATE + 1, 2 * n_group)), dma((6, n_group)),
            dma((FIRST + 1,)), dma((FIRST + 1,)), dma((4, 2 * n_group)), dma((4, 2 * n_group)),
            dma((row_parts,)), dma((row_parts,)), dma((3,)), dma((3,)),
            dma((n_model - 1,)), dma((n_model - 1,)), dma((3,)), dma((2,)),
        ],
        compiler_params=pltpu.CompilerParams(collective_id=2 * layer, has_side_effects=True, vmem_limit_bytes=VMEM_LIMIT),
        cost_estimate=pl.CostEstimate(flops=4 * rows * d_model * 4 * (c + 2 * ff), bytes_accessed=16 * rows * d_model, transcendentals=0),
        name=f"project_{layer}",
    )(*args)


def attend_and_sum(layer, last, n_data, n_model, partner, neighbour, next_partner, lens, q, m, kv, x_own, w_in, w_out, head, first, column):
    n_blocks, _, rows, c = q.shape
    ff = m.shape[3]
    d_model = x_own.shape[1]
    depth, out_part = w_out.shape[1:]
    head_dim = c // 2
    n_batch = lens.shape[0]
    slab_len = rows // n_batch
    chunks = 4
    n_seq = n_batch // chunks
    crow = rows // chunks
    tiles = chunks * n_data
    heads = n_blocks * 2
    qrows = heads * slab_len
    key_rows = 2 * slab_len
    scale = head_dim ** -0.5 * 1.4426950408889634
    part = head.shape[1]
    n_group = 1 + ff // c
    ready = column is not None
    held = tiles // 2

    def kernel(*refs):
        lens_ref, q_ref, m_ref, kv_ref, x_ref, wo_ref, first_ref = refs[:7]
        at = 7
        column_ref = None
        if ready:
            column_ref = refs[at]
            at += 1
        if not last:
            head_ref, wi_ref = refs[at:at + 2]
            at += 2
        y_ref = refs[at]
        at += 1
        if not last:
            par_ref, in_column_ref = refs[at:at + 2]
            at += 2
        (wbuf, obuf, kvb, mbuf, xb, zb, zr, z_stage, s_ref, mx_ref, sum_ref, acc_ref,
         send, recv, w_local, in_send, in_recv, z_send, z_recv, y_send, y_recv, y_save, x_sem, m_sem, local) = refs[at:]

        place = Place(n_data, n_model, partner, neighbour)
        place.meet()
        w = GatherOut(place, wbuf, wo_ref.at[layer], send, recv, w_local, first_ref, column_ref)

        def tile_of(k):
            which = k // chunks
            slot = jnp.where(which == 0, place.y, jnp.where(which == 1, place.down, jnp.where(which == 2, place.up, place.far)))
            return lax.rem(k, chunks), which, slot

        def whole(ref, chunk, slot):
            return ref.at[pl.ds(pl.multiple_of(chunk * crow, crow), crow), pl.ds(pl.multiple_of(slot * out_part, out_part), out_part)]

        load_q = pltpu.make_async_copy(q_ref, obuf, local.at[0])
        load_kv = pltpu.make_async_copy(kv_ref, kvb, local.at[1])

        def load_m(k):
            chunk, _, _ = tile_of(k)
            slot = lax.rem(k, 2)
            return pltpu.make_async_copy(
                m_ref.at[:, :, pl.ds(pl.multiple_of(chunk * crow, crow), crow)], mbuf.at[slot], m_sem.at[slot]
            )

        def load_x(k):
            chunk, _, slot = tile_of(k)
            return pltpu.make_async_copy(whole(x_ref, chunk, slot), xb.at[chunk, slot], x_sem.at[k])

        def c_z(k):
            chunk, _, slot = tile_of(k)
            return remote(z_stage.at[lax.rem(k, 4)], zr.at[chunk, slot], z_send.at[k], z_recv.at[k], {"model": place.partner})

        def c_y(k):
            chunk, _, slot = tile_of(k)
            target = {"model": next_partner(place.me)}
            return remote(xb.at[chunk, slot], whole(par_ref, chunk, slot), y_send.at[k], y_recv.at[k], target)

        def save_y(k):
            chunk, _, slot = tile_of(k)
            return pltpu.make_async_copy(xb.at[chunk, slot], whole(y_ref, chunk, slot), y_save.at[k])

        load_q.start()
        load_kv.start()
        load_m(0).start()
        w.load_own().start()
        w.load_first().start()
        w.mate(0).start()
        w.side_mate(0).start()
        if ready:
            w.far().start()
            for which in range(1, 4):
                w.load_column(which).start()
                w.mate(which).start()
        else:
            w.up().start()
            w.down().start()
        w.side_up().start()
        w.side_down().start()
        if not last:
            in_own = in_halves(layer + 1, head_ref, wi_ref, c, ff)
            in_next = FetchIn(place, in_own, in_send, in_recv, column=in_column_ref)

        @pl.loop(0, tiles)
        def _(k):
            load_x(k).start()

        load_q.wait()
        load_kv.wait()

        def attend_one(batch, side):
            slab = jnp.where(side == 0, place.me, place.partner)
            length = lens_ref[batch]
            n_key = slab // 2 + 1
            at_row = pl.ds(pl.multiple_of(batch * slab_len, slab_len), slab_len)
            parts = []
            for blk in range(n_blocks):
                for one in range(2):
                    parts.append(obuf[blk, side, at_row, one * head_dim:(one + 1) * head_dim])
            q_val = jnp.concatenate(parts, axis=0)
            row_pos = slab * slab_len + lax.rem(lax.broadcasted_iota(jnp.int32, (qrows, key_rows), 0), slab_len)
            key_pos = lax.broadcasted_iota(jnp.int32, (qrows, key_rows), 1)
            room = jnp.minimum(row_pos + 1, length) - key_pos
            mx_ref[...] = jnp.full_like(mx_ref, -1e30)

            def score(kb, carry):
                k = kvb[pl.ds(2 * kb, 2), at_row, :head_dim].reshape(key_rows, head_dim)
                s = lax.dot_general(q_val, k, (((1,), (1,)), ((), ())), preferred_element_type=F32) * scale
                s = jnp.where(room > kb * key_rows, s, -1e30)
                s_ref[kb] = s
                mx_ref[...] = jnp.maximum(mx_ref[...], jnp.maximum(s[:, :slab_len], s[:, slab_len:]))
                return carry

            lax.fori_loop(0, n_key, score, 0)
            top = jnp.max(mx_ref[...], axis=-1, keepdims=True)
            mx_ref[...] = jnp.broadcast_to(top, mx_ref.shape)
            sum_ref[...] = jnp.zeros_like(sum_ref)
            acc_ref[...] = jnp.zeros_like(acc_ref)

            def weigh(kb, carry):
                v = kvb[pl.ds(2 * kb, 2), at_row, head_dim:].reshape(key_rows, head_dim)
                top_b = mx_ref[...]
                e_lo = jnp.exp2(s_ref[kb, :, :slab_len] - top_b)
                e_hi = jnp.exp2(s_ref[kb, :, slab_len:] - top_b)
                sum_ref[...] += e_lo + e_hi
                e = jnp.concatenate([e_lo, e_hi], axis=1).astype(BF16)
                acc_ref[...] += jnp.dot(e, v, preferred_element_type=F32)
                return carry

            lax.fori_loop(0, n_key, weigh, 0)
            out = (acc_ref[...] / jnp.sum(sum_ref[...], axis=-1, keepdims=True)).astype(BF16)
            for blk in range(n_blocks):
                for one in range(2):
                    first_row = (blk * 2 + one) * slab_len
                    obuf[blk, side, at_row, one * head_dim:(one + 1) * head_dim] = out[first_row:first_row + slab_len]

        def settle(k):
            chunk, _, slot = tile_of(k)
            load_x(k).wait()
            c_z(k).wait_recv()
            z = zb[chunk, slot].astype(F32) + zr[chunk, slot].astype(F32)
            xb[chunk, slot] = (xb[chunk, slot].astype(F32) + z).astype(BF16)
            save_y(k).start()
            if not last:
                c_y(k).start()

        @pl.loop(0, tiles)
        def _(step):
            chunk, which, slot = tile_of(step)

            @pl.when(step + 1 < tiles)
            def _():
                load_m(step + 1).start()

            @pl.when(step < chunks)
            def _():
                @pl.loop(0, 2 * n_seq)
                def _(unit):
                    attend_one(step * n_seq + unit // 2, lax.rem(unit, 2))

            @pl.when(step == 0)
            def _():
                w.load_own().wait()
                w.load_first().wait()
                w.mate(0).wait_recv()
                w.side_mate(0).wait_recv()

            if not ready:

                @pl.when(step == 2)
                def _():
                    w.up().wait_recv()
                    w.down().wait_recv()
                    w.forward().start()
                    w.forward_b().start()
                    w.mate(1).start()
                    w.mate(2).start()
                    if not last:
                        for g in range(2):
                            for half in range(2):
                                in_next.up(g, half).start()
                                in_next.down(g, half).start()

                @pl.when(step == chunks + 2)
                def _():
                    w.forward().wait_recv()
                    w.forward_b().wait_recv()
                    w.far().start()
                    w.mate(3).start()

            @pl.when(step == chunks)
            def _():
                w.side_up().wait_recv()
                w.side_mate(1).start()
                w.side_down().wait_recv()
                w.side_mate(2).start()
                for one in (1, 2):
                    if ready:
                        w.load_column(one).wait()
                    w.mate(one).wait_recv()
                    w.side_mate(one).wait_recv()

            @pl.when(step == 3 * chunks)
            def _():
                w.far().wait_recv()
                w.side_mate(3).start()
                if ready:
                    w.load_column(3).wait()
                w.mate(3).wait_recv()
                w.side_mate(3).wait_recv()

            if not last:
                @pl.when((step >= chunks + 3) & (lax.rem(step, 2) == 1))
                def _():
                    g = (step - chunks - 3) // 2

                    @pl.when(g < n_group - 2)
                    def _():
                        for half in range(2):
                            in_next.up(g + 2, half).start()
                            in_next.down(g + 2, half).start()

            @pl.when(step >= 4)
            def _():
                c_z(step - 4).wait_send()

            load_m(step).wait()
            here = lax.rem(step, 2)
            rows_c = pl.ds(pl.multiple_of(chunk * crow, crow), crow)
            total = None
            for blk in range(n_blocks):
                mid = mbuf[here, blk].reshape(2 * crow, ff)
                attn = obuf[blk, :, rows_c, :].reshape(2 * crow, c)
                one = jnp.dot(mid, wbuf[blk, slot, c:, :], preferred_element_type=F32)
                one = one + jnp.dot(attn, wbuf[blk, slot, :c, :], preferred_element_type=F32)
                total = one if total is None else total + one
            z = total.astype(BF16)
            zb[chunk, slot] = z[:crow]
            z_stage[lax.rem(step, 4)] = z[crow:]
            c_z(step).start()

            early = (step >= 1) & (step <= chunks)
            paced = (step >= 2 * chunks) & (lax.rem(step, 2) == 0)

            @pl.when(early | paced)
            def _():
                settle(jnp.where(early, step - 1, step // 2))

        if not last:

            @pl.loop(0, n_group)
            def _(g):
                for half in range(2):
                    in_next.up(g, half).wait_recv()
                    in_next.down(g, half).wait_recv()
                in_next.forward(g).start()

        @pl.loop(held, tiles)
        def _(k):
            settle(k)

        @pl.loop(0, tiles)
        def _(k):
            save_y(k).wait()
            if not last:
                c_y(k).wait()

        @pl.loop(tiles - 4, tiles)
        def _(k):
            c_z(k).wait_send()

        made = [w.side_up(), w.side_down(), w.far()]
        made += [w.mate(which) for which in range(4)] + [w.side_mate(which) for which in range(4)]
        if not ready:
            made += [w.up(), w.down(), w.forward(), w.forward_b()]
        for copy in made:
            copy.wait_send()
        if not last:

            @pl.loop(0, n_group)
            def _(g):
                in_next.forward(g).wait()
                for half in range(2):
                    in_next.up(g, half).wait_send()
                    in_next.down(g, half).wait_send()

    anywhere = pl.BlockSpec(memory_space=pl.ANY)
    args = [lens, q, m, kv, x_own, w_out, first]
    if ready:
        args.append(column)
    if not last:
        args += [head, w_in]
    out_shape = [jax.ShapeDtypeStruct((rows, d_model), BF16)]
    if not last:
        out_shape += [
            jax.ShapeDtypeStruct((rows, d_model), BF16),
            jax.ShapeDtypeStruct((n_group, n_data, 2, part, c), BF16),
        ]
    dma = pltpu.SemaphoreType.DMA
    tile = (chunks, n_data, crow, out_part)
    return pl.pallas_call(
        kernel,
        out_shape=out_shape,
        in_specs=[pl.BlockSpec(memory_space=pltpu.SMEM)] + [anywhere] * (len(args) - 1),
        out_specs=[anywhere] * len(out_shape),
        scratch_shapes=[
            pltpu.VMEM((n_blocks, n_data, depth, out_part), BF16),
            pltpu.VMEM(q.shape, BF16),
            pltpu.VMEM(kv.shape, BF16),
            pltpu.VMEM((2, n_blocks, 2, crow, ff), BF16),
            pltpu.VMEM(tile, BF16),
            pltpu.VMEM(tile, BF16),
            pltpu.VMEM(tile, BF16),
            pltpu.VMEM((4, crow, out_part), BF16),
            pltpu.VMEM((n_model // 2, qrows, key_rows), F32),
            pltpu.VMEM((qrows, slab_len), F32),
            pltpu.VMEM((qrows, slab_len), F32),
            pltpu.VMEM((qrows, head_dim), F32),
            dma((SIDE_MATE + 7,)), dma((SIDE_MATE + 7,)), dma((5,)), dma((3, 2 * n_group)), dma((3, 2 * n_group)),
            dma((tiles,)), dma((tiles,)), dma((tiles,)), dma((tiles,)), dma((tiles,)), dma((tiles,)), dma((2,)), dma((2,)),
        ],
        compiler_params=pltpu.CompilerParams(collective_id=2 * layer + 1, has_side_effects=True, vmem_limit_bytes=VMEM_LIMIT),
        cost_estimate=pl.CostEstimate(flops=4 * rows * n_blocks * depth * d_model, bytes_accessed=16 * rows * d_model, transcendentals=0),
        name=f"attend_and_sum_{layer}",
    )(*args)


def solution(mesh):
    batch_axes = ("rep", "data")
    n_data, n_model = mesh.shape["data"], mesh.shape["model"]
    n_chip = n_model // 2

    def near(x):
        return x + 1 - 2 * (x % 2)

    def across(x):
        return n_chip - 1 - x

    def on_chip(other):
        return lambda m: 2 * other(m // 2) + m % 2

    def local_step(x_loc, lens_loc, gamma_loc, w_in_loc, w_kv_loc, w_out_loc):
        n_batch, slab_len, d_model = x_loc.shape
        n_layers, part = gamma_loc.shape
        attn_cols = w_kv_loc.shape[2]
        partners = [on_chip(near if layer % 2 == 0 else across) for layer in range(n_layers)]
        neighbours = [on_chip(across if layer % 2 == 0 else near) for layer in range(n_layers)]

        head = jnp.concatenate([w_in_loc[:, :, :attn_cols], w_kv_loc], axis=2)
        gain_rows = jnp.zeros((8, part), F32).at[:n_layers].set(gamma_loc.astype(F32))
        own = x_loc.reshape(n_batch * slab_len, d_model)
        for layer in range(n_layers):
            last = layer + 1 == n_layers
            following = min(layer + 1, n_layers - 1)
            if layer == 0:
                extra = (gain_rows,)
                q, m, kv, gains, out_first, in_first = project(
                    layer, n_data, n_model, partners[layer], neighbours[layer], neighbours[following],
                    own, head, w_in_loc, w_out_loc, extra,
                )
                out_column = None
            else:
                extra = (other, gains, in_first, in_column)
                q, m, kv, out_first, out_column = project(
                    layer, n_data, n_model, partners[layer], neighbours[layer], neighbours[following],
                    own, head, w_in_loc, w_out_loc, extra,
                )
            outs = attend_and_sum(
                layer, last, n_data, n_model, partners[layer], neighbours[layer], partners[following],
                lens_loc, q, m, kv, own, w_in_loc, w_out_loc, head, out_first, out_column,
            )
            own = outs[0]
            if not last:
                other, in_column = outs[1:]
        return own.reshape(n_batch, slab_len, d_model)

    in_specs = (
        P(batch_axes, "model", None),
        P(batch_axes),
        P(None, "data"),
        P(None, "data", "model"),
        P(None, "data", None),
        P(None, "model", "data"),
    )
    return jax.shard_map(local_step, mesh=mesh, in_specs=in_specs, out_specs=P(batch_axes, "model", None), check_vma=False)
```

```python
import functools

import jax
import jax.numpy as jnp
from jax import lax
from jax.experimental import pallas as pl
from jax.experimental.pallas import tpu as pltpu
from jax.sharding import PartitionSpec as P

EPSILON = 1e-6
VMEM_LIMIT = 66_000_000
MESH = pl.DeviceIdType.MESH
BF16, F32 = jnp.bfloat16, jnp.float32

UP, DOWN, FORWARD, FORWARD_B, FIRST, SIDE_UP, SIDE_DOWN, FAR, MATE, SIDE_MATE = range(10)


def rms_norm(x_in, gain):
    x_f32 = x_in.astype(F32)
    inv_rms = lax.rsqrt(jnp.mean(x_f32 * x_f32, axis=-1, keepdims=True) + EPSILON)
    return (x_f32 * inv_rms * gain.astype(F32)).astype(BF16)


class Place:
    def __init__(self, n_data, n_model, partner, neighbour):
        self.n_data, self.n_model = n_data, n_model
        self.y = lax.axis_index("data")
        self.me = lax.axis_index("model")
        self.up = lax.rem(self.y + 1, n_data)
        self.down = lax.rem(self.y + n_data - 1, n_data)
        self.far = lax.rem(self.y + 2, n_data)
        self.slots = (self.y, self.down, self.up, self.far)
        self.mate = self.me + 1 - 2 * lax.rem(self.me, 2)
        self.partner, self.neighbour = partner(self.me), neighbour(self.me)
        n_other = n_model // 2 - 1
        self.ahead = [lax.rem(self.me + 2 * k, n_model) for k in range(1, n_other + 1)]
        self.behind = [lax.rem(self.me + n_model - 2 * k, n_model) for k in range(1, n_other + 1)]

    def meet(self):
        barrier = pltpu.get_barrier_semaphore()
        targets = [{"data": self.up}, {"data": self.down}, {"data": self.far}, {"model": self.mate}]
        targets += [{"model": m} for m in self.ahead]
        for target in targets:
            pl.semaphore_signal(barrier, inc=1, device_id=target, device_id_type=MESH)
        pl.semaphore_wait(barrier, len(targets))


def remote(src, dst, send, recv, target):
    return pltpu.make_async_remote_copy(
        src_ref=src, dst_ref=dst, send_sem=send, recv_sem=recv, device_id=target, device_id_type=MESH
    )


class GatherIn:
    def __init__(self, place, buf, own, send, recv, local, first=None, column=None):
        self.place, self.buf, self.own, self.first, self.column = place, buf, own, first, column
        self.send, self.recv, self.local = send, recv, local

    def at(self, block, g, slot):
        return self.buf.at[block, g, slot]

    def _copy(self, src, dst, kind, at, target):
        return remote(src, dst, self.send.at[kind, at], self.recv.at[kind, at], target)

    def up(self, g, half):
        dst = self.at(0, g, self.place.y).at[half]
        return self._copy(self.own(g, half), dst, UP, 2 * g + half, {"data": self.place.up})

    def down(self, g, half):
        dst = self.at(0, g, self.place.y).at[half]
        return self._copy(self.own(g, half), dst, DOWN, 2 * g + half, {"data": self.place.down})

    def neighbour_first(self, g, half):
        dst = self.at(2, g, self.place.y).at[half]
        return self._copy(self.own(g, half), dst, FIRST, 2 * g + half, {"model": self.place.neighbour})

    def forward(self, g):
        even = lax.rem(g, 2) == 0
        ref = self.at(0, g, jnp.where(even, self.place.down, self.place.up))
        target = jnp.where(even, self.place.up, self.place.down)
        return self._copy(ref, ref, FORWARD, g, {"data": target})

    def _side(self, g):
        return self.at(2, g, self.place.y) if self.first is None else self.first.at[g]

    def side_up(self, g):
        return self._copy(self._side(g), self.at(2, g, self.place.y), SIDE_UP, g, {"data": self.place.up})

    def side_down(self, g):
        return self._copy(self._side(g), self.at(2, g, self.place.y), SIDE_DOWN, g, {"data": self.place.down})

    def far(self, g):
        slot = self.place.far
        src = self.at(0, g, slot) if self.column is None else self.column.at[g, slot]
        return self._copy(src, self.at(2, g, slot), FAR, g, {"model": self.place.neighbour})

    def mate(self, g):
        return self._copy(self.buf.at[0, g], self.buf.at[1, g], MATE, g, {"model": self.place.mate})

    def side_mate(self, g):
        return self._copy(self.buf.at[2, g], self.buf.at[3, g], SIDE_MATE, g, {"model": self.place.mate})

    def load_own(self, g, half):
        dst = self.at(0, g, self.place.y).at[half]
        return pltpu.make_async_copy(self.own(g, half), dst, self.local.at[half, g])

    def load_column(self, g, which):
        slot = self.place.slots[which]
        return pltpu.make_async_copy(self.column.at[g, slot], self.at(0, g, slot), self.local.at[1 + which, g])

    def load_first(self, g):
        return pltpu.make_async_copy(self.first.at[g], self.at(2, g, self.place.y), self.local.at[5, g])

    def pass_side(self, g):
        if self.first is not None:
            self.load_first(g).wait()
        self.side_up(g).wait_recv()
        self.side_down(g).wait_recv()
        self.far(g).wait_recv()
        self.side_mate(g).start()

    def wait_sends(self, g):
        made = [self.side_up(g), self.side_down(g), self.far(g), self.mate(g), self.side_mate(g)]
        if self.column is None:
            made += [self.forward(g)] + [copy(g, half) for copy in (self.up, self.down) for half in range(2)]
        if self.first is None:
            made += [self.neighbour_first(g, half) for half in range(2)]
        for copy in made:
            copy.wait_send()


class FetchIn:
    def __init__(self, place, own, send, recv, neighbour=None, first=None, column=None):
        self.place, self.own, self.send, self.recv = place, own, send, recv
        self.neighbour, self.first, self.column = neighbour, first, column

    def _ring(self, g, half, kind, target):
        at = 2 * g + half
        dst = self.column.at[g, self.place.y, half]
        return remote(self.own(g, half), dst, self.send.at[kind, at], self.recv.at[kind, at], {"data": target})

    def up(self, g, half):
        return self._ring(g, half, 0, self.place.up)

    def down(self, g, half):
        return self._ring(g, half, 1, self.place.down)

    def forward(self, g):
        even = lax.rem(g, 2) == 0
        ref = self.column.at[g, jnp.where(even, self.place.down, self.place.up)]
        target = jnp.where(even, self.place.up, self.place.down)
        return remote(ref, ref, self.send.at[2, g], self.recv.at[2, g], {"data": target})

    def neighbour_first(self, g, half):
        at = 2 * g + half
        dst = self.first.at[g, half]
        return remote(self.own(g, half), dst, self.send.at[3, at], self.recv.at[3, at], {"model": self.neighbour})


class GatherOut:
    def __init__(self, place, buf, own, send, recv, local=None, first=None, column=None):
        self.place, self.buf, self.own, self.first, self.column = place, buf, own, first, column
        self.send, self.recv, self.local = send, recv, local

    def _copy(self, src, dst, kind, target):
        return remote(src, dst, self.send.at[kind], self.recv.at[kind], target)

    def up(self):
        return self._copy(self.own, self.buf.at[0, self.place.y], UP, {"data": self.place.up})

    def down(self):
        return self._copy(self.own, self.buf.at[0, self.place.y], DOWN, {"data": self.place.down})

    def _half(self, ref, second):
        size = ref.shape[0] // 2
        return ref.at[pl.ds(second * size, size)]

    def forward(self):
        ref = self._half(self.buf.at[0, self.place.down], 0)
        return self._copy(ref, ref, FORWARD, {"data": self.place.up})

    def forward_b(self):
        ref = self._half(self.buf.at[0, self.place.up], 1)
        return self._copy(ref, ref, FORWARD_B, {"data": self.place.down})

    def neighbour_first(self, dst):
        return self._copy(self.own, dst, FIRST, {"model": self.place.neighbour})

    def side_up(self):
        return self._copy(self.first, self.buf.at[2, self.place.y], SIDE_UP, {"data": self.place.up})

    def side_down(self):
        return self._copy(self.first, self.buf.at[2, self.place.y], SIDE_DOWN, {"data": self.place.down})

    def far(self):
        slot = self.place.far
        src = self.buf.at[0, slot] if self.column is None else self.column.at[0, slot]
        return self._copy(src, self.buf.at[2, slot], FAR, {"model": self.place.neighbour})

    def mate(self, which):
        slot = self.place.slots[which]
        if which == 0:
            src = self.own
        else:
            src = self.buf.at[0, slot] if self.column is None else self.column.at[0, slot]
        return self._copy(src, self.buf.at[1, slot], MATE + 2 * which, {"model": self.place.mate})

    def side_mate(self, which):
        slot = self.place.slots[which]
        src = self.first if which == 0 else self.buf.at[2, slot]
        return self._copy(src, self.buf.at[3, slot], SIDE_MATE + 2 * which, {"model": self.place.mate})

    def load_own(self):
        return pltpu.make_async_copy(self.own, self.buf.at[0, self.place.y], self.local.at[0])

    def load_column(self, which):
        slot = self.place.slots[which]
        return pltpu.make_async_copy(self.column.at[0, slot], self.buf.at[0, slot], self.local.at[which])

    def load_first(self):
        return pltpu.make_async_copy(self.first, self.buf.at[2, self.place.y], self.local.at[4])


def in_halves(layer, head_ref, w_ref, c, ff):
    def own(g, half):
        if isinstance(g, int) and g == 0:
            return head_ref.at[layer, :, pl.ds(half * c, c)]
        return w_ref.at[layer, :, pl.ds(pl.multiple_of(g * c + half * ff, c), c)]

    return own


def project(layer, n_data, n_model, partner, neighbour, next_neighbour, x_own, head, w_in, w_out, extra):
    start_layer = layer == 0
    part, two_c = head.shape[1:]
    d_model = part * n_data
    rows = x_own.size // d_model
    c = two_c // 2
    depth, out_part = w_out.shape[1:]
    ff = depth - c
    n_group = 1 + ff // c
    n_units = 8 * n_group
    row_parts = 4
    row_part = rows // row_parts
    n_other = n_model // 2 - 1
    gain_shape = (n_data, 8, part)
    n_tiles = 1 if start_layer else x_own.shape[0] * x_own.shape[1]

    def kernel(*refs):
        x_ref, head_ref, w_ref, wo_ref = refs[:4]
        if start_layer:
            gain_ref = refs[4]
            q_ref, m_ref, kv_ref, gains_ref, out_first_ref, in_first_ref = refs[5:11]
            first_ref = column_ref = None
            rest = refs[11:]
        else:
            par_ref, gain_ref, first_ref, column_ref = refs[4:8]
            q_ref, m_ref, kv_ref, out_first_ref, out_column_ref = refs[8:13]
            rest = refs[13:]
        wbuf, h_ref, gbuf, stage, kv_stage, send, recv, w_local, next_send, next_recv, late_send, late_recv = rest[:12]
        x_send, x_recv, g_send, g_recv, kv_send, kv_recv, local, out_sem, tile_sem = rest[12:]

        place = Place(n_data, n_model, partner, neighbour)
        place.meet()
        w = GatherIn(place, wbuf, in_halves(layer, head_ref, w_ref, c, ff), send, recv, w_local, first_ref, column_ref)
        out_column = None if start_layer else out_column_ref
        out_next = GatherOut(place, out_column, wo_ref.at[layer], next_send, next_recv)
        if start_layer:
            in_own = in_halves(layer + 1, head_ref, w_ref, c, ff)
            in_next = FetchIn(place, in_own, late_send, late_recv, next_neighbour(place.me), in_first_ref)

        def c_x(part_no):
            piece = pl.ds(part_no * row_part, row_part)
            return remote(
                x_ref.at[piece], h_ref.at[1, piece], x_send.at[part_no], x_recv.at[part_no], {"model": place.partner}
            )

        def c_gain(which):
            target = {"data": (place.up, place.down, place.far)[which]}
            return remote(gain_ref, gbuf.at[place.y], g_send.at[which], g_recv.at[which], target)

        def c_kv(which):
            ref = kv_ref.at[place.me]
            return remote(ref, ref, kv_send.at[which], kv_recv.at[which], {"model": place.ahead[which]})

        def c_kv_mate(which):
            ref = kv_ref.at[place.me if which == 0 else place.behind[which - 1]]
            at = n_other + which
            return remote(ref, ref, kv_send.at[at], kv_recv.at[at], {"model": place.mate})

        save_kv = pltpu.make_async_copy(kv_stage, kv_ref.at[place.me], local.at[0])
        if start_layer:
            load_x = pltpu.make_async_copy(x_ref, h_ref.at[0], local.at[0])

        def load_tile(side, k):
            chunk, slot = k // n_data, lax.rem(k, n_data)
            src = (x_ref, par_ref)[side].at[chunk, slot]
            height, across = src.shape
            down_to, along = pl.multiple_of(chunk * height, height), pl.multiple_of(slot * across, across)
            return pltpu.make_async_copy(src, h_ref.at[side, pl.ds(down_to, height), pl.ds(along, across)], tile_sem.at[side, k])

        if start_layer:
            load_gain = pltpu.make_async_copy(gain_ref, gbuf.at[place.y], local.at[1])
            for which in range(3):
                c_gain(which).start()
        else:
            load_gain = pltpu.make_async_copy(gain_ref, gbuf, local.at[1])
        load_gain.start()
        if start_layer:
            load_x.start()
        else:
            for side in range(2):

                @pl.loop(0, n_tiles)
                def _(k):
                    load_tile(side, k).start()

        if start_layer:
            for g in range(2):
                for half in range(2):
                    w.up(g, half).start()
                    w.down(g, half).start()
            for g in range(n_group):
                for half in range(2):
                    w.neighbour_first(g, half).start()
                    w.load_own(g, half).start()
            for part_no in range(row_parts):
                c_x(part_no).start()
        else:
            for g in range(n_group):
                for half in range(2):
                    w.load_own(g, half).start()
                for which in range(1, 4):
                    w.load_column(g, which).start()
                w.side_up(g).start()
                w.side_down(g).start()
                w.far(g).start()
            for g in range(n_group):
                w.load_first(g).start()
            out_next.neighbour_first(out_first_ref).start()
            out_next.up().start()
            out_next.down().start()

        def ring_stage(g):
            for half in range(2):
                w.up(g, half).wait_recv()
                w.down(g, half).wait_recv()
            w.forward(g).start()

            @pl.when(g + 2 < n_group)
            def _():
                for half in range(2):
                    w.up(g + 2, half).start()
                    w.down(g + 2, half).start()

        if start_layer:
            for which in range(3):
                c_gain(which).wait_recv()
        load_gain.wait()
        gain = jnp.concatenate([gbuf[k, layer:layer + 1, :] for k in range(n_data)], axis=1)
        if start_layer:
            save_gain = pltpu.make_async_copy(gbuf, gains_ref, local.at[1])
            save_gain.start()
        if start_layer:
            load_x.wait()
        else:

            @pl.loop(0, n_tiles)
            def _(k):
                load_tile(0, k).wait()

        def norm_rows(side, part_no):
            piece = pl.ds(part_no * row_part, row_part)
            h_ref[side, piece] = rms_norm(h_ref[side, piece], gain)

        @pl.loop(0, row_parts)
        def _(part_no):
            norm_rows(0, part_no)

        if start_layer:
            ring_stage(0)
        else:
            for g in range(n_group):
                for half in range(2):
                    w.load_own(g, half).wait()
                for which in range(1, 4):
                    w.load_column(g, which).wait()
                w.mate(g).start()

            @pl.loop(0, n_tiles)
            def _(k):
                load_tile(1, k).wait()

            @pl.loop(0, row_parts)
            def _(part_no):
                norm_rows(1, part_no)

        halfway, quarter = n_units // 2, n_units // 4

        def out_copy(slot, blk, side, g):
            def to_q():
                return pltpu.make_async_copy(stage.at[slot], q_ref.at[blk, side], out_sem.at[slot])

            def to_m():
                return pltpu.make_async_copy(stage.at[slot], m_ref.at[blk, side, g - 1], out_sem.at[slot])

            return to_q, to_m

        @pl.loop(0, n_units)
        def _(step):
            late = step - halfway
            if start_layer:
                opening, second = step < quarter, (step >= quarter) & (step < halfway)
                g = jnp.where(opening, step // 2, jnp.where(second, (step - quarter) // 2, late // 4))
                blk = jnp.where(step < halfway, lax.rem(step, 2), 2 + lax.rem(late, 4) // 2)
                side = jnp.where(opening, 0, jnp.where(second, 1, lax.rem(late, 2)))

                @pl.when(opening & (blk == 0))
                def _():
                    @pl.when(g + 1 < n_group)
                    def _():
                        ring_stage(g + 1)

                    @pl.when(g + 2 == n_group)
                    def _():
                        @pl.loop(0, n_group)
                        def _(k):
                            for half in range(2):
                                w.neighbour_first(k, half).wait_recv()
                            w.side_up(k).start()
                            w.side_down(k).start()

                    w.forward(g).wait_recv()
                    w.far(g).start()
                    for half in range(2):
                        w.load_own(g, half).wait()
                    w.mate(g).start()

                @pl.when(opening & (blk == 1))
                def _():
                    w.mate(g).wait_recv()

                @pl.when(step == quarter)
                def _():
                    @pl.loop(0, row_parts)
                    def _(part_no):
                        c_x(part_no).wait_recv()
                        norm_rows(1, part_no)

                    out_next.neighbour_first(out_first_ref).start()
                    for k in range(n_group):
                        for half in range(2):
                            in_next.neighbour_first(k, half).start()
            else:
                g = jnp.where(late < 0, step, late) // 4
                blk = jnp.where(late < 0, 0, 2) + lax.rem(step, 4) // 2
                side = lax.rem(step, 2)

                @pl.when((late < 0) & (lax.rem(step, 4) == 2))
                def _():
                    w.mate(g).wait_recv()

                @pl.when(step == n_units - 6)
                def _():
                    out_next.up().wait_recv()
                    out_next.down().wait_recv()
                    out_next.forward().start()
                    out_next.forward_b().start()

            @pl.when(step == halfway - 2)
            def _():
                w.pass_side(0)

            @pl.when((late >= 0) & (lax.rem(late, 4) == 2))
            def _():
                @pl.when(g + 1 < n_group)
                def _():
                    w.pass_side(g + 1)

                w.side_mate(g).wait_recv()

            slot = lax.rem(step, 2)
            to_q, to_m = out_copy(slot, blk, side, g)

            @pl.when(step >= 2)
            def _():
                to_q().wait()

            def columns(half):
                return wbuf[blk, g, :, half].reshape(d_model, c)

            @pl.when(g == 0)
            def _():
                q = jnp.dot(h_ref[side], columns(0), preferred_element_type=F32)
                stage[slot] = q.astype(BF16)
                to_q().start()

            @pl.when(g > 0)
            def _():
                h_val = h_ref[side]
                gate = jnp.dot(h_val, columns(0), preferred_element_type=F32).astype(BF16).astype(F32)
                raised = jnp.dot(h_val, columns(1), preferred_element_type=F32).astype(BF16).astype(F32)
                stage[slot] = (gate * jax.nn.sigmoid(gate) * raised).astype(BF16)
                to_m().start()

            @pl.when(step == 0)
            def _():
                kv_stage[...] = jnp.dot(h_ref[0], columns(1), preferred_element_type=F32).astype(BF16)
                save_kv.start()

            @pl.when(step == 1)
            def _():
                save_kv.wait()
                for which in range(n_other):
                    c_kv(which).start()
                c_kv_mate(0).start()

            @pl.when(step == quarter)
            def _():
                for which in range(n_other):
                    c_kv(which).wait_recv()
                    c_kv_mate(1 + which).start()

        for which in range(n_other + 1):
            c_kv_mate(which).wait()
        for which in range(n_other):
            c_kv(which).wait_send()
        if start_layer:
            save_gain.wait()
            for which in range(3):
                c_gain(which).wait_send()
            for part_no in range(row_parts):
                c_x(part_no).wait_send()
            for g in range(n_group):
                for half in range(2):
                    in_next.neighbour_first(g, half).wait()
        else:
            for copy in (out_next.forward(), out_next.forward_b()):
                copy.wait()
            for copy in (out_next.up(), out_next.down()):
                copy.wait_send()
        out_next.neighbour_first(out_first_ref).wait()
        for slot in range(2):
            pltpu.make_async_copy(stage.at[slot], q_ref.at[0, 0], out_sem.at[slot]).wait()

        @pl.loop(0, n_group)
        def _(g):
            w.wait_sends(g)

    anywhere = pl.BlockSpec(memory_space=pl.ANY)
    out_shape = [
        jax.ShapeDtypeStruct((4, 2, rows, c), BF16),
        jax.ShapeDtypeStruct((4, 2, n_group - 1, rows, c), BF16),
        jax.ShapeDtypeStruct((n_model, rows, c), BF16),
    ]
    if start_layer:
        out_shape += [
            jax.ShapeDtypeStruct(gain_shape, F32),
            jax.ShapeDtypeStruct((depth, out_part), BF16),
            jax.ShapeDtypeStruct((n_group, 2, part, c), BF16),
        ]
    else:
        out_shape += [
            jax.ShapeDtypeStruct((depth, out_part), BF16),
            jax.ShapeDtypeStruct((1, n_data, depth, out_part), BF16),
        ]
    dma = pltpu.SemaphoreType.DMA
    args = (x_own, head, w_in, w_out) + tuple(extra)
    return pl.pallas_call(
        kernel,
        out_shape=out_shape,
        in_specs=[anywhere] * len(args),
        out_specs=[anywhere] * len(out_shape),
        scratch_shapes=[
            pltpu.VMEM((4, n_group, n_data, 2, part, c), BF16),
            pltpu.VMEM((2, rows, d_model), BF16),
            pltpu.VMEM(gain_shape, F32),
            pltpu.VMEM((2, rows, c), BF16),
            pltpu.VMEM((rows, c), BF16),
            dma((SIDE_MATE + 1, 2 * n_group)), dma((SIDE_MATE + 1, 2 * n_group)), dma((6, n_group)),
            dma((FIRST + 1,)), dma((FIRST + 1,)), dma((4, 2 * n_group)), dma((4, 2 * n_group)),
            dma((row_parts,)), dma((row_parts,)), dma((3,)), dma((3,)),
            dma((n_model - 1,)), dma((n_model - 1,)), dma((3,)), dma((2,)), dma((2, n_tiles)),
        ],
        compiler_params=pltpu.CompilerParams(collective_id=2 * layer, has_side_effects=True, vmem_limit_bytes=VMEM_LIMIT),
        cost_estimate=pl.CostEstimate(flops=4 * rows * d_model * 4 * (c + 2 * ff), bytes_accessed=16 * rows * d_model, transcendentals=0),
        name=f"project_{layer}",
    )(*args)


def attend_and_sum(layer, last, n_data, n_model, partner, neighbour, next_partner, lens, q, m, kv, x_own, w_in, w_out, head, first, column):
    n_blocks, _, rows, c = q.shape
    n_mid = m.shape[2]
    ff = n_mid * c
    d_model = w_out.shape[2] * n_data
    tiled = x_own.ndim == 4
    depth, out_part = w_out.shape[1:]
    head_dim = c // 2
    n_batch = lens.shape[0]
    slab_len = rows // n_batch
    chunks = 4
    n_seq = n_batch // chunks
    crow = rows // chunks
    tiles = chunks * n_data
    heads = n_blocks * 2
    qrows = heads * slab_len
    key_rows = 2 * slab_len
    scale = head_dim ** -0.5 * 1.4426950408889634
    part = head.shape[1]
    n_group = 1 + ff // c
    ready = column is not None
    held = tiles // 2

    def kernel(*refs):
        lens_ref, q_ref, m_ref, kv_ref, x_ref, wo_ref, first_ref = refs[:7]
        at = 7
        column_ref = None
        if ready:
            column_ref = refs[at]
            at += 1
        if not last:
            head_ref, wi_ref = refs[at:at + 2]
            at += 2
        y_ref = refs[at]
        at += 1
        if not last:
            par_ref, in_column_ref = refs[at:at + 2]
            at += 2
        (wbuf, obuf, kvb, mbuf, xb, zb, zr, z_stage, s_ref, mx_ref, sum_ref, acc_ref,
         send, recv, w_local, in_send, in_recv, z_send, z_recv, y_send, y_recv, y_save, x_sem, m_sem, local) = refs[at:]

        place = Place(n_data, n_model, partner, neighbour)
        place.meet()
        w = GatherOut(place, wbuf, wo_ref.at[layer], send, recv, w_local, first_ref, column_ref)

        def tile_of(k):
            which = k // chunks
            slot = jnp.where(which == 0, place.y, jnp.where(which == 1, place.down, jnp.where(which == 2, place.up, place.far)))
            return lax.rem(k, chunks), which, slot

        def whole(ref, chunk, slot):
            return ref.at[pl.ds(pl.multiple_of(chunk * crow, crow), crow), pl.ds(pl.multiple_of(slot * out_part, out_part), out_part)]

        load_q = pltpu.make_async_copy(q_ref, obuf, local.at[0])
        load_kv = pltpu.make_async_copy(kv_ref, kvb, local.at[1])

        def load_m(k):
            chunk, _, _ = tile_of(k)
            slot = lax.rem(k, 2)
            return pltpu.make_async_copy(
                m_ref.at[:, :, :, pl.ds(pl.multiple_of(chunk * crow, crow), crow)], mbuf.at[slot], m_sem.at[slot]
            )

        def load_x(k):
            chunk, _, slot = tile_of(k)
            src = x_ref.at[chunk, slot] if tiled else whole(x_ref, chunk, slot)
            return pltpu.make_async_copy(src, xb.at[chunk, slot], x_sem.at[k])

        def c_z(k):
            chunk, _, slot = tile_of(k)
            return remote(z_stage.at[lax.rem(k, 4)], zr.at[chunk, slot], z_send.at[k], z_recv.at[k], {"model": place.partner})

        def c_y(k):
            chunk, _, slot = tile_of(k)
            target = {"model": next_partner(place.me)}
            return remote(xb.at[chunk, slot], par_ref.at[chunk, slot], y_send.at[k], y_recv.at[k], target)

        def save_y(k):
            chunk, _, slot = tile_of(k)
            dst = whole(y_ref, chunk, slot) if last else y_ref.at[chunk, slot]
            return pltpu.make_async_copy(xb.at[chunk, slot], dst, y_save.at[k])

        load_q.start()
        load_kv.start()
        load_m(0).start()
        w.load_own().start()
        w.load_first().start()
        w.mate(0).start()
        w.side_mate(0).start()
        if ready:
            w.far().start()
            for which in range(1, 4):
                w.load_column(which).start()
                w.mate(which).start()
        else:
            w.up().start()
            w.down().start()
        w.side_up().start()
        w.side_down().start()
        if not last:
            in_own = in_halves(layer + 1, head_ref, wi_ref, c, ff)
            in_next = FetchIn(place, in_own, in_send, in_recv, column=in_column_ref)

        @pl.loop(0, tiles)
        def _(k):
            load_x(k).start()

        load_q.wait()
        load_kv.wait()

        def attend_one(batch, side):
            slab = jnp.where(side == 0, place.me, place.partner)
            length = lens_ref[batch]
            n_key = slab // 2 + 1
            at_row = pl.ds(pl.multiple_of(batch * slab_len, slab_len), slab_len)
            parts = []
            for blk in range(n_blocks):
                for one in range(2):
                    parts.append(obuf[blk, side, at_row, one * head_dim:(one + 1) * head_dim])
            q_val = jnp.concatenate(parts, axis=0)
            row_pos = slab * slab_len + lax.rem(lax.broadcasted_iota(jnp.int32, (qrows, key_rows), 0), slab_len)
            key_pos = lax.broadcasted_iota(jnp.int32, (qrows, key_rows), 1)
            room = jnp.minimum(row_pos + 1, length) - key_pos
            mx_ref[...] = jnp.full_like(mx_ref, -1e30)

            def score(kb, carry):
                k = kvb[pl.ds(2 * kb, 2), at_row, :head_dim].reshape(key_rows, head_dim)
                s = lax.dot_general(q_val, k, (((1,), (1,)), ((), ())), preferred_element_type=F32) * scale
                s = jnp.where(room > kb * key_rows, s, -1e30)
                s_ref[kb] = s
                mx_ref[...] = jnp.maximum(mx_ref[...], jnp.maximum(s[:, :slab_len], s[:, slab_len:]))
                return carry

            lax.fori_loop(0, n_key, score, 0)
            top = jnp.max(mx_ref[...], axis=-1, keepdims=True)
            mx_ref[...] = jnp.broadcast_to(top, mx_ref.shape)
            sum_ref[...] = jnp.zeros_like(sum_ref)
            acc_ref[...] = jnp.zeros_like(acc_ref)

            def weigh(kb, carry):
                v = kvb[pl.ds(2 * kb, 2), at_row, head_dim:].reshape(key_rows, head_dim)
                top_b = mx_ref[...]
                e_lo = jnp.exp2(s_ref[kb, :, :slab_len] - top_b)
                e_hi = jnp.exp2(s_ref[kb, :, slab_len:] - top_b)
                sum_ref[...] += e_lo + e_hi
                e = jnp.concatenate([e_lo, e_hi], axis=1).astype(BF16)
                acc_ref[...] += jnp.dot(e, v, preferred_element_type=F32)
                return carry

            lax.fori_loop(0, n_key, weigh, 0)
            out = (acc_ref[...] / jnp.sum(sum_ref[...], axis=-1, keepdims=True)).astype(BF16)
            for blk in range(n_blocks):
                for one in range(2):
                    first_row = (blk * 2 + one) * slab_len
                    obuf[blk, side, at_row, one * head_dim:(one + 1) * head_dim] = out[first_row:first_row + slab_len]

        def settle(k):
            chunk, _, slot = tile_of(k)
            load_x(k).wait()
            c_z(k).wait_recv()
            z = zb[chunk, slot].astype(F32) + zr[chunk, slot].astype(F32)
            xb[chunk, slot] = (xb[chunk, slot].astype(F32) + z).astype(BF16)
            save_y(k).start()
            if not last:
                c_y(k).start()

        @pl.loop(0, tiles)
        def _(step):
            chunk, which, slot = tile_of(step)

            @pl.when(step + 1 < tiles)
            def _():
                load_m(step + 1).start()

            @pl.when(step < chunks)
            def _():
                @pl.loop(0, 2 * n_seq)
                def _(unit):
                    attend_one(step * n_seq + unit // 2, lax.rem(unit, 2))

            @pl.when(step == 0)
            def _():
                w.load_own().wait()
                w.load_first().wait()
                w.mate(0).wait_recv()
                w.side_mate(0).wait_recv()

            if not ready:

                @pl.when(step == 2)
                def _():
                    w.up().wait_recv()
                    w.down().wait_recv()
                    w.forward().start()
                    w.forward_b().start()
                    w.mate(1).start()
                    w.mate(2).start()
                    if not last:
                        for g in range(2):
                            for half in range(2):
                                in_next.up(g, half).start()
                                in_next.down(g, half).start()

                @pl.when(step == chunks + 2)
                def _():
                    w.forward().wait_recv()
                    w.forward_b().wait_recv()
                    w.far().start()
                    w.mate(3).start()

            @pl.when(step == chunks)
            def _():
                w.side_up().wait_recv()
                w.side_mate(1).start()
                w.side_down().wait_recv()
                w.side_mate(2).start()
                for one in (1, 2):
                    if ready:
                        w.load_column(one).wait()
                    w.mate(one).wait_recv()
                    w.side_mate(one).wait_recv()

            @pl.when(step == 3 * chunks)
            def _():
                w.far().wait_recv()
                w.side_mate(3).start()
                if ready:
                    w.load_column(3).wait()
                w.mate(3).wait_recv()
                w.side_mate(3).wait_recv()

            if not last:
                @pl.when((step >= chunks + 3) & (lax.rem(step, 2) == 1))
                def _():
                    g = (step - chunks - 3) // 2

                    @pl.when(g < n_group - 2)
                    def _():
                        for half in range(2):
                            in_next.up(g + 2, half).start()
                            in_next.down(g + 2, half).start()

            @pl.when(step >= 4)
            def _():
                c_z(step - 4).wait_send()

            load_m(step).wait()
            here = lax.rem(step, 2)
            rows_c = pl.ds(pl.multiple_of(chunk * crow, crow), crow)
            total = None
            for blk in range(n_blocks):
                mid = jnp.concatenate([mbuf[here, blk, :, k].reshape(2 * crow, c) for k in range(n_mid)], axis=1)
                attn = obuf[blk, :, rows_c, :].reshape(2 * crow, c)
                one = jnp.dot(mid, wbuf[blk, slot, c:, :], preferred_element_type=F32)
                one = one + jnp.dot(attn, wbuf[blk, slot, :c, :], preferred_element_type=F32)
                total = one if total is None else total + one
            z = total.astype(BF16)
            zb[chunk, slot] = z[:crow]
            z_stage[lax.rem(step, 4)] = z[crow:]
            c_z(step).start()

            early = (step >= 1) & (step <= chunks)
            paced = (step >= 2 * chunks) & (lax.rem(step, 2) == 0)

            @pl.when(early | paced)
            def _():
                settle(jnp.where(early, step - 1, step // 2))

        if not last:

            @pl.loop(0, n_group)
            def _(g):
                for half in range(2):
                    in_next.up(g, half).wait_recv()
                    in_next.down(g, half).wait_recv()
                in_next.forward(g).start()

        @pl.loop(held, tiles)
        def _(k):
            settle(k)

        @pl.loop(0, tiles)
        def _(k):
            save_y(k).wait()
            if not last:
                c_y(k).wait()

        @pl.loop(tiles - 4, tiles)
        def _(k):
            c_z(k).wait_send()

        made = [w.side_up(), w.side_down(), w.far()]
        made += [w.mate(which) for which in range(4)] + [w.side_mate(which) for which in range(4)]
        if not ready:
            made += [w.up(), w.down(), w.forward(), w.forward_b()]
        for copy in made:
            copy.wait_send()
        if not last:

            @pl.loop(0, n_group)
            def _(g):
                in_next.forward(g).wait()
                for half in range(2):
                    in_next.up(g, half).wait_send()
                    in_next.down(g, half).wait_send()

    anywhere = pl.BlockSpec(memory_space=pl.ANY)
    args = [lens, q, m, kv, x_own, w_out, first]
    if ready:
        args.append(column)
    if not last:
        args += [head, w_in]
    tile = (chunks, n_data, crow, out_part)
    out_shape = [jax.ShapeDtypeStruct((rows, d_model) if last else tile, BF16)]
    if not last:
        out_shape += [
            jax.ShapeDtypeStruct(tile, BF16),
            jax.ShapeDtypeStruct((n_group, n_data, 2, part, c), BF16),
        ]
    dma = pltpu.SemaphoreType.DMA
    return pl.pallas_call(
        kernel,
        out_shape=out_shape,
        in_specs=[pl.BlockSpec(memory_space=pltpu.SMEM)] + [anywhere] * (len(args) - 1),
        out_specs=[anywhere] * len(out_shape),
        scratch_shapes=[
            pltpu.VMEM((n_blocks, n_data, depth, out_part), BF16),
            pltpu.VMEM(q.shape, BF16),
            pltpu.VMEM(kv.shape, BF16),
            pltpu.VMEM((2, n_blocks, 2, n_mid, crow, c), BF16),
            pltpu.VMEM(tile, BF16),
            pltpu.VMEM(tile, BF16),
            pltpu.VMEM(tile, BF16),
            pltpu.VMEM((4, crow, out_part), BF16),
            pltpu.VMEM((n_model // 2, qrows, key_rows), F32),
            pltpu.VMEM((qrows, slab_len), F32),
            pltpu.VMEM((qrows, slab_len), F32),
            pltpu.VMEM((qrows, head_dim), F32),
            dma((SIDE_MATE + 7,)), dma((SIDE_MATE + 7,)), dma((5,)), dma((3, 2 * n_group)), dma((3, 2 * n_group)),
            dma((tiles,)), dma((tiles,)), dma((tiles,)), dma((tiles,)), dma((tiles,)), dma((tiles,)), dma((2,)), dma((2,)),
        ],
        compiler_params=pltpu.CompilerParams(collective_id=2 * layer + 1, has_side_effects=True, vmem_limit_bytes=VMEM_LIMIT),
        cost_estimate=pl.CostEstimate(flops=4 * rows * n_blocks * depth * d_model, bytes_accessed=16 * rows * d_model, transcendentals=0),
        name=f"attend_and_sum_{layer}",
    )(*args)


def solution(mesh):
    batch_axes = ("rep", "data")
    n_data, n_model = mesh.shape["data"], mesh.shape["model"]
    n_chip = n_model // 2

    def near(x):
        return x + 1 - 2 * (x % 2)

    def across(x):
        return n_chip - 1 - x

    def on_chip(other):
        return lambda m: 2 * other(m // 2) + m % 2

    def local_step(x_loc, lens_loc, gamma_loc, w_in_loc, w_kv_loc, w_out_loc):
        n_batch, slab_len, d_model = x_loc.shape
        n_layers, part = gamma_loc.shape
        attn_cols = w_kv_loc.shape[2]
        partners = [on_chip(near if layer % 2 == 0 else across) for layer in range(n_layers)]
        neighbours = [on_chip(across if layer % 2 == 0 else near) for layer in range(n_layers)]

        head = jnp.concatenate([w_in_loc[:, :, :attn_cols], w_kv_loc], axis=2)
        gain_rows = jnp.zeros((8, part), F32).at[:n_layers].set(gamma_loc.astype(F32))
        own = x_loc.reshape(n_batch * slab_len, d_model)
        for layer in range(n_layers):
            last = layer + 1 == n_layers
            following = min(layer + 1, n_layers - 1)
            if layer == 0:
                extra = (gain_rows,)
                q, m, kv, gains, out_first, in_first = project(
                    layer, n_data, n_model, partners[layer], neighbours[layer], neighbours[following],
                    own, head, w_in_loc, w_out_loc, extra,
                )
                out_column = None
            else:
                extra = (other, gains, in_first, in_column)
                q, m, kv, out_first, out_column = project(
                    layer, n_data, n_model, partners[layer], neighbours[layer], neighbours[following],
                    own, head, w_in_loc, w_out_loc, extra,
                )
            outs = attend_and_sum(
                layer, last, n_data, n_model, partners[layer], neighbours[layer], partners[following],
                lens_loc, q, m, kv, own, w_in_loc, w_out_loc, head, out_first, out_column,
            )
            own = outs[0]
            if not last:
                other, in_column = outs[1:]
        return own.reshape(n_batch, slab_len, d_model)

    in_specs = (
        P(batch_axes, "model", None),
        P(batch_axes),
        P(None, "data"),
        P(None, "data", "model"),
        P(None, "data", None),
        P(None, "model", "data"),
    )
    return jax.shard_map(local_step, mesh=mesh, in_specs=in_specs, out_specs=P(batch_axes, "model", None), check_vma=False)
```

```python
import functools

import jax
import jax.numpy as jnp
from jax import lax
from jax.experimental import pallas as pl
from jax.experimental.pallas import tpu as pltpu
from jax.sharding import PartitionSpec as P

EPSILON = 1e-6
VMEM_LIMIT = 66_000_000
MESH = pl.DeviceIdType.MESH
BF16, F32 = jnp.bfloat16, jnp.float32

UP, DOWN, FORWARD, FORWARD_B, FIRST, SIDE_UP, SIDE_DOWN, FAR, MATE, SIDE_MATE = range(10)


def rms_norm(x_in, gain):
    x_f32 = x_in.astype(F32)
    inv_rms = lax.rsqrt(jnp.mean(x_f32 * x_f32, axis=-1, keepdims=True) + EPSILON)
    return (x_f32 * inv_rms * gain.astype(F32)).astype(BF16)


class Place:
    def __init__(self, n_data, n_model, partner, neighbour):
        self.n_data, self.n_model = n_data, n_model
        self.y = lax.axis_index("data")
        self.me = lax.axis_index("model")
        self.up = lax.rem(self.y + 1, n_data)
        self.down = lax.rem(self.y + n_data - 1, n_data)
        self.far = lax.rem(self.y + 2, n_data)
        self.slots = (self.y, self.down, self.up, self.far)
        self.mate = self.me + 1 - 2 * lax.rem(self.me, 2)
        self.partner, self.neighbour = partner(self.me), neighbour(self.me)
        n_other = n_model // 2 - 1
        self.ahead = [lax.rem(self.me + 2 * k, n_model) for k in range(1, n_other + 1)]
        self.behind = [lax.rem(self.me + n_model - 2 * k, n_model) for k in range(1, n_other + 1)]

    def meet(self):
        barrier = pltpu.get_barrier_semaphore()
        targets = [{"data": self.up}, {"data": self.down}, {"data": self.far}, {"model": self.mate}]
        targets += [{"model": m} for m in self.ahead]
        for target in targets:
            pl.semaphore_signal(barrier, inc=1, device_id=target, device_id_type=MESH)
        pl.semaphore_wait(barrier, len(targets))


def remote(src, dst, send, recv, target):
    return pltpu.make_async_remote_copy(
        src_ref=src, dst_ref=dst, send_sem=send, recv_sem=recv, device_id=target, device_id_type=MESH
    )


class GatherIn:
    def __init__(self, place, buf, pool, own, send, recv, local, first=None, column=None):
        self.place, self.buf, self.pool, self.own, self.first, self.column = place, buf, pool, own, first, column
        self.send, self.recv, self.local = send, recv, local

    def at(self, block, g, slot):
        return self.buf.at[block, g, slot]

    def _copy(self, src, dst, kind, at, target):
        return remote(src, dst, self.send.at[kind, at], self.recv.at[kind, at], target)

    def up(self, g, half):
        dst = self.at(0, g, self.place.y).at[half]
        return self._copy(self.own(g, half), dst, UP, 2 * g + half, {"data": self.place.up})

    def down(self, g, half):
        dst = self.at(0, g, self.place.y).at[half]
        return self._copy(self.own(g, half), dst, DOWN, 2 * g + half, {"data": self.place.down})

    def neighbour_first(self, g, half):
        dst = self.at(2, g, self.place.y).at[half]
        return self._copy(self.own(g, half), dst, FIRST, 2 * g + half, {"model": self.place.neighbour})

    def forward(self, g, half):
        ref = self.at(0, g, (self.place.down, self.place.up)[half]).at[half]
        target = (self.place.up, self.place.down)[half]
        return self._copy(ref, ref, FORWARD, 2 * g + half, {"data": target})

    def _side(self, g):
        return self.at(2, g, self.place.y) if self.first is None else self.first.at[g]

    def side_up(self, g):
        return self._copy(self._side(g), self.at(2, g, self.place.y), SIDE_UP, g, {"data": self.place.up})

    def side_down(self, g):
        return self._copy(self._side(g), self.at(2, g, self.place.y), SIDE_DOWN, g, {"data": self.place.down})

    def far(self, g):
        slot = self.place.far
        src = self.at(0, g, slot) if self.column is None else self.column.at[g, slot]
        return self._copy(src, self.at(2, g, slot), FAR, g, {"model": self.place.neighbour})

    def mate(self, g):
        return self._copy(self.buf.at[0, g], self.pool.at[0, g], MATE, g, {"model": self.place.mate})

    def side_mate(self, g):
        return self._copy(self.buf.at[2, g], self.pool.at[1, g], SIDE_MATE, g, {"model": self.place.mate})

    def load_mate(self, g):
        return pltpu.make_async_copy(self.pool.at[0, g], self.buf.at[1, g], self.local.at[6, g])

    def load_side(self, g):
        return pltpu.make_async_copy(self.pool.at[1, g], self.buf.at[3, g], self.local.at[7, g])

    def take_mate(self, g):
        self.mate(g).wait_recv()
        self.load_mate(g).start()

    def take_side(self, g):
        self.side_mate(g).wait_recv()
        self.load_side(g).start()

    def load_own(self, g, half):
        dst = self.at(0, g, self.place.y).at[half]
        return pltpu.make_async_copy(self.own(g, half), dst, self.local.at[half, g])

    def load_column(self, g, which):
        slot = self.place.slots[which]
        return pltpu.make_async_copy(self.column.at[g, slot], self.at(0, g, slot), self.local.at[1 + which, g])

    def load_first(self, g):
        return pltpu.make_async_copy(self.first.at[g], self.at(2, g, self.place.y), self.local.at[5, g])

    def pass_side(self, g):
        if self.first is not None:
            self.load_first(g).wait()
        self.side_up(g).wait_recv()
        self.side_down(g).wait_recv()
        self.far(g).wait_recv()
        self.side_mate(g).start()

    def wait_sends(self, g):
        made = [self.side_up(g), self.side_down(g), self.far(g), self.mate(g), self.side_mate(g)]
        if self.column is None:
            made += [copy(g, half) for copy in (self.up, self.down, self.forward) for half in range(2)]
        if self.first is None:
            made += [self.neighbour_first(g, half) for half in range(2)]
        for copy in made:
            copy.wait_send()


class FetchIn:
    def __init__(self, place, own, send, recv, neighbour=None, first=None, column=None):
        self.place, self.own, self.send, self.recv = place, own, send, recv
        self.neighbour, self.first, self.column = neighbour, first, column

    def _ring(self, g, half, kind, target):
        at = 2 * g + half
        dst = self.column.at[g, self.place.y, half]
        return remote(self.own(g, half), dst, self.send.at[kind, at], self.recv.at[kind, at], {"data": target})

    def up(self, g, half):
        return self._ring(g, half, 0, self.place.up)

    def down(self, g, half):
        return self._ring(g, half, 1, self.place.down)

    def forward(self, g, half):
        at = 2 * g + half
        ref = self.column.at[g, (self.place.down, self.place.up)[half], half]
        target = (self.place.up, self.place.down)[half]
        return remote(ref, ref, self.send.at[2, at], self.recv.at[2, at], {"data": target})

    def ring_stage(self, g, n_group):
        for half in range(2):
            self.up(g, half).wait_recv()
            self.down(g, half).wait_recv()
        for half in range(2):
            self.forward(g, half).start()
        if g + 2 < n_group:
            for half in range(2):
                self.up(g + 2, half).start()
                self.down(g + 2, half).start()

    def neighbour_first(self, g, half):
        at = 2 * g + half
        dst = self.first.at[g, half]
        return remote(self.own(g, half), dst, self.send.at[3, at], self.recv.at[3, at], {"model": self.neighbour})


class GatherOut:
    def __init__(self, place, buf, own, send, recv, local=None, first=None, column=None, pool=None, whole_column=True):
        self.place, self.buf, self.own, self.first, self.column = place, buf, own, first, column
        self.far_held = column is not None and whole_column
        self.send, self.recv, self.local, self.pool = send, recv, local, pool

    def _copy(self, src, dst, kind, target):
        return remote(src, dst, self.send.at[kind], self.recv.at[kind], target)

    def up(self):
        return self._copy(self.own, self.buf.at[0, self.place.y], UP, {"data": self.place.up})

    def down(self):
        return self._copy(self.own, self.buf.at[0, self.place.y], DOWN, {"data": self.place.down})

    def _half(self, ref, second):
        size = ref.shape[0] // 2
        return ref.at[pl.ds(second * size, size)]

    def _forward(self, kind, slot, second, target):
        src = self.buf if self.column is None else self.column
        dst = self._half(self.buf.at[0, slot], second)
        return self._copy(self._half(src.at[0, slot], second), dst, kind, {"data": target})

    def forward(self):
        return self._forward(FORWARD, self.place.down, 0, self.place.up)

    def forward_b(self):
        return self._forward(FORWARD_B, self.place.up, 1, self.place.down)

    def neighbour_first(self, dst):
        return self._copy(self.own, dst, FIRST, {"model": self.place.neighbour})

    def side_up(self):
        return self._copy(self.first, self.buf.at[2, self.place.y], SIDE_UP, {"data": self.place.up})

    def side_down(self):
        return self._copy(self.first, self.buf.at[2, self.place.y], SIDE_DOWN, {"data": self.place.down})

    def far(self):
        slot = self.place.far
        src = self.column.at[0, slot] if self.far_held else self.buf.at[0, slot]
        return self._copy(src, self.buf.at[2, slot], FAR, {"model": self.place.neighbour})

    def mate(self, which):
        slot = self.place.slots[which]
        if which == 0:
            src = self.own
        else:
            src = self.column.at[0, slot] if which < 3 or self.far_held else self.buf.at[0, slot]
        return self._copy(src, self.pool.at[0, slot], MATE + 2 * which, {"model": self.place.mate})

    def side_mate(self, which):
        slot = self.place.slots[which]
        src = self.first if which == 0 else self.buf.at[2, slot]
        return self._copy(src, self.pool.at[1, slot], SIDE_MATE + 2 * which, {"model": self.place.mate})

    def load_mate(self, which):
        slot = self.place.slots[which]
        return pltpu.make_async_copy(self.pool.at[0, slot], self.buf.at[1, slot], self.local.at[5 + which])

    def load_side(self, which):
        slot = self.place.slots[which]
        return pltpu.make_async_copy(self.pool.at[1, slot], self.buf.at[3, slot], self.local.at[9 + which])

    def take(self, which):
        self.mate(which).wait_recv()
        self.load_mate(which).start()
        self.side_mate(which).wait_recv()
        self.load_side(which).start()

    def load_own(self):
        return pltpu.make_async_copy(self.own, self.buf.at[0, self.place.y], self.local.at[0])

    def load_column(self, which):
        slot = self.place.slots[which]
        return pltpu.make_async_copy(self.column.at[0, slot], self.buf.at[0, slot], self.local.at[which])

    def load_first(self):
        return pltpu.make_async_copy(self.first, self.buf.at[2, self.place.y], self.local.at[4])


def in_halves(layer, w_kv_ref, w_ref, c, ff):
    def own(g, half):
        if isinstance(g, int) and g == 0:
            return w_kv_ref.at[layer] if half else w_ref.at[layer, :, pl.ds(0, c)]
        return w_ref.at[layer, :, pl.ds(pl.multiple_of(g * c + half * ff, c), c)]

    return own


def project(layer, n_data, n_model, partner, neighbour, next_neighbour, x_own, w_kv, w_in, w_out, extra):
    start_layer = layer == 0
    part, c = w_kv.shape[1:]
    d_model = part * n_data
    rows = x_own.size // d_model
    depth, out_part = w_out.shape[1:]
    ff = depth - c
    n_group = 1 + ff // c
    n_units = 8 * n_group
    row_parts = 4
    row_part = rows // row_parts
    n_other = n_model // 2 - 1
    gain_shape = (n_data, 8, part)
    n_tiles = 1 if start_layer else x_own.shape[0] * x_own.shape[1]

    def kernel(*refs):
        x_ref, w_kv_ref, w_ref, wo_ref = refs[:4]
        if start_layer:
            gain_ref = refs[4]
            q_ref, m_ref, kv_ref, pool_ref, gains_ref, out_first_ref, out_column_ref, in_first_ref = refs[5:13]
            first_ref = column_ref = None
            rest = refs[13:]
        else:
            par_ref, gain_ref, first_ref, column_ref = refs[4:8]
            q_ref, m_ref, kv_ref, pool_ref, out_first_ref, out_column_ref = refs[8:14]
            rest = refs[14:]
        wbuf, h_ref, gbuf, stage, kv_stage, send, recv, w_local, next_send, next_recv, late_send, late_recv = rest[:12]
        x_send, x_recv, g_send, g_recv, kv_send, kv_recv, local, out_sem, tile_sem = rest[12:]

        place = Place(n_data, n_model, partner, neighbour)
        place.meet()
        in_own = in_halves(layer, w_kv_ref, w_ref, c, ff)
        w = GatherIn(place, wbuf, pool_ref, in_own, send, recv, w_local, first_ref, column_ref)
        out_next = GatherOut(place, out_column_ref, wo_ref.at[layer], next_send, next_recv)
        if start_layer:
            in_own_next = in_halves(layer + 1, w_kv_ref, w_ref, c, ff)
            in_next = FetchIn(place, in_own_next, late_send, late_recv, next_neighbour(place.me), in_first_ref)

        def c_x(part_no):
            piece = pl.ds(part_no * row_part, row_part)
            return remote(
                x_ref.at[piece], h_ref.at[1, piece], x_send.at[part_no], x_recv.at[part_no], {"model": place.partner}
            )

        def c_gain(which):
            target = {"data": (place.up, place.down, place.far)[which]}
            return remote(gain_ref, gbuf.at[place.y], g_send.at[which], g_recv.at[which], target)

        def c_kv(which):
            ref = kv_ref.at[place.me]
            return remote(ref, ref, kv_send.at[which], kv_recv.at[which], {"model": place.ahead[which]})

        def c_kv_mate(which):
            ref = kv_ref.at[place.me if which == 0 else place.behind[which - 1]]
            at = n_other + which
            return remote(ref, ref, kv_send.at[at], kv_recv.at[at], {"model": place.mate})

        save_kv = pltpu.make_async_copy(kv_stage, kv_ref.at[place.me], local.at[0])
        if start_layer:
            load_x = pltpu.make_async_copy(x_ref, h_ref.at[0], local.at[0])

        def load_tile(side, k):
            chunk, slot = k // n_data, lax.rem(k, n_data)
            src = (x_ref, par_ref)[side].at[chunk, slot]
            height, across = src.shape
            down_to, along = pl.multiple_of(chunk * height, height), pl.multiple_of(slot * across, across)
            return pltpu.make_async_copy(src, h_ref.at[side, pl.ds(down_to, height), pl.ds(along, across)], tile_sem.at[side, k])

        if start_layer:
            load_gain = pltpu.make_async_copy(gain_ref, gbuf.at[place.y], local.at[1])
            for which in range(3):
                c_gain(which).start()
        else:
            load_gain = pltpu.make_async_copy(gain_ref, gbuf, local.at[1])
        load_gain.start()
        if start_layer:
            load_x.start()
        else:
            for side in range(2):

                @pl.loop(0, n_tiles)
                def _(k):
                    load_tile(side, k).start()

        if start_layer:
            for g in range(2):
                for half in range(2):
                    w.up(g, half).start()
                    w.down(g, half).start()
            for g in range(n_group):
                for half in range(2):
                    w.neighbour_first(g, half).start()
                    w.load_own(g, half).start()
            for part_no in range(row_parts):
                c_x(part_no).start()
        else:
            for g in range(n_group):
                for half in range(2):
                    w.load_own(g, half).start()
                for which in range(1, 4):
                    w.load_column(g, which).start()
                w.side_up(g).start()
                w.side_down(g).start()
                w.far(g).start()
            for g in range(n_group):
                w.load_first(g).start()
            out_next.neighbour_first(out_first_ref).start()
            out_next.up().start()
            out_next.down().start()

        def ring_stage(g):
            for half in range(2):
                w.up(g, half).wait_recv()
                w.down(g, half).wait_recv()
            for half in range(2):
                w.forward(g, half).start()

            @pl.when(g + 2 < n_group)
            def _():
                for half in range(2):
                    w.up(g + 2, half).start()
                    w.down(g + 2, half).start()

        def column_stage(g):
            for half in range(2):
                w.load_own(g, half).wait()
            for which in range(1, 4):
                w.load_column(g, which).wait()
            w.mate(g).start()

        if start_layer:
            for which in range(3):
                c_gain(which).wait_recv()
        load_gain.wait()
        gain = jnp.concatenate([gbuf[k, layer:layer + 1, :] for k in range(n_data)], axis=1)
        if start_layer:
            save_gain = pltpu.make_async_copy(gbuf, gains_ref, local.at[1])
            save_gain.start()
        if start_layer:
            load_x.wait()
        else:

            @pl.loop(0, n_tiles)
            def _(k):
                load_tile(0, k).wait()

        def norm_rows(side, part_no):
            piece = pl.ds(part_no * row_part, row_part)
            h_ref[side, piece] = rms_norm(h_ref[side, piece], gain)

        @pl.loop(0, row_parts)
        def _(part_no):
            norm_rows(0, part_no)

        if start_layer:
            ring_stage(0)
        else:
            column_stage(0)

        halfway, quarter = n_units // 2, n_units // 4

        def out_copy(slot, blk, side, g):
            def to_q():
                return pltpu.make_async_copy(stage.at[slot], q_ref.at[blk, side], out_sem.at[slot])

            def to_m():
                return pltpu.make_async_copy(stage.at[slot], m_ref.at[blk, side, g - 1], out_sem.at[slot])

            return to_q, to_m

        @pl.loop(0, n_units)
        def _(step):
            late = step - halfway
            if start_layer:
                opening, second = step < quarter, (step >= quarter) & (step < halfway)
                ahead = (step == 0) | ((lax.rem(step, 2) == 1) & (step < quarter - 1))
                open_g = jnp.where(ahead, (step + 1) // 2, jnp.where(step == quarter - 1, n_group - 1, step // 2 - 1))
                g = jnp.where(opening, open_g, jnp.where(second, (step - quarter) // 2, late // 4))
                open_blk = jnp.where(ahead, 0, 1)
                blk = jnp.where(opening, open_blk, jnp.where(second, lax.rem(step, 2), 2 + lax.rem(late, 4) // 2))
                side = jnp.where(opening, 0, jnp.where(second, 1, lax.rem(late, 2)))

                @pl.when(opening & (blk == 0))
                def _():
                    with jax.named_scope("a_ring"):
                        @pl.when(g + 1 < n_group)
                        def _():
                            ring_stage(g + 1)

                        @pl.when(g + 2 == n_group)
                        def _():
                            @pl.loop(0, n_group)
                            def _(k):
                                for half in range(2):
                                    w.neighbour_first(k, half).wait_recv()
                                w.side_up(k).start()
                                w.side_down(k).start()

                            out_next.up().start()
                            out_next.down().start()

                        for half in range(2):
                            w.forward(g, half).wait_recv()
                        w.far(g).start()
                        for half in range(2):
                            w.load_own(g, half).wait()
                        w.mate(g).start()

                        @pl.when(g > 0)
                        def _():
                            w.take_mate(g - 1)

                @pl.when(step == quarter - 2)
                def _():
                    with jax.named_scope("a_take_last"):
                        w.take_mate(n_group - 1)

                @pl.when(opening & (blk == 1))
                def _():
                    with jax.named_scope("a_load_mate"):
                        w.load_mate(g).wait()

                @pl.when(step == quarter)
                def _():
                    with jax.named_scope("a_par"):
                        @pl.loop(0, row_parts)
                        def _(part_no):
                            c_x(part_no).wait_recv()
                            norm_rows(1, part_no)

                        out_next.neighbour_first(out_first_ref).start()
                        for k in range(n_group):
                            for half in range(2):
                                in_next.neighbour_first(k, half).start()
            else:
                g = jnp.where(late < 0, step, late) // 4
                blk = jnp.where(late < 0, 0, 2) + lax.rem(step, 4) // 2
                side = lax.rem(step, 2)

                @pl.when((late < 0) & (lax.rem(step, 4) == 0) & (g + 1 < n_group))
                def _():
                    with jax.named_scope("a_col"):
                        column_stage(g + 1)

                @pl.when(step == 1)
                def _():
                    with jax.named_scope("a_par1"):
                        @pl.loop(0, n_tiles)
                        def _(k):
                            load_tile(1, k).wait()

                        @pl.loop(0, row_parts)
                        def _(part_no):
                            norm_rows(1, part_no)

                @pl.when((late < 0) & (lax.rem(step, 4) == 1))
                def _():
                    with jax.named_scope("a_take_mate"):
                        w.take_mate(g)

                @pl.when((late < 0) & (lax.rem(step, 4) == 2))
                def _():
                    with jax.named_scope("a_wait_mate"):
                        w.load_mate(g).wait()

                @pl.when(step == n_units - 6)
                def _():
                    with jax.named_scope("a_next"):
                        out_next.up().wait_recv()
                        out_next.down().wait_recv()
                        out_next.forward().start()
                        out_next.forward_b().start()

            @pl.when(step == halfway - 2)
            def _():
                with jax.named_scope("a_pass0"):
                    w.pass_side(0)

            @pl.when((late >= 0) & (lax.rem(late, 4) == 1))
            def _():
                with jax.named_scope("a_take_side"):
                    w.take_side(g)

            @pl.when((late >= 0) & (lax.rem(late, 4) == 2))
            def _():
                with jax.named_scope("a_pass_side"):
                    @pl.when(g + 1 < n_group)
                    def _():
                        w.pass_side(g + 1)

                    w.load_side(g).wait()

            slot = lax.rem(step, 2)
            to_q, to_m = out_copy(slot, blk, side, g)

            @pl.when(step >= 2)
            def _():
                with jax.named_scope("a_outwait"):
                    to_q().wait()

            def columns(half):
                return wbuf[blk, g, :, half].reshape(d_model, c)

            @pl.when(g == 0)
            def _():
                with jax.named_scope("a_unit_q"):
                    q = jnp.dot(h_ref[side], columns(0), preferred_element_type=F32)
                    stage[slot] = q.astype(BF16)
                    to_q().start()

            @pl.when(g > 0)
            def _():
                with jax.named_scope("a_unit_m"):
                    h_val = h_ref[side]
                    gate = jnp.dot(h_val, columns(0), preferred_element_type=F32).astype(BF16).astype(F32)
                    raised = jnp.dot(h_val, columns(1), preferred_element_type=F32).astype(BF16).astype(F32)
                    stage[slot] = (gate * jax.nn.sigmoid(gate) * raised).astype(BF16)
                    to_m().start()

            @pl.when(step == 0)
            def _():
                kv_stage[...] = jnp.dot(h_ref[0], columns(1), preferred_element_type=F32).astype(BF16)
                save_kv.start()

            @pl.when(step == 1)
            def _():
                with jax.named_scope("a_kv1"):
                    save_kv.wait()
                    for which in range(n_other):
                        c_kv(which).start()
                    c_kv_mate(0).start()

            @pl.when(step == n_units - 3)
            def _():
                with jax.named_scope("a_kvq"):
                    for which in range(n_other):
                        c_kv(which).wait_recv()
                        c_kv_mate(1 + which).start()

        for which in range(n_other + 1):
            c_kv_mate(which).wait()
        for which in range(n_other):
            c_kv(which).wait_send()
        if start_layer:
            save_gain.wait()
            for which in range(3):
                c_gain(which).wait_send()
            for part_no in range(row_parts):
                c_x(part_no).wait_send()
            for g in range(n_group):
                for half in range(2):
                    in_next.neighbour_first(g, half).wait()
            for copy in (out_next.up(), out_next.down()):
                copy.wait()
        else:
            for copy in (out_next.forward(), out_next.forward_b()):
                copy.wait()
            for copy in (out_next.up(), out_next.down()):
                copy.wait_send()
        out_next.neighbour_first(out_first_ref).wait()
        for slot in range(2):
            pltpu.make_async_copy(stage.at[slot], q_ref.at[0, 0], out_sem.at[slot]).wait()

        @pl.loop(0, n_group)
        def _(g):
            w.wait_sends(g)

    anywhere = pl.BlockSpec(memory_space=pl.ANY)
    out_shape = [
        jax.ShapeDtypeStruct((4, 2, rows, c), BF16),
        jax.ShapeDtypeStruct((4, 2, n_group - 1, rows, c), BF16),
        jax.ShapeDtypeStruct((n_model, rows, c), BF16),
        jax.ShapeDtypeStruct((2, n_group, n_data, 2, part, c), BF16),
    ]
    if start_layer:
        out_shape += [
            jax.ShapeDtypeStruct(gain_shape, F32),
            jax.ShapeDtypeStruct((depth, out_part), BF16),
            jax.ShapeDtypeStruct((1, n_data, depth, out_part), BF16),
            jax.ShapeDtypeStruct((n_group, 2, part, c), BF16),
        ]
    else:
        out_shape += [
            jax.ShapeDtypeStruct((depth, out_part), BF16),
            jax.ShapeDtypeStruct((1, n_data, depth, out_part), BF16),
        ]
    dma = pltpu.SemaphoreType.DMA
    args = (x_own, w_kv, w_in, w_out) + tuple(extra)
    return pl.pallas_call(
        kernel,
        out_shape=out_shape,
        in_specs=[anywhere] * len(args),
        out_specs=[anywhere] * len(out_shape),
        scratch_shapes=[
            pltpu.VMEM((4, n_group, n_data, 2, part, c), BF16),
            pltpu.VMEM((2, rows, d_model), BF16),
            pltpu.VMEM(gain_shape, F32),
            pltpu.VMEM((2, rows, c), BF16),
            pltpu.VMEM((rows, c), BF16),
            dma((SIDE_MATE + 1, 2 * n_group)), dma((SIDE_MATE + 1, 2 * n_group)), dma((8, n_group)),
            dma((FIRST + 1,)), dma((FIRST + 1,)), dma((4, 2 * n_group)), dma((4, 2 * n_group)),
            dma((row_parts,)), dma((row_parts,)), dma((3,)), dma((3,)),
            dma((n_model - 1,)), dma((n_model - 1,)), dma((3,)), dma((2,)), dma((2, n_tiles)),
        ],
        compiler_params=pltpu.CompilerParams(collective_id=2 * layer, has_side_effects=True, vmem_limit_bytes=VMEM_LIMIT),
        cost_estimate=pl.CostEstimate(flops=4 * rows * d_model * 4 * (c + 2 * ff), bytes_accessed=16 * rows * d_model, transcendentals=0),
        name=f"project_{layer}",
    )(*args)


def pick(step, values):
    found = jnp.int32(values[0])
    for at in range(1, len(values)):
        if values[at] != values[at - 1]:
            found = jnp.where(step >= at, jnp.int32(values[at]), found)
    return found


def attend_and_sum(layer, last, n_data, n_model, partner, neighbour, next_partner, lens, q, m, kv, x_own, w_in, w_out, w_kv, first, column):
    n_blocks, _, rows, c = q.shape
    n_mid = m.shape[2]
    ff = n_mid * c
    d_model = w_out.shape[2] * n_data
    tiled = x_own.ndim == 4
    depth, out_part = w_out.shape[1:]
    head_dim = c // 2
    n_batch = lens.shape[0]
    slab_len = rows // n_batch
    chunks = 4
    n_seq = n_batch // chunks
    crow = rows // chunks
    tiles = chunks * n_data
    heads = n_blocks * 2
    qrows = heads * slab_len
    key_rows = 2 * slab_len
    scale = head_dim ** -0.5 * 1.4426950408889634
    part = w_kv.shape[1]
    n_group = 1 + ff // c
    order = [(0, 0), (1, 0), (0, 1), (1, 1), (0, 2), (1, 2), (2, 0), (2, 1), (2, 2), (0, 3), (1, 3), (2, 3)]
    order += [(3, which) for which in range(4)]
    opens = {0: 0, 1: 1, 6: 2, 12: 3}
    settles = {2: 0, 3: 1, 6: 2, 7: 3, 8: 4, 9: 5, 10: 6, 12: 7, 13: 8, 15: 9}
    held = len(settles)
    whole_column = layer > 0

    def kernel(*refs):
        lens_ref, q_ref, m_ref, kv_ref, x_ref, wo_ref, first_ref = refs[:7]
        at = 7
        column_ref = refs[at]
        at += 1
        if not last:
            w_kv_ref, wi_ref = refs[at:at + 2]
            at += 2
        y_ref, pool_ref = refs[at:at + 2]
        at += 2
        if not last:
            par_ref, in_column_ref = refs[at:at + 2]
            at += 2
        (wbuf, obuf, kvb, mbuf, xb, zb, zr, z_stage, s_ref, mx_ref, sum_ref, acc_ref,
         send, recv, w_local, in_send, in_recv, z_send, z_recv, y_send, y_recv, y_save, x_sem, m_sem, local) = refs[at:]

        place = Place(n_data, n_model, partner, neighbour)
        place.meet()
        w = GatherOut(place, wbuf, wo_ref.at[layer], send, recv, w_local, first_ref, column_ref, pool_ref, whole_column)

        def tile_of(k):
            which = pick(k, [one for _, one in order])
            slot = jnp.where(which == 0, place.y, jnp.where(which == 1, place.down, jnp.where(which == 2, place.up, place.far)))
            return pick(k, [one for one, _ in order]), which, slot

        def whole(ref, chunk, slot):
            return ref.at[pl.ds(pl.multiple_of(chunk * crow, crow), crow), pl.ds(pl.multiple_of(slot * out_part, out_part), out_part)]

        load_q = pltpu.make_async_copy(q_ref, obuf, local.at[0])
        load_kv = pltpu.make_async_copy(kv_ref, kvb, local.at[1])

        def load_m(k):
            chunk, _, _ = tile_of(k)
            slot = lax.rem(k, 2)
            return pltpu.make_async_copy(
                m_ref.at[:, :, :, pl.ds(pl.multiple_of(chunk * crow, crow), crow)], mbuf.at[slot], m_sem.at[slot]
            )

        def load_x(k):
            chunk, _, slot = tile_of(k)
            src = x_ref.at[chunk, slot] if tiled else whole(x_ref, chunk, slot)
            return pltpu.make_async_copy(src, xb.at[chunk, slot], x_sem.at[k])

        def c_z(k):
            chunk, _, slot = tile_of(k)
            return remote(z_stage.at[lax.rem(k, 4)], zr.at[chunk, slot], z_send.at[k], z_recv.at[k], {"model": place.partner})

        def c_y(k):
            chunk, _, slot = tile_of(k)
            target = {"model": next_partner(place.me)}
            return remote(xb.at[chunk, slot], par_ref.at[chunk, slot], y_send.at[k], y_recv.at[k], target)

        def save_y(k):
            chunk, _, slot = tile_of(k)
            dst = whole(y_ref, chunk, slot) if last else y_ref.at[chunk, slot]
            return pltpu.make_async_copy(xb.at[chunk, slot], dst, y_save.at[k])

        load_q.start()
        load_kv.start()
        load_m(0).start()
        w.load_own().start()
        w.load_first().start()
        w.mate(0).start()
        w.side_mate(0).start()
        for which in range(1, 4 if whole_column else 3):
            w.load_column(which).start()
            w.mate(which).start()
        w.side_up().start()
        w.side_down().start()
        if whole_column:
            w.far().start()
        else:
            w.forward().start()
            w.forward_b().start()
        if not last:
            in_own = in_halves(layer + 1, w_kv_ref, wi_ref, c, ff)
            in_next = FetchIn(place, in_own, in_send, in_recv, column=in_column_ref)
            for g in range(2):
                for half in range(2):
                    in_next.up(g, half).start()
                    in_next.down(g, half).start()

        @pl.loop(0, tiles)
        def _(k):
            load_x(k).start()

        load_q.wait()
        load_kv.wait()

        def attend_one(batch, side):
            slab = jnp.where(side == 0, place.me, place.partner)
            length = lens_ref[batch]
            n_key = slab // 2 + 1
            at_row = pl.ds(pl.multiple_of(batch * slab_len, slab_len), slab_len)
            parts = []
            for blk in range(n_blocks):
                for one in range(2):
                    parts.append(obuf[blk, side, at_row, one * head_dim:(one + 1) * head_dim])
            q_val = jnp.concatenate(parts, axis=0)
            row_pos = slab * slab_len + lax.rem(lax.broadcasted_iota(jnp.int32, (qrows, key_rows), 0), slab_len)
            key_pos = lax.broadcasted_iota(jnp.int32, (qrows, key_rows), 1)
            room = jnp.minimum(row_pos + 1, length) - key_pos
            mx_ref[...] = jnp.full_like(mx_ref, -1e30)

            def score(kb, carry):
                k = kvb[pl.ds(2 * kb, 2), at_row, :head_dim].reshape(key_rows, head_dim)
                s = lax.dot_general(q_val, k, (((1,), (1,)), ((), ())), preferred_element_type=F32) * scale
                s = jnp.where(room > kb * key_rows, s, -1e30)
                s_ref[kb] = s
                mx_ref[...] = jnp.maximum(mx_ref[...], jnp.maximum(s[:, :slab_len], s[:, slab_len:]))
                return carry

            lax.fori_loop(0, n_key, score, 0)
            top = jnp.max(mx_ref[...], axis=-1, keepdims=True)
            mx_ref[...] = jnp.broadcast_to(top, mx_ref.shape)
            sum_ref[...] = jnp.zeros_like(sum_ref)
            acc_ref[...] = jnp.zeros_like(acc_ref)

            def weigh(kb, carry):
                v = kvb[pl.ds(2 * kb, 2), at_row, head_dim:].reshape(key_rows, head_dim)
                top_b = mx_ref[...]
                e_lo = jnp.exp2(s_ref[kb, :, :slab_len] - top_b)
                e_hi = jnp.exp2(s_ref[kb, :, slab_len:] - top_b)
                sum_ref[...] += e_lo + e_hi
                e = jnp.concatenate([e_lo, e_hi], axis=1).astype(BF16)
                acc_ref[...] += jnp.dot(e, v, preferred_element_type=F32)
                return carry

            lax.fori_loop(0, n_key, weigh, 0)
            out = (acc_ref[...] / jnp.sum(sum_ref[...], axis=-1, keepdims=True)).astype(BF16)
            for blk in range(n_blocks):
                for one in range(2):
                    first_row = (blk * 2 + one) * slab_len
                    obuf[blk, side, at_row, one * head_dim:(one + 1) * head_dim] = out[first_row:first_row + slab_len]

        def settle(k):
            chunk, _, slot = tile_of(k)
            load_x(k).wait()
            c_z(k).wait_recv()
            z = zb[chunk, slot].astype(F32) + zr[chunk, slot].astype(F32)
            xb[chunk, slot] = (xb[chunk, slot].astype(F32) + z).astype(BF16)
            save_y(k).start()
            if not last:
                c_y(k).start()

        @pl.loop(0, tiles)
        def _(step):
            chunk, which, slot = tile_of(step)

            @pl.when(step + 1 < tiles)
            def _():
                load_m(step + 1).start()

            opening = functools.reduce(lambda one, other: one | other, [step == at for at in opens])

            @pl.when(opening)
            def _():
                with jax.named_scope("b_attn"):
                    @pl.loop(0, 2 * n_seq)
                    def _(unit):
                        attend_one(chunk * n_seq + unit // 2, lax.rem(unit, 2))

            @pl.when(step == 0)
            def _():
                with jax.named_scope("b_w0"):
                    w.load_own().wait()
                    w.load_first().wait()
                    w.take(0)
                    w.load_mate(0).wait()
                    w.load_side(0).wait()

            @pl.when(step == 1)
            def _():
                with jax.named_scope("b_s1"):
                    w.side_up().wait_recv()
                    w.side_mate(1).start()
                    w.side_down().wait_recv()
                    w.side_mate(2).start()

            @pl.when(step == 2)
            def _():
                with jax.named_scope("b_s2"):
                    for one in (1, 2):
                        w.take(one)
                    for one in (1, 2):
                        w.load_column(one).wait()
                        w.load_mate(one).wait()
                        w.load_side(one).wait()

            if not whole_column:

                @pl.when(step == 4)
                def _():
                    with jax.named_scope("b_s4"):
                        w.forward().wait_recv()
                        w.forward_b().wait_recv()
                        w.far().start()
                        w.mate(3).start()

            @pl.when(step == 8)
            def _():
                with jax.named_scope("b_s8"):
                    w.far().wait_recv()
                    w.side_mate(3).start()

            @pl.when(step == 9)
            def _():
                with jax.named_scope("b_s9"):
                    w.take(3)
                    if whole_column:
                        w.load_column(3).wait()
                    w.load_mate(3).wait()
                    w.load_side(3).wait()

            if not last:
                for g, at in enumerate((6, 12)):

                    @pl.when(step == at)
                    def _(g=g):
                        with jax.named_scope("b_ring"):
                            in_next.ring_stage(g, n_group)

            @pl.when(step >= 4)
            def _():
                with jax.named_scope("b_zsend"):
                    c_z(step - 4).wait_send()

            with jax.named_scope("b_mwait"):
                load_m(step).wait()
            here = lax.rem(step, 2)
            rows_c = pl.ds(pl.multiple_of(chunk * crow, crow), crow)
            with jax.named_scope("b_dot"):
                total = None
                for blk in range(n_blocks):
                    mid = jnp.concatenate([mbuf[here, blk, :, k].reshape(2 * crow, c) for k in range(n_mid)], axis=1)
                    attn = obuf[blk, :, rows_c, :].reshape(2 * crow, c)
                    one = jnp.dot(mid, wbuf[blk, slot, c:, :], preferred_element_type=F32)
                    one = one + jnp.dot(attn, wbuf[blk, slot, :c, :], preferred_element_type=F32)
                    total = one if total is None else total + one
                z = total.astype(BF16)
                zb[chunk, slot] = z[:crow]
                z_stage[lax.rem(step, 4)] = z[crow:]
            c_z(step).start()

            settling = functools.reduce(lambda one, other: one | other, [step == at for at in settles])

            @pl.when(settling)
            def _():
                with jax.named_scope("b_settle"):
                    settle(pick(step, [sum(1 for at in settles if at < k) for k in range(tiles)]))

        stages = list(range(2, n_group)) if not last else []
        for k in range(held, tiles):
            if stages and (k - held) % 2 == 0:
                with jax.named_scope("b_tailring"):
                    in_next.ring_stage(stages.pop(0), n_group)
            with jax.named_scope("b_tail"):
                settle(k)
        for g in stages:
            with jax.named_scope("b_tailring"):
                in_next.ring_stage(g, n_group)

        @pl.loop(0, tiles)
        def _(k):
            save_y(k).wait()
            if not last:
                c_y(k).wait()

        @pl.loop(tiles - 4, tiles)
        def _(k):
            with jax.named_scope("b_tailz"):
                c_z(k).wait_send()

        made = [w.side_up(), w.side_down(), w.far()]
        made += [w.mate(which) for which in range(4)] + [w.side_mate(which) for which in range(4)]
        if not whole_column:
            made += [w.forward(), w.forward_b()]
        for copy in made:
            copy.wait_send()
        if not last:

            @pl.loop(0, n_group)
            def _(g):
                for half in range(2):
                    in_next.forward(g, half).wait()
                    in_next.up(g, half).wait_send()
                    in_next.down(g, half).wait_send()

    anywhere = pl.BlockSpec(memory_space=pl.ANY)
    args = [lens, q, m, kv, x_own, w_out, first, column]
    if not last:
        args += [w_kv, w_in]
    tile = (chunks, n_data, crow, out_part)
    out_shape = [
        jax.ShapeDtypeStruct((rows, d_model) if last else tile, BF16),
        jax.ShapeDtypeStruct((2, n_data, depth, out_part), BF16),
    ]
    if not last:
        out_shape += [
            jax.ShapeDtypeStruct(tile, BF16),
            jax.ShapeDtypeStruct((n_group, n_data, 2, part, c), BF16),
        ]
    dma = pltpu.SemaphoreType.DMA
    return pl.pallas_call(
        kernel,
        out_shape=out_shape,
        in_specs=[pl.BlockSpec(memory_space=pltpu.SMEM)] + [anywhere] * (len(args) - 1),
        out_specs=[anywhere] * len(out_shape),
        scratch_shapes=[
            pltpu.VMEM((n_blocks, n_data, depth, out_part), BF16),
            pltpu.VMEM(q.shape, BF16),
            pltpu.VMEM(kv.shape, BF16),
            pltpu.VMEM((2, n_blocks, 2, n_mid, crow, c), BF16),
            pltpu.VMEM(tile, BF16),
            pltpu.VMEM(tile, BF16),
            pltpu.VMEM(tile, BF16),
            pltpu.VMEM((4, crow, out_part), BF16),
            pltpu.VMEM((n_model // 2, qrows, key_rows), F32),
            pltpu.VMEM((qrows, slab_len), F32),
            pltpu.VMEM((qrows, slab_len), F32),
            pltpu.VMEM((qrows, head_dim), F32),
            dma((SIDE_MATE + 7,)), dma((SIDE_MATE + 7,)), dma((13,)), dma((3, 2 * n_group)), dma((3, 2 * n_group)),
            dma((tiles,)), dma((tiles,)), dma((tiles,)), dma((tiles,)), dma((tiles,)), dma((tiles,)), dma((2,)), dma((2,)),
        ],
        compiler_params=pltpu.CompilerParams(collective_id=2 * layer + 1, has_side_effects=True, vmem_limit_bytes=VMEM_LIMIT),
        cost_estimate=pl.CostEstimate(flops=4 * rows * n_blocks * depth * d_model, bytes_accessed=16 * rows * d_model, transcendentals=0),
        name=f"attend_and_sum_{layer}",
    )(*args)


def solution(mesh):
    batch_axes = ("rep", "data")
    n_data, n_model = mesh.shape["data"], mesh.shape["model"]
    n_chip = n_model // 2

    def near(x):
        return x + 1 - 2 * (x % 2)

    def across(x):
        return n_chip - 1 - x

    def on_chip(other):
        return lambda m: 2 * other(m // 2) + m % 2

    def local_step(x_loc, lens_loc, gamma_loc, w_in_loc, w_kv_loc, w_out_loc):
        n_batch, slab_len, d_model = x_loc.shape
        n_layers, part = gamma_loc.shape
        partners = [on_chip(near if layer % 2 == 0 else across) for layer in range(n_layers)]
        neighbours = [on_chip(across if layer % 2 == 0 else near) for layer in range(n_layers)]

        gain_rows = jnp.zeros((8, part), F32).at[:n_layers].set(gamma_loc.astype(F32))
        own = x_loc.reshape(n_batch * slab_len, d_model)
        for layer in range(n_layers):
            last = layer + 1 == n_layers
            following = min(layer + 1, n_layers - 1)
            if layer == 0:
                extra = (gain_rows,)
                q, m, kv, _, gains, out_first, out_column, in_first = project(
                    layer, n_data, n_model, partners[layer], neighbours[layer], neighbours[following],
                    own, w_kv_loc, w_in_loc, w_out_loc, extra,
                )
            else:
                extra = (other, gains, in_first, in_column)
                q, m, kv, _, out_first, out_column = project(
                    layer, n_data, n_model, partners[layer], neighbours[layer], neighbours[following],
                    own, w_kv_loc, w_in_loc, w_out_loc, extra,
                )
            outs = attend_and_sum(
                layer, last, n_data, n_model, partners[layer], neighbours[layer], partners[following],
                lens_loc, q, m, kv, own, w_in_loc, w_out_loc, w_kv_loc, out_first, out_column,
            )
            own = outs[0]
            if not last:
                other, in_column = outs[2:]
        return own.reshape(n_batch, slab_len, d_model)

    in_specs = (
        P(batch_axes, "model", None),
        P(batch_axes),
        P(None, "data"),
        P(None, "data", "model"),
        P(None, "data", None),
        P(None, "model", "data"),
    )
    return jax.shard_map(local_step, mesh=mesh, in_specs=in_specs, out_specs=P(batch_axes, "model", None), check_vma=False)
```

```python
import functools

import jax
import jax.numpy as jnp
from jax import lax
from jax.experimental import pallas as pl
from jax.experimental.pallas import tpu as pltpu
from jax.sharding import PartitionSpec as P

EPSILON = 1e-6
VMEM_LIMIT = 66_000_000
MESH = pl.DeviceIdType.MESH
BF16, F32 = jnp.bfloat16, jnp.float32

UP, DOWN, FORWARD, FORWARD_B, FIRST, SIDE_UP, SIDE_DOWN, FAR, MATE, SIDE_MATE = range(10)


def rms_norm(x_in, gain):
    x_f32 = x_in.astype(F32)
    inv_rms = lax.rsqrt(jnp.mean(x_f32 * x_f32, axis=-1, keepdims=True) + EPSILON)
    return (x_f32 * inv_rms * gain.astype(F32)).astype(BF16)


class Place:
    def __init__(self, n_data, n_model, partner, neighbour):
        self.n_data, self.n_model = n_data, n_model
        self.y = lax.axis_index("data")
        self.me = lax.axis_index("model")
        self.up = lax.rem(self.y + 1, n_data)
        self.down = lax.rem(self.y + n_data - 1, n_data)
        self.far = lax.rem(self.y + 2, n_data)
        self.slots = (self.y, self.down, self.up, self.far)
        self.mate = self.me + 1 - 2 * lax.rem(self.me, 2)
        self.partner, self.neighbour = partner(self.me), neighbour(self.me)
        n_other = n_model // 2 - 1
        self.ahead = [lax.rem(self.me + 2 * k, n_model) for k in range(1, n_other + 1)]
        self.behind = [lax.rem(self.me + n_model - 2 * k, n_model) for k in range(1, n_other + 1)]

    def meet(self):
        barrier = pltpu.get_barrier_semaphore()
        targets = [{"data": self.up}, {"data": self.down}, {"data": self.far}, {"model": self.mate}]
        targets += [{"model": m} for m in self.ahead]
        for target in targets:
            pl.semaphore_signal(barrier, inc=1, device_id=target, device_id_type=MESH)
        pl.semaphore_wait(barrier, len(targets))


def remote(src, dst, send, recv, target):
    return pltpu.make_async_remote_copy(
        src_ref=src, dst_ref=dst, send_sem=send, recv_sem=recv, device_id=target, device_id_type=MESH
    )


class GatherIn:
    def __init__(self, place, buf, pool, own, send, recv, local, first=None, column=None):
        self.place, self.buf, self.pool, self.own, self.first, self.column = place, buf, pool, own, first, column
        self.send, self.recv, self.local = send, recv, local

    def at(self, block, g, slot):
        return self.buf.at[block, g, slot]

    def _copy(self, src, dst, kind, at, target):
        return remote(src, dst, self.send.at[kind, at], self.recv.at[kind, at], target)

    def up(self, g, half):
        dst = self.at(0, g, self.place.y).at[half]
        return self._copy(self.own(g, half), dst, UP, 2 * g + half, {"data": self.place.up})

    def down(self, g, half):
        dst = self.at(0, g, self.place.y).at[half]
        return self._copy(self.own(g, half), dst, DOWN, 2 * g + half, {"data": self.place.down})

    def neighbour_first(self, g, half):
        dst = self.at(2, g, self.place.y).at[half]
        return self._copy(self.own(g, half), dst, FIRST, 2 * g + half, {"model": self.place.neighbour})

    def forward(self, g, half):
        ref = self.at(0, g, (self.place.down, self.place.up)[half]).at[half]
        target = (self.place.up, self.place.down)[half]
        return self._copy(ref, ref, FORWARD, 2 * g + half, {"data": target})

    def _needed(self, ref, g):
        return ref.at[0] if isinstance(g, int) and g == 0 else ref

    def _side(self, g, kind, target):
        src = self.at(2, g, self.place.y) if self.first is None else self.first.at[g]
        dst = self.at(2, g, self.place.y)
        return self._copy(self._needed(src, g), self._needed(dst, g), kind, g, {"data": target})

    def side_up(self, g):
        return self._side(g, SIDE_UP, self.place.up)

    def side_down(self, g):
        return self._side(g, SIDE_DOWN, self.place.down)

    def far(self, g):
        slot = self.place.far
        src = self.at(0, g, slot) if self.column is None else self.column.at[g, slot]
        dst = self.at(2, g, slot)
        return self._copy(self._needed(src, g), self._needed(dst, g), FAR, g, {"model": self.place.neighbour})

    def mate(self, g):
        return self._copy(self.buf.at[0, g], self.pool.at[0, g], MATE, g, {"model": self.place.mate})

    def side_mate(self, g):
        src, dst = self.buf.at[2, g], self.pool.at[1, g]
        if isinstance(g, int) and g == 0:
            src, dst = src.at[:, 0], dst.at[:, 0]
        return self._copy(src, dst, SIDE_MATE, g, {"model": self.place.mate})

    def load_mate(self, g):
        return pltpu.make_async_copy(self.pool.at[0, g], self.buf.at[1, g], self.local.at[6, g])

    def load_side(self, g):
        src, dst = self.pool.at[1, g], self.buf.at[3, g]
        if isinstance(g, int) and g == 0:
            src, dst = src.at[:, 0], dst.at[:, 0]
        return pltpu.make_async_copy(src, dst, self.local.at[7, g])

    def take_mate(self, g):
        self.mate(g).wait_recv()
        self.load_mate(g).start()

    def take_side(self, g):
        self.side_mate(g).wait_recv()
        self.load_side(g).start()

    def load_own(self, g, half):
        dst = self.at(0, g, self.place.y).at[half]
        return pltpu.make_async_copy(self.own(g, half), dst, self.local.at[half, g])

    def load_column(self, g, which):
        slot = self.place.slots[which]
        return pltpu.make_async_copy(self.column.at[g, slot], self.at(0, g, slot), self.local.at[1 + which, g])

    def load_first(self, g):
        return pltpu.make_async_copy(self.first.at[g], self.at(2, g, self.place.y), self.local.at[5, g])

    def pass_side(self, g):
        if self.first is not None:
            self.load_first(g).wait()
        self.side_up(g).wait_recv()
        self.side_down(g).wait_recv()
        self.far(g).wait_recv()
        self.side_mate(g).start()

    def wait_sends(self, g):
        made = [self.side_up(g), self.side_down(g), self.far(g), self.mate(g), self.side_mate(g)]
        if self.column is None:
            made += [copy(g, half) for copy in (self.up, self.down, self.forward) for half in range(2)]
        if self.first is None:
            made += [self.neighbour_first(g, half) for half in range(2)]
        for copy in made:
            copy.wait_send()


class FetchIn:
    def __init__(self, place, own, send, recv, neighbour=None, first=None, column=None):
        self.place, self.own, self.send, self.recv = place, own, send, recv
        self.neighbour, self.first, self.column = neighbour, first, column

    def _ring(self, g, half, kind, target):
        at = 2 * g + half
        dst = self.column.at[g, self.place.y, half]
        return remote(self.own(g, half), dst, self.send.at[kind, at], self.recv.at[kind, at], {"data": target})

    def up(self, g, half):
        return self._ring(g, half, 0, self.place.up)

    def down(self, g, half):
        return self._ring(g, half, 1, self.place.down)

    def forward(self, g, half):
        at = 2 * g + half
        ref = self.column.at[g, (self.place.down, self.place.up)[half], half]
        target = (self.place.up, self.place.down)[half]
        return remote(ref, ref, self.send.at[2, at], self.recv.at[2, at], {"data": target})

    def ring_stage(self, g):
        for half in range(2):
            self.up(g, half).wait_recv()
            self.down(g, half).wait_recv()
        for half in range(2):
            self.forward(g, half).start()

    def send_slices(self, g):
        for half in range(2):
            self.up(g, half).start()
            self.down(g, half).start()

    def neighbour_first(self, g, half):
        at = 2 * g + half
        dst = self.first.at[g, half]
        return remote(self.own(g, half), dst, self.send.at[3, at], self.recv.at[3, at], {"model": self.neighbour})


class GatherOut:
    def __init__(self, place, buf, own, send, recv, local=None, first=None, column=None, pool=None, whole_column=True):
        self.place, self.buf, self.own, self.first, self.column = place, buf, own, first, column
        self.far_held = column is not None and whole_column
        self.send, self.recv, self.local, self.pool = send, recv, local, pool

    def _copy(self, src, dst, kind, target):
        return remote(src, dst, self.send.at[kind], self.recv.at[kind], target)

    def up(self):
        return self._copy(self.own, self.buf.at[0, self.place.y], UP, {"data": self.place.up})

    def down(self):
        return self._copy(self.own, self.buf.at[0, self.place.y], DOWN, {"data": self.place.down})

    def _half(self, ref, second):
        size = ref.shape[0] // 2
        return ref.at[pl.ds(second * size, size)]

    def _forward(self, kind, slot, second, target):
        src = self.buf if self.column is None else self.column
        dst = self._half(self.buf.at[0, slot], second)
        return self._copy(self._half(src.at[0, slot], second), dst, kind, {"data": target})

    def forward(self):
        return self._forward(FORWARD, self.place.down, 0, self.place.up)

    def forward_b(self):
        return self._forward(FORWARD_B, self.place.up, 1, self.place.down)

    def neighbour_first(self, dst):
        return self._copy(self.own, dst, FIRST, {"model": self.place.neighbour})

    def side_up(self):
        return self._copy(self.first, self.buf.at[2, self.place.y], SIDE_UP, {"data": self.place.up})

    def side_down(self):
        return self._copy(self.first, self.buf.at[2, self.place.y], SIDE_DOWN, {"data": self.place.down})

    def far(self):
        slot = self.place.far
        src = self.column.at[0, slot] if self.far_held else self.buf.at[0, slot]
        return self._copy(src, self.buf.at[2, slot], FAR, {"model": self.place.neighbour})

    def mate(self, which):
        slot = self.place.slots[which]
        if which == 0:
            src = self.own
        else:
            src = self.column.at[0, slot] if which < 3 or self.far_held else self.buf.at[0, slot]
        return self._copy(src, self.pool.at[0, slot], MATE + 2 * which, {"model": self.place.mate})

    def side_mate(self, which):
        slot = self.place.slots[which]
        src = self.first if which == 0 else self.buf.at[2, slot]
        return self._copy(src, self.pool.at[1, slot], SIDE_MATE + 2 * which, {"model": self.place.mate})

    def load_mate(self, which):
        slot = self.place.slots[which]
        return pltpu.make_async_copy(self.pool.at[0, slot], self.buf.at[1, slot], self.local.at[5 + which])

    def load_side(self, which):
        slot = self.place.slots[which]
        return pltpu.make_async_copy(self.pool.at[1, slot], self.buf.at[3, slot], self.local.at[9 + which])

    def take(self, which):
        self.mate(which).wait_recv()
        self.load_mate(which).start()
        self.side_mate(which).wait_recv()
        self.load_side(which).start()

    def load_own(self):
        return pltpu.make_async_copy(self.own, self.buf.at[0, self.place.y], self.local.at[0])

    def load_column(self, which):
        slot = self.place.slots[which]
        return pltpu.make_async_copy(self.column.at[0, slot], self.buf.at[0, slot], self.local.at[which])

    def load_first(self):
        return pltpu.make_async_copy(self.first, self.buf.at[2, self.place.y], self.local.at[4])


def in_halves(layer, w_kv_ref, w_ref, c, ff):
    def own(g, half):
        if isinstance(g, int) and g == 0:
            return w_kv_ref.at[layer] if half else w_ref.at[layer, :, pl.ds(0, c)]
        return w_ref.at[layer, :, pl.ds(pl.multiple_of(g * c + half * ff, c), c)]

    return own


def project(layer, n_data, n_model, partner, neighbour, next_neighbour, x_own, w_kv, w_in, w_out, extra):
    start_layer = layer == 0
    part, c = w_kv.shape[1:]
    d_model = part * n_data
    rows = x_own.size // d_model
    depth, out_part = w_out.shape[1:]
    ff = depth - c
    n_group = 1 + ff // c
    n_units = 8 * n_group
    row_parts = 4
    row_part = rows // row_parts
    n_other = n_model // 2 - 1
    gain_shape = (n_data, 8, part)
    n_tiles = 1 if start_layer else x_own.shape[0] * x_own.shape[1]

    def kernel(*refs):
        x_ref, w_kv_ref, w_ref, wo_ref = refs[:4]
        if start_layer:
            gain_ref = refs[4]
            q_ref, m_ref, kv_ref, pool_ref, gains_ref, out_first_ref, out_column_ref, in_first_ref = refs[5:13]
            first_ref = column_ref = None
            rest = refs[13:]
        else:
            par_ref, gain_ref, first_ref, column_ref = refs[4:8]
            q_ref, m_ref, kv_ref, pool_ref, out_first_ref, out_column_ref = refs[8:14]
            rest = refs[14:]
        wbuf, h_ref, gbuf, stage, kv_stage, send, recv, w_local, next_send, next_recv, late_send, late_recv = rest[:12]
        x_send, x_recv, g_send, g_recv, kv_send, kv_recv, local, out_sem, tile_sem = rest[12:]

        place = Place(n_data, n_model, partner, neighbour)
        place.meet()
        in_own = in_halves(layer, w_kv_ref, w_ref, c, ff)
        w = GatherIn(place, wbuf, pool_ref, in_own, send, recv, w_local, first_ref, column_ref)
        out_next = GatherOut(place, out_column_ref, wo_ref.at[layer], next_send, next_recv)
        if start_layer:
            in_own_next = in_halves(layer + 1, w_kv_ref, w_ref, c, ff)
            in_next = FetchIn(place, in_own_next, late_send, late_recv, next_neighbour(place.me), in_first_ref)

        def c_x(part_no):
            piece = pl.ds(part_no * row_part, row_part)
            return remote(
                x_ref.at[piece], h_ref.at[1, piece], x_send.at[part_no], x_recv.at[part_no], {"model": place.partner}
            )

        def c_gain(which):
            target = {"data": (place.up, place.down, place.far)[which]}
            return remote(gain_ref, gbuf.at[place.y], g_send.at[which], g_recv.at[which], target)

        def c_kv(which):
            ref = kv_ref.at[place.me]
            return remote(ref, ref, kv_send.at[which], kv_recv.at[which], {"model": place.ahead[which]})

        def c_kv_mate(which):
            ref = kv_ref.at[place.me if which == 0 else place.behind[which - 1]]
            at = n_other + which
            return remote(ref, ref, kv_send.at[at], kv_recv.at[at], {"model": place.mate})

        save_kv = pltpu.make_async_copy(kv_stage, kv_ref.at[place.me], local.at[0])
        if start_layer:
            load_x = pltpu.make_async_copy(x_ref, h_ref.at[0], local.at[0])

        def load_tile(side, k):
            chunk, slot = k // n_data, lax.rem(k, n_data)
            src = (x_ref, par_ref)[side].at[chunk, slot]
            height, across = src.shape
            down_to, along = pl.multiple_of(chunk * height, height), pl.multiple_of(slot * across, across)
            return pltpu.make_async_copy(src, h_ref.at[side, pl.ds(down_to, height), pl.ds(along, across)], tile_sem.at[side, k])

        if start_layer:
            load_gain = pltpu.make_async_copy(gain_ref, gbuf.at[place.y], local.at[1])
            for which in range(3):
                c_gain(which).start()
        else:
            load_gain = pltpu.make_async_copy(gain_ref, gbuf, local.at[1])
        def send_slices(g):
            for half in range(2):
                w.up(g, half).start()
                w.down(g, half).start()

        load_gain.start()
        if start_layer:
            load_x.start()
        else:
            for side in range(2):

                @pl.loop(0, n_tiles)
                def _(k):
                    load_tile(side, k).start()

        if start_layer:
            send_slices(0)
            for g in range(n_group):
                for half in range(2):
                    w.neighbour_first(g, half).start()
                    w.load_own(g, half).start()
            for part_no in range(row_parts // 2):
                c_x(part_no).start()
        else:
            for g in range(n_group):
                for half in range(2):
                    w.load_own(g, half).start()
                for which in range(1, 4):
                    w.load_column(g, which).start()
                w.side_up(g).start()
                w.side_down(g).start()
                if g < 2:
                    w.far(g).start()
            for g in range(n_group):
                w.load_first(g).start()

        def ring_stage(g):
            for half in range(2):
                w.up(g, half).wait_recv()
                w.down(g, half).wait_recv()
            for half in range(2):
                w.forward(g, half).start()

        def column_stage(g):
            for half in range(2):
                w.load_own(g, half).wait()
            for which in range(1, 4):
                w.load_column(g, which).wait()
            w.mate(g).start()

        if start_layer:
            for which in range(3):
                c_gain(which).wait_recv()
        load_gain.wait()
        gain = jnp.concatenate([gbuf[k, layer:layer + 1, :] for k in range(n_data)], axis=1)
        if start_layer:
            save_gain = pltpu.make_async_copy(gbuf, gains_ref, local.at[1])
            save_gain.start()
        if start_layer:
            load_x.wait()
        else:

            @pl.loop(0, n_tiles)
            def _(k):
                load_tile(0, k).wait()

        def norm_rows(side, part_no):
            piece = pl.ds(part_no * row_part, row_part)
            h_ref[side, piece] = rms_norm(h_ref[side, piece], gain)

        @pl.loop(0, row_parts)
        def _(part_no):
            norm_rows(0, part_no)

        if start_layer:
            send_slices(1)
            ring_stage(0)
        else:
            column_stage(0)

        halfway, quarter = n_units // 2, n_units // 4

        def out_copy(slot, blk, side, g):
            def to_q():
                return pltpu.make_async_copy(stage.at[slot], q_ref.at[blk, side], out_sem.at[slot])

            def to_m():
                return pltpu.make_async_copy(stage.at[slot], m_ref.at[blk, side, g - 1], out_sem.at[slot])

            return to_q, to_m

        @pl.loop(0, n_units)
        def _(step):
            late = step - halfway
            if start_layer:
                opening, second = step < quarter, (step >= quarter) & (step < halfway)
                ahead = (step == 0) | ((lax.rem(step, 2) == 1) & (step < quarter - 1))
                open_g = jnp.where(ahead, (step + 1) // 2, jnp.where(step == quarter - 1, n_group - 1, step // 2 - 1))
                g = jnp.where(opening, open_g, jnp.where(second, (step - quarter) // 2, late // 4))
                open_blk = jnp.where(ahead, 0, 1)
                blk = jnp.where(opening, open_blk, jnp.where(second, lax.rem(step, 2), 2 + lax.rem(late, 4) // 2))
                side = jnp.where(opening, 0, jnp.where(second, 1, lax.rem(late, 2)))

                @pl.when(opening & (blk == 0))
                def _():
                    with jax.named_scope("a_ring"):
                        for half in range(2):
                            w.forward(g, half).wait_recv()

                        @pl.when(g + 2 < n_group)
                        def _():
                            send_slices(g + 2)

                        @pl.when(g + 1 < n_group)
                        def _():
                            ring_stage(g + 1)

                        @pl.when(g + 2 == n_group)
                        def _():
                            for k in range(n_group):
                                for half in range(2):
                                    w.neighbour_first(k, half).wait_recv()
                                w.side_up(k).start()
                                w.side_down(k).start()

                        @pl.when(g == 0)
                        def _():
                            w.far(0).start()

                        @pl.when(g > 0)
                        def _():
                            w.far(g).start()

                        @pl.when(g == 1)
                        def _():
                            for part_no in range(row_parts // 2, row_parts):
                                c_x(part_no).start()

                        for half in range(2):
                            w.load_own(g, half).wait()
                        w.mate(g).start()

                        @pl.when(g > 0)
                        def _():
                            w.take_mate(g - 1)

                @pl.when(step == quarter - 2)
                def _():
                    with jax.named_scope("a_take_last"):
                        w.take_mate(n_group - 1)

                @pl.when(opening & (blk == 1))
                def _():
                    with jax.named_scope("a_load_mate"):
                        w.load_mate(g).wait()

                @pl.when(step == quarter)
                def _():
                    with jax.named_scope("a_par"):
                        @pl.loop(0, row_parts)
                        def _(part_no):
                            c_x(part_no).wait_recv()
                            norm_rows(1, part_no)

                        out_next.neighbour_first(out_first_ref).start()
                        out_next.up().start()
                        out_next.down().start()
                        for k in range(n_group):
                            for half in range(2):
                                in_next.neighbour_first(k, half).start()
            else:
                g = jnp.where(late < 0, step, late) // 4
                blk = jnp.where(late < 0, 0, 2) + lax.rem(step, 4) // 2
                side = lax.rem(step, 2)

                @pl.when((late < 0) & (lax.rem(step, 4) == 0) & (g + 1 < n_group))
                def _():
                    with jax.named_scope("a_col"):
                        column_stage(g + 1)

                @pl.when(step == 1)
                def _():
                    with jax.named_scope("a_par1"):
                        @pl.loop(0, n_tiles)
                        def _(k):
                            load_tile(1, k).wait()

                        @pl.loop(0, row_parts)
                        def _(part_no):
                            norm_rows(1, part_no)

                @pl.when((late < 0) & (lax.rem(step, 4) == 1))
                def _():
                    with jax.named_scope("a_take_mate"):
                        w.take_mate(g)

                @pl.when((late < 0) & (lax.rem(step, 4) == 2))
                def _():
                    with jax.named_scope("a_wait_mate"):
                        w.load_mate(g).wait()

                @pl.when(step == n_units - 6)
                def _():
                    with jax.named_scope("a_next"):
                        out_next.up().wait_recv()
                        out_next.down().wait_recv()
                        out_next.forward().start()
                        out_next.forward_b().start()

            @pl.when(step == halfway - 2)
            def _():
                with jax.named_scope("a_pass0"):
                    w.pass_side(0)

            @pl.when(step == halfway + 1)
            def _():
                w.take_side(0)

            @pl.when((late > 1) & (lax.rem(late, 4) == 1))
            def _():
                w.take_side(g)

            @pl.when((late >= 0) & (lax.rem(late, 4) == 2))
            def _():
                with jax.named_scope("a_pass_side"):
                    @pl.when(g + 1 < n_group)
                    def _():
                        w.pass_side(g + 1)

                    @pl.when(g == 0)
                    def _():
                        w.load_side(0).wait()

                    @pl.when(g > 0)
                    def _():
                        w.load_side(g).wait()

            slot = lax.rem(step, 2)
            to_q, to_m = out_copy(slot, blk, side, g)

            @pl.when(step >= 2)
            def _():
                with jax.named_scope("a_outwait"):
                    to_q().wait()

            def columns(half):
                return wbuf[blk, g, :, half].reshape(d_model, c)

            @pl.when(g == 0)
            def _():
                with jax.named_scope("a_unit_q"):
                    q = jnp.dot(h_ref[side], columns(0), preferred_element_type=F32)
                    stage[slot] = q.astype(BF16)
                    to_q().start()

            @pl.when(g > 0)
            def _():
                with jax.named_scope("a_unit_m"):
                    h_val = h_ref[side]
                    gate = jnp.dot(h_val, columns(0), preferred_element_type=F32).astype(BF16).astype(F32)
                    raised = jnp.dot(h_val, columns(1), preferred_element_type=F32).astype(BF16).astype(F32)
                    stage[slot] = (gate * jax.nn.sigmoid(gate) * raised).astype(BF16)
                    to_m().start()

            @pl.when(step == 0)
            def _():
                kv_stage[...] = jnp.dot(h_ref[0], columns(1), preferred_element_type=F32).astype(BF16)
                save_kv.start()

            @pl.when(step == 1)
            def _():
                with jax.named_scope("a_kv1"):
                    save_kv.wait()
                    for which in range(n_other):
                        c_kv(which).start()
                    c_kv_mate(0).start()
                    if not start_layer:
                        for k in range(2, n_group):
                            w.far(k).start()

            if not start_layer:

                @pl.when(step == 8)
                def _():
                    with jax.named_scope("b_s8"):
                        out_next.up().start()
                        out_next.down().start()
                        out_next.neighbour_first(out_first_ref).start()

        for which in range(n_other):
            c_kv(which).wait_recv()
            c_kv_mate(1 + which).start()
        for which in range(n_other + 1):
            c_kv_mate(which).wait()
        for which in range(n_other):
            c_kv(which).wait_send()
        if start_layer:
            save_gain.wait()
            for which in range(3):
                c_gain(which).wait_send()
            for part_no in range(row_parts):
                c_x(part_no).wait_send()
            for g in range(n_group):
                for half in range(2):
                    in_next.neighbour_first(g, half).wait()
            for copy in (out_next.up(), out_next.down()):
                copy.wait()
        else:
            for copy in (out_next.forward(), out_next.forward_b()):
                copy.wait()
            for copy in (out_next.up(), out_next.down()):
                copy.wait_send()
        out_next.neighbour_first(out_first_ref).wait()
        for slot in range(2):
            pltpu.make_async_copy(stage.at[slot], q_ref.at[0, 0], out_sem.at[slot]).wait()

        for g in range(n_group):
            w.wait_sends(g)

    anywhere = pl.BlockSpec(memory_space=pl.ANY)
    out_shape = [
        jax.ShapeDtypeStruct((4, 2, rows, c), BF16),
        jax.ShapeDtypeStruct((4, 2, n_group - 1, rows, c), BF16),
        jax.ShapeDtypeStruct((n_model, rows, c), BF16),
        jax.ShapeDtypeStruct((2, n_group, n_data, 2, part, c), BF16),
    ]
    if start_layer:
        out_shape += [
            jax.ShapeDtypeStruct(gain_shape, F32),
            jax.ShapeDtypeStruct((depth, out_part), BF16),
            jax.ShapeDtypeStruct((1, n_data, depth, out_part), BF16),
            jax.ShapeDtypeStruct((n_group, 2, part, c), BF16),
        ]
    else:
        out_shape += [
            jax.ShapeDtypeStruct((depth, out_part), BF16),
            jax.ShapeDtypeStruct((1, n_data, depth, out_part), BF16),
        ]
    dma = pltpu.SemaphoreType.DMA
    args = (x_own, w_kv, w_in, w_out) + tuple(extra)
    return pl.pallas_call(
        kernel,
        out_shape=out_shape,
        in_specs=[anywhere] * len(args),
        out_specs=[anywhere] * len(out_shape),
        scratch_shapes=[
            pltpu.VMEM((4, n_group, n_data, 2, part, c), BF16),
            pltpu.VMEM((2, rows, d_model), BF16),
            pltpu.VMEM(gain_shape, F32),
            pltpu.VMEM((2, rows, c), BF16),
            pltpu.VMEM((rows, c), BF16),
            dma((SIDE_MATE + 1, 2 * n_group)), dma((SIDE_MATE + 1, 2 * n_group)), dma((8, n_group)),
            dma((FIRST + 1,)), dma((FIRST + 1,)), dma((4, 2 * n_group)), dma((4, 2 * n_group)),
            dma((row_parts,)), dma((row_parts,)), dma((3,)), dma((3,)),
            dma((n_model - 1,)), dma((n_model - 1,)), dma((3,)), dma((2,)), dma((2, n_tiles)),
        ],
        compiler_params=pltpu.CompilerParams(collective_id=2 * layer, has_side_effects=True, vmem_limit_bytes=VMEM_LIMIT),
        cost_estimate=pl.CostEstimate(flops=4 * rows * d_model * 4 * (c + 2 * ff), bytes_accessed=16 * rows * d_model, transcendentals=0),
        name=f"project_{layer}",
    )(*args)


def pick(step, values):
    found = jnp.int32(values[0])
    for at in range(1, len(values)):
        if values[at] != values[at - 1]:
            found = jnp.where(step >= at, jnp.int32(values[at]), found)
    return found


def attend_and_sum(layer, last, n_data, n_model, partner, neighbour, next_partner, lens, q, m, kv, x_own, w_in, w_out, w_kv, first, column):
    n_blocks, _, rows, c = q.shape
    n_mid = m.shape[2]
    ff = n_mid * c
    d_model = w_out.shape[2] * n_data
    tiled = x_own.ndim == 4
    depth, out_part = w_out.shape[1:]
    head_dim = c // 2
    n_batch = lens.shape[0]
    slab_len = rows // n_batch
    chunks = 4
    n_seq = n_batch // chunks
    crow = rows // chunks
    tiles = chunks * n_data
    heads = n_blocks * 2
    qrows = heads * slab_len
    key_rows = 2 * slab_len
    scale = head_dim ** -0.5 * 1.4426950408889634
    part = w_kv.shape[1]
    n_group = 1 + ff // c
    order = [(0, 0), (1, 0), (0, 1), (1, 1), (0, 2), (1, 2), (2, 0), (2, 1), (2, 2), (0, 3), (1, 3), (2, 3)]
    order += [(3, which) for which in range(4)]
    opens = {0: 0, 1: 1, 6: 2, 12: 3}
    settles = {2: 0, 3: 1, 6: 2, 7: 3, 8: 4, 9: 5, 10: 6, 12: 7, 13: 8, 15: 9}
    held = len(settles)
    whole_column = layer > 0

    def kernel(*refs):
        lens_ref, q_ref, m_ref, kv_ref, x_ref, wo_ref, first_ref = refs[:7]
        at = 7
        column_ref = refs[at]
        at += 1
        if not last:
            w_kv_ref, wi_ref = refs[at:at + 2]
            at += 2
        y_ref, pool_ref = refs[at:at + 2]
        at += 2
        if not last:
            par_ref, in_column_ref = refs[at:at + 2]
            at += 2
        (wbuf, obuf, kvb, mbuf, xb, zb, zr, z_stage, s_ref, mx_ref, sum_ref, acc_ref,
         send, recv, w_local, in_send, in_recv, z_send, z_recv, y_send, y_recv, y_save, x_sem, m_sem, local) = refs[at:]

        place = Place(n_data, n_model, partner, neighbour)
        place.meet()
        w = GatherOut(place, wbuf, wo_ref.at[layer], send, recv, w_local, first_ref, column_ref, pool_ref, whole_column)

        def tile_of(k):
            which = pick(k, [one for _, one in order])
            slot = jnp.where(which == 0, place.y, jnp.where(which == 1, place.down, jnp.where(which == 2, place.up, place.far)))
            return pick(k, [one for one, _ in order]), which, slot

        def whole(ref, chunk, slot):
            return ref.at[pl.ds(pl.multiple_of(chunk * crow, crow), crow), pl.ds(pl.multiple_of(slot * out_part, out_part), out_part)]

        load_q = pltpu.make_async_copy(q_ref, obuf, local.at[0])
        load_kv = pltpu.make_async_copy(kv_ref, kvb, local.at[1])

        def load_m(k):
            chunk, _, _ = tile_of(k)
            slot = lax.rem(k, 2)
            return pltpu.make_async_copy(
                m_ref.at[:, :, :, pl.ds(pl.multiple_of(chunk * crow, crow), crow)], mbuf.at[slot], m_sem.at[slot]
            )

        def load_x(k):
            chunk, _, slot = tile_of(k)
            src = x_ref.at[chunk, slot] if tiled else whole(x_ref, chunk, slot)
            return pltpu.make_async_copy(src, xb.at[chunk, slot], x_sem.at[k])

        def c_z(k):
            chunk, _, slot = tile_of(k)
            return remote(z_stage.at[lax.rem(k, 4)], zr.at[chunk, slot], z_send.at[k], z_recv.at[k], {"model": place.partner})

        def c_y(k):
            chunk, _, slot = tile_of(k)
            target = {"model": next_partner(place.me)}
            return remote(xb.at[chunk, slot], par_ref.at[chunk, slot], y_send.at[k], y_recv.at[k], target)

        def save_y(k):
            chunk, _, slot = tile_of(k)
            dst = whole(y_ref, chunk, slot) if last else y_ref.at[chunk, slot]
            return pltpu.make_async_copy(xb.at[chunk, slot], dst, y_save.at[k])

        load_q.start()
        load_kv.start()
        load_m(0).start()
        w.load_own().start()
        w.load_first().start()
        w.mate(0).start()
        w.side_mate(0).start()
        for which in range(1, 4 if whole_column else 3):
            w.load_column(which).start()
            w.mate(which).start()
        w.side_up().start()
        w.side_down().start()
        if whole_column:
            w.far().start()
        else:
            w.forward().start()
            w.forward_b().start()
        if not last:
            in_own = in_halves(layer + 1, w_kv_ref, wi_ref, c, ff)
            in_next = FetchIn(place, in_own, in_send, in_recv, column=in_column_ref)

        @pl.loop(0, tiles)
        def _(k):
            load_x(k).start()

        load_q.wait()
        load_kv.wait()

        def attend_one(batch, side):
            slab = jnp.where(side == 0, place.me, place.partner)
            length = lens_ref[batch]
            n_key = slab // 2 + 1
            at_row = pl.ds(pl.multiple_of(batch * slab_len, slab_len), slab_len)
            parts = []
            for blk in range(n_blocks):
                for one in range(2):
                    parts.append(obuf[blk, side, at_row, one * head_dim:(one + 1) * head_dim])
            q_val = jnp.concatenate(parts, axis=0)
            row_pos = slab * slab_len + lax.rem(lax.broadcasted_iota(jnp.int32, (qrows, key_rows), 0), slab_len)
            key_pos = lax.broadcasted_iota(jnp.int32, (qrows, key_rows), 1)
            room = jnp.minimum(row_pos + 1, length) - key_pos
            mx_ref[...] = jnp.full_like(mx_ref, -1e30)

            def score(kb, carry):
                k = kvb[pl.ds(2 * kb, 2), at_row, :head_dim].reshape(key_rows, head_dim)
                s = lax.dot_general(q_val, k, (((1,), (1,)), ((), ())), preferred_element_type=F32) * scale
                s = jnp.where(room > kb * key_rows, s, -1e30)
                s_ref[kb] = s
                mx_ref[...] = jnp.maximum(mx_ref[...], jnp.maximum(s[:, :slab_len], s[:, slab_len:]))
                return carry

            lax.fori_loop(0, n_key, score, 0)
            top = jnp.max(mx_ref[...], axis=-1, keepdims=True)
            mx_ref[...] = jnp.broadcast_to(top, mx_ref.shape)
            sum_ref[...] = jnp.zeros_like(sum_ref)
            acc_ref[...] = jnp.zeros_like(acc_ref)

            def weigh(kb, carry):
                v = kvb[pl.ds(2 * kb, 2), at_row, head_dim:].reshape(key_rows, head_dim)
                top_b = mx_ref[...]
                e_lo = jnp.exp2(s_ref[kb, :, :slab_len] - top_b)
                e_hi = jnp.exp2(s_ref[kb, :, slab_len:] - top_b)
                sum_ref[...] += e_lo + e_hi
                e = jnp.concatenate([e_lo, e_hi], axis=1).astype(BF16)
                acc_ref[...] += jnp.dot(e, v, preferred_element_type=F32)
                return carry

            lax.fori_loop(0, n_key, weigh, 0)
            out = (acc_ref[...] / jnp.sum(sum_ref[...], axis=-1, keepdims=True)).astype(BF16)
            for blk in range(n_blocks):
                for one in range(2):
                    first_row = (blk * 2 + one) * slab_len
                    obuf[blk, side, at_row, one * head_dim:(one + 1) * head_dim] = out[first_row:first_row + slab_len]

        def settle(k):
            chunk, _, slot = tile_of(k)
            load_x(k).wait()
            c_z(k).wait_recv()
            z = zb[chunk, slot].astype(F32) + zr[chunk, slot].astype(F32)
            xb[chunk, slot] = (xb[chunk, slot].astype(F32) + z).astype(BF16)
            save_y(k).start()
            if not last:
                c_y(k).start()

        @pl.loop(0, tiles)
        def _(step):
            chunk, which, slot = tile_of(step)

            @pl.when(step + 1 < tiles)
            def _():
                load_m(step + 1).start()

            opening = functools.reduce(lambda one, other: one | other, [step == at for at in opens])

            @pl.when(opening)
            def _():
                with jax.named_scope("b_attn"):
                    @pl.loop(0, 2 * n_seq)
                    def _(unit):
                        attend_one(chunk * n_seq + unit // 2, lax.rem(unit, 2))

            @pl.when(step == 0)
            def _():
                with jax.named_scope("b_w0"):
                    w.load_own().wait()
                    w.load_first().wait()
                    w.take(0)
                    w.load_mate(0).wait()
                    w.load_side(0).wait()

            @pl.when(step == 1)
            def _():
                with jax.named_scope("b_s1"):
                    w.side_up().wait_recv()
                    w.side_mate(1).start()
                    w.side_down().wait_recv()
                    w.side_mate(2).start()

            @pl.when(step == 2)
            def _():
                with jax.named_scope("b_s2"):
                    for one in (1, 2):
                        w.take(one)
                    for one in (1, 2):
                        w.load_column(one).wait()
                        w.load_mate(one).wait()
                        w.load_side(one).wait()

            if not whole_column:

                @pl.when(step == 2)
                def _():
                    w.forward().wait_recv()
                    w.forward_b().wait_recv()
                    w.far().start()
                    w.mate(3).start()

            @pl.when(step == 8)
            def _():
                w.far().wait_recv()
                w.side_mate(3).start()

            @pl.when(step == 9)
            def _():
                with jax.named_scope("b_s9"):
                    w.take(3)
                    if whole_column:
                        w.load_column(3).wait()
                    w.load_mate(3).wait()
                    w.load_side(3).wait()

            if not last:
                for g, at in enumerate((2, 2, 4, 6, 7)[:n_group]):

                    @pl.when(step == at)
                    def _(g=g):
                        with jax.named_scope("b_ring"):
                            in_next.send_slices(g)

                for g, at in enumerate((8, 11, 13)[:n_group]):

                    @pl.when(step == at)
                    def _(g=g):
                        in_next.ring_stage(g)

            @pl.when(step >= 4)
            def _():
                with jax.named_scope("b_zsend"):
                    c_z(step - 4).wait_send()

            with jax.named_scope("b_mwait"):
                load_m(step).wait()
            here = lax.rem(step, 2)
            rows_c = pl.ds(pl.multiple_of(chunk * crow, crow), crow)
            with jax.named_scope("b_dot"):
                total = None
                for blk in range(n_blocks):
                    mid = jnp.concatenate([mbuf[here, blk, :, k].reshape(2 * crow, c) for k in range(n_mid)], axis=1)
                    attn = obuf[blk, :, rows_c, :].reshape(2 * crow, c)
                    one = jnp.dot(mid, wbuf[blk, slot, c:, :], preferred_element_type=F32)
                    one = one + jnp.dot(attn, wbuf[blk, slot, :c, :], preferred_element_type=F32)
                    total = one if total is None else total + one
                z = total.astype(BF16)
                zb[chunk, slot] = z[:crow]
                z_stage[lax.rem(step, 4)] = z[crow:]
            c_z(step).start()

            settling = functools.reduce(lambda one, other: one | other, [step == at for at in settles])

            @pl.when(settling)
            def _():
                with jax.named_scope("b_settle"):
                    settle(pick(step, [sum(1 for at in settles if at < k) for k in range(tiles)]))

        stages = list(range(3, n_group)) if not last else []
        for k in range(held, tiles):
            if stages and (k - held) % 2 == 0:
                in_next.ring_stage(stages.pop(0))
            settle(k)
        for g in stages:
            in_next.ring_stage(g)

        @pl.loop(0, tiles)
        def _(k):
            save_y(k).wait()
            if not last:
                c_y(k).wait()

        @pl.loop(tiles - 4, tiles)
        def _(k):
            with jax.named_scope("b_tailz"):
                c_z(k).wait_send()

        made = [w.side_up(), w.side_down(), w.far()]
        made += [w.mate(which) for which in range(4)] + [w.side_mate(which) for which in range(4)]
        if not whole_column:
            made += [w.forward(), w.forward_b()]
        for copy in made:
            copy.wait_send()
        if not last:

            @pl.loop(0, n_group)
            def _(g):
                for half in range(2):
                    in_next.forward(g, half).wait()
                    in_next.up(g, half).wait_send()
                    in_next.down(g, half).wait_send()

    anywhere = pl.BlockSpec(memory_space=pl.ANY)
    args = [lens, q, m, kv, x_own, w_out, first, column]
    if not last:
        args += [w_kv, w_in]
    tile = (chunks, n_data, crow, out_part)
    out_shape = [
        jax.ShapeDtypeStruct((rows, d_model) if last else tile, BF16),
        jax.ShapeDtypeStruct((2, n_data, depth, out_part), BF16),
    ]
    if not last:
        out_shape += [
            jax.ShapeDtypeStruct(tile, BF16),
            jax.ShapeDtypeStruct((n_group, n_data, 2, part, c), BF16),
        ]
    dma = pltpu.SemaphoreType.DMA
    return pl.pallas_call(
        kernel,
        out_shape=out_shape,
        in_specs=[pl.BlockSpec(memory_space=pltpu.SMEM)] + [anywhere] * (len(args) - 1),
        out_specs=[anywhere] * len(out_shape),
        scratch_shapes=[
            pltpu.VMEM((n_blocks, n_data, depth, out_part), BF16),
            pltpu.VMEM(q.shape, BF16),
            pltpu.VMEM(kv.shape, BF16),
            pltpu.VMEM((2, n_blocks, 2, n_mid, crow, c), BF16),
            pltpu.VMEM(tile, BF16),
            pltpu.VMEM(tile, BF16),
            pltpu.VMEM(tile, BF16),
            pltpu.VMEM((4, crow, out_part), BF16),
            pltpu.VMEM((n_model // 2, qrows, key_rows), F32),
            pltpu.VMEM((qrows, slab_len), F32),
            pltpu.VMEM((qrows, slab_len), F32),
            pltpu.VMEM((qrows, head_dim), F32),
            dma((SIDE_MATE + 7,)), dma((SIDE_MATE + 7,)), dma((13,)), dma((3, 2 * n_group)), dma((3, 2 * n_group)),
            dma((tiles,)), dma((tiles,)), dma((tiles,)), dma((tiles,)), dma((tiles,)), dma((tiles,)), dma((2,)), dma((2,)),
        ],
        compiler_params=pltpu.CompilerParams(collective_id=2 * layer + 1, has_side_effects=True, vmem_limit_bytes=VMEM_LIMIT),
        cost_estimate=pl.CostEstimate(flops=4 * rows * n_blocks * depth * d_model, bytes_accessed=16 * rows * d_model, transcendentals=0),
        name=f"attend_and_sum_{layer}",
    )(*args)


def solution(mesh):
    batch_axes = ("rep", "data")
    n_data, n_model = mesh.shape["data"], mesh.shape["model"]
    n_chip = n_model // 2

    def near(x):
        return x + 1 - 2 * (x % 2)

    def across(x):
        return n_chip - 1 - x

    def on_chip(other):
        return lambda m: 2 * other(m // 2) + m % 2

    def local_step(x_loc, lens_loc, gamma_loc, w_in_loc, w_kv_loc, w_out_loc):
        n_batch, slab_len, d_model = x_loc.shape
        n_layers, part = gamma_loc.shape
        partners = [on_chip(near if layer % 2 == 0 else across) for layer in range(n_layers)]
        neighbours = [on_chip(across if layer % 2 == 0 else near) for layer in range(n_layers)]

        gain_rows = jnp.zeros((8, part), F32).at[:n_layers].set(gamma_loc.astype(F32))
        own = x_loc.reshape(n_batch * slab_len, d_model)
        for layer in range(n_layers):
            last = layer + 1 == n_layers
            following = min(layer + 1, n_layers - 1)
            if layer == 0:
                extra = (gain_rows,)
                q, m, kv, _, gains, out_first, out_column, in_first = project(
                    layer, n_data, n_model, partners[layer], neighbours[layer], neighbours[following],
                    own, w_kv_loc, w_in_loc, w_out_loc, extra,
                )
            else:
                extra = (other, gains, in_first, in_column)
                q, m, kv, _, out_first, out_column = project(
                    layer, n_data, n_model, partners[layer], neighbours[layer], neighbours[following],
                    own, w_kv_loc, w_in_loc, w_out_loc, extra,
                )
            outs = attend_and_sum(
                layer, last, n_data, n_model, partners[layer], neighbours[layer], partners[following],
                lens_loc, q, m, kv, own, w_in_loc, w_out_loc, w_kv_loc, out_first, out_column,
            )
            own = outs[0]
            if not last:
                other, in_column = outs[2:]
        return own.reshape(n_batch, slab_len, d_model)

    in_specs = (
        P(batch_axes, "model", None),
        P(batch_axes),
        P(None, "data"),
        P(None, "data", "model"),
        P(None, "data", None),
        P(None, "model", "data"),
    )
    return jax.shard_map(local_step, mesh=mesh, in_specs=in_specs, out_specs=P(batch_axes, "model", None), check_vma=False)
```

```python
import functools

import jax
import jax.numpy as jnp
from jax import lax
from jax.experimental import pallas as pl
from jax.experimental.pallas import tpu as pltpu
from jax.sharding import PartitionSpec as P

EPSILON = 1e-6
VMEM_LIMIT = 66_000_000
MESH = pl.DeviceIdType.MESH
BF16, F32 = jnp.bfloat16, jnp.float32

UP, DOWN, FORWARD, FORWARD_B, FIRST, SIDE_UP, SIDE_DOWN, FAR, MATE, SIDE_MATE = range(10)


def rms_norm(x_in, gain):
    x_f32 = x_in.astype(F32)
    inv_rms = lax.rsqrt(jnp.mean(x_f32 * x_f32, axis=-1, keepdims=True) + EPSILON)
    return (x_f32 * inv_rms * gain.astype(F32)).astype(BF16)


class Place:
    def __init__(self, n_data, n_model, partner, neighbour):
        self.n_data, self.n_model = n_data, n_model
        self.y = lax.axis_index("data")
        self.me = lax.axis_index("model")
        self.up = lax.rem(self.y + 1, n_data)
        self.down = lax.rem(self.y + n_data - 1, n_data)
        self.far = lax.rem(self.y + 2, n_data)
        self.slots = (self.y, self.down, self.up, self.far)
        self.mate = self.me + 1 - 2 * lax.rem(self.me, 2)
        self.partner, self.neighbour = partner(self.me), neighbour(self.me)
        n_other = n_model // 2 - 1
        self.ahead = [lax.rem(self.me + 2 * k, n_model) for k in range(1, n_other + 1)]
        self.behind = [lax.rem(self.me + n_model - 2 * k, n_model) for k in range(1, n_other + 1)]

    def meet(self):
        barrier = pltpu.get_barrier_semaphore()
        targets = [{"data": self.up}, {"data": self.down}, {"data": self.far}, {"model": self.mate}]
        targets += [{"model": m} for m in self.ahead]
        for target in targets:
            pl.semaphore_signal(barrier, inc=1, device_id=target, device_id_type=MESH)
        pl.semaphore_wait(barrier, len(targets))


def remote(src, dst, send, recv, target):
    return pltpu.make_async_remote_copy(
        src_ref=src, dst_ref=dst, send_sem=send, recv_sem=recv, device_id=target, device_id_type=MESH
    )


class GatherIn:
    def __init__(self, place, buf, pool, own, send, recv, local, first=None, column=None):
        self.place, self.buf, self.pool, self.own, self.first, self.column = place, buf, pool, own, first, column
        self.send, self.recv, self.local = send, recv, local

    def at(self, block, g, slot):
        return self.buf.at[block, g, slot]

    def _copy(self, src, dst, kind, at, target):
        return remote(src, dst, self.send.at[kind, at], self.recv.at[kind, at], target)

    def up(self, g, half):
        dst = self.at(0, g, self.place.y).at[half]
        return self._copy(self.own(g, half), dst, UP, 2 * g + half, {"data": self.place.up})

    def down(self, g, half):
        dst = self.at(0, g, self.place.y).at[half]
        return self._copy(self.own(g, half), dst, DOWN, 2 * g + half, {"data": self.place.down})

    def neighbour_first(self, g, half):
        dst = self.at(2, g, self.place.y).at[half]
        return self._copy(self.own(g, half), dst, FIRST, 2 * g + half, {"model": self.place.neighbour})

    def forward(self, g, half):
        ref = self.at(0, g, (self.place.down, self.place.up)[half]).at[half]
        target = (self.place.up, self.place.down)[half]
        return self._copy(ref, ref, FORWARD, 2 * g + half, {"data": target})

    def _needed(self, ref, g):
        return ref.at[0] if isinstance(g, int) and g == 0 else ref

    def _side(self, g, kind, target):
        src = self.at(2, g, self.place.y) if self.first is None else self.first.at[g]
        dst = self.at(2, g, self.place.y)
        return self._copy(self._needed(src, g), self._needed(dst, g), kind, g, {"data": target})

    def side_up(self, g):
        return self._side(g, SIDE_UP, self.place.up)

    def side_down(self, g):
        return self._side(g, SIDE_DOWN, self.place.down)

    def far(self, g):
        slot = self.place.far
        src = self.at(0, g, slot) if self.column is None else self.column.at[g, slot]
        dst = self.at(2, g, slot)
        return self._copy(self._needed(src, g), self._needed(dst, g), FAR, g, {"model": self.place.neighbour})

    def mate(self, g):
        return self._copy(self.buf.at[0, g], self.pool.at[0, g], MATE, g, {"model": self.place.mate})

    def side_mate(self, g):
        src, dst = self.buf.at[2, g], self.pool.at[1, g]
        if isinstance(g, int) and g == 0:
            src, dst = src.at[:, 0], dst.at[:, 0]
        return self._copy(src, dst, SIDE_MATE, g, {"model": self.place.mate})

    def load_mate(self, g):
        return pltpu.make_async_copy(self.pool.at[0, g], self.buf.at[1, g], self.local.at[6, g])

    def load_side(self, g):
        src, dst = self.pool.at[1, g], self.buf.at[3, g]
        if isinstance(g, int) and g == 0:
            src, dst = src.at[:, 0], dst.at[:, 0]
        return pltpu.make_async_copy(src, dst, self.local.at[7, g])

    def take_mate(self, g):
        self.mate(g).wait_recv()
        self.load_mate(g).start()

    def take_side(self, g):
        self.side_mate(g).wait_recv()
        self.load_side(g).start()

    def load_own(self, g, half):
        dst = self.at(0, g, self.place.y).at[half]
        return pltpu.make_async_copy(self.own(g, half), dst, self.local.at[half, g])

    def load_column(self, g, which):
        slot = self.place.slots[which]
        return pltpu.make_async_copy(self.column.at[g, slot], self.at(0, g, slot), self.local.at[1 + which, g])

    def load_first(self, g):
        return pltpu.make_async_copy(self.first.at[g], self.at(2, g, self.place.y), self.local.at[5, g])

    def pass_side(self, g):
        if self.first is not None:
            self.load_first(g).wait()
        self.side_up(g).wait_recv()
        self.side_down(g).wait_recv()
        self.far(g).wait_recv()
        self.side_mate(g).start()

    def wait_sends(self, g):
        made = [self.side_up(g), self.side_down(g), self.far(g), self.mate(g), self.side_mate(g)]
        if self.column is None:
            made += [copy(g, half) for copy in (self.up, self.down, self.forward) for half in range(2)]
        if self.first is None:
            made += [self.neighbour_first(g, half) for half in range(2)]
        for copy in made:
            copy.wait_send()


class FetchIn:
    def __init__(self, place, own, send, recv, neighbour=None, first=None, column=None):
        self.place, self.own, self.send, self.recv = place, own, send, recv
        self.neighbour, self.first, self.column = neighbour, first, column

    def _ring(self, g, half, kind, target):
        at = 2 * g + half
        dst = self.column.at[g, self.place.y, half]
        return remote(self.own(g, half), dst, self.send.at[kind, at], self.recv.at[kind, at], {"data": target})

    def up(self, g, half):
        return self._ring(g, half, 0, self.place.up)

    def down(self, g, half):
        return self._ring(g, half, 1, self.place.down)

    def forward(self, g, half):
        at = 2 * g + half
        ref = self.column.at[g, (self.place.down, self.place.up)[half], half]
        target = (self.place.up, self.place.down)[half]
        return remote(ref, ref, self.send.at[2, at], self.recv.at[2, at], {"data": target})

    def ring_stage(self, g):
        for half in range(2):
            self.up(g, half).wait_recv()
            self.down(g, half).wait_recv()
        for half in range(2):
            self.forward(g, half).start()

    def send_slices(self, g):
        for half in range(2):
            self.up(g, half).start()
            self.down(g, half).start()

    def neighbour_first(self, g, half):
        at = 2 * g + half
        dst = self.first.at[g, half]
        return remote(self.own(g, half), dst, self.send.at[3, at], self.recv.at[3, at], {"model": self.neighbour})


class GatherOut:
    def __init__(self, place, buf, own, send, recv, local=None, first=None, column=None, pool=None, whole_column=True):
        self.place, self.buf, self.own, self.first, self.column = place, buf, own, first, column
        self.far_held = column is not None and whole_column
        self.send, self.recv, self.local, self.pool = send, recv, local, pool

    def _copy(self, src, dst, kind, target):
        return remote(src, dst, self.send.at[kind], self.recv.at[kind], target)

    def up(self):
        return self._copy(self.own, self.buf.at[0, self.place.y], UP, {"data": self.place.up})

    def down(self):
        return self._copy(self.own, self.buf.at[0, self.place.y], DOWN, {"data": self.place.down})

    def _half(self, ref, second):
        size = ref.shape[0] // 2
        return ref.at[pl.ds(second * size, size)]

    def _forward(self, kind, slot, second, target):
        src = self.buf if self.column is None else self.column
        dst = self._half(self.buf.at[0, slot], second)
        return self._copy(self._half(src.at[0, slot], second), dst, kind, {"data": target})

    def forward(self):
        return self._forward(FORWARD, self.place.down, 0, self.place.up)

    def forward_b(self):
        return self._forward(FORWARD_B, self.place.up, 1, self.place.down)

    def neighbour_first(self, dst):
        return self._copy(self.own, dst, FIRST, {"model": self.place.neighbour})

    def side_up(self):
        return self._copy(self.first, self.buf.at[2, self.place.y], SIDE_UP, {"data": self.place.up})

    def side_down(self):
        return self._copy(self.first, self.buf.at[2, self.place.y], SIDE_DOWN, {"data": self.place.down})

    def far(self):
        slot = self.place.far
        src = self.column.at[0, slot] if self.far_held else self.buf.at[0, slot]
        return self._copy(src, self.buf.at[2, slot], FAR, {"model": self.place.neighbour})

    def mate(self, which):
        slot = self.place.slots[which]
        if which == 0:
            src = self.own
        else:
            src = self.column.at[0, slot] if which < 3 or self.far_held else self.buf.at[0, slot]
        return self._copy(src, self.pool.at[0, slot], MATE + 2 * which, {"model": self.place.mate})

    def side_mate(self, which):
        slot = self.place.slots[which]
        src = self.first if which == 0 else self.buf.at[2, slot]
        return self._copy(src, self.pool.at[1, slot], SIDE_MATE + 2 * which, {"model": self.place.mate})

    def load_mate(self, which):
        slot = self.place.slots[which]
        return pltpu.make_async_copy(self.pool.at[0, slot], self.buf.at[1, slot], self.local.at[5 + which])

    def load_side(self, which):
        slot = self.place.slots[which]
        return pltpu.make_async_copy(self.pool.at[1, slot], self.buf.at[3, slot], self.local.at[9 + which])

    def take(self, which):
        self.mate(which).wait_recv()
        self.load_mate(which).start()
        self.side_mate(which).wait_recv()
        self.load_side(which).start()

    def load_own(self):
        return pltpu.make_async_copy(self.own, self.buf.at[0, self.place.y], self.local.at[0])

    def load_column(self, which):
        slot = self.place.slots[which]
        return pltpu.make_async_copy(self.column.at[0, slot], self.buf.at[0, slot], self.local.at[which])

    def load_first(self):
        return pltpu.make_async_copy(self.first, self.buf.at[2, self.place.y], self.local.at[4])


def in_halves(layer, w_kv_ref, w_ref, c, ff):
    def own(g, half):
        if isinstance(g, int) and g == 0:
            return w_kv_ref.at[layer] if half else w_ref.at[layer, :, pl.ds(0, c)]
        return w_ref.at[layer, :, pl.ds(pl.multiple_of(g * c + half * ff, c), c)]

    return own


def project(layer, n_data, n_model, partner, neighbour, next_neighbour, x_own, w_kv, w_in, w_out, extra):
    start_layer = layer == 0
    part, c = w_kv.shape[1:]
    d_model = part * n_data
    rows = x_own.size // d_model
    depth, out_part = w_out.shape[1:]
    ff = depth - c
    n_group = 1 + ff // c
    n_units = 8 * n_group
    row_parts = 4
    row_part = rows // row_parts
    n_other = n_model // 2 - 1
    gain_shape = (n_data, 8, part)
    n_tiles = 1 if start_layer else x_own.shape[0] * x_own.shape[1]

    def kernel(*refs):
        x_ref, w_kv_ref, w_ref, wo_ref = refs[:4]
        if start_layer:
            gain_ref = refs[4]
            q_ref, m_ref, kv_ref, pool_ref, gains_ref, out_first_ref, out_column_ref, in_first_ref = refs[5:13]
            first_ref = column_ref = None
            rest = refs[13:]
        else:
            par_ref, gain_ref, first_ref, column_ref = refs[4:8]
            q_ref, m_ref, kv_ref, pool_ref, out_first_ref, out_column_ref = refs[8:14]
            rest = refs[14:]
        wbuf, h_ref, gbuf, stage, kv_stage, send, recv, w_local, next_send, next_recv, late_send, late_recv = rest[:12]
        x_send, x_recv, g_send, g_recv, kv_send, kv_recv, local, out_sem, tile_sem = rest[12:]

        place = Place(n_data, n_model, partner, neighbour)
        place.meet()
        in_own = in_halves(layer, w_kv_ref, w_ref, c, ff)
        w = GatherIn(place, wbuf, pool_ref, in_own, send, recv, w_local, first_ref, column_ref)
        out_next = GatherOut(place, out_column_ref, wo_ref.at[layer], next_send, next_recv)
        if start_layer:
            in_own_next = in_halves(layer + 1, w_kv_ref, w_ref, c, ff)
            in_next = FetchIn(place, in_own_next, late_send, late_recv, next_neighbour(place.me), in_first_ref)

        def c_x(part_no):
            piece = pl.ds(part_no * row_part, row_part)
            return remote(
                x_ref.at[piece], h_ref.at[1, piece], x_send.at[part_no], x_recv.at[part_no], {"model": place.partner}
            )

        def c_gain(which):
            target = {"data": (place.up, place.down, place.far)[which]}
            return remote(gain_ref, gbuf.at[place.y], g_send.at[which], g_recv.at[which], target)

        def c_kv(which):
            ref = kv_ref.at[place.me]
            return remote(ref, ref, kv_send.at[which], kv_recv.at[which], {"model": place.ahead[which]})

        def c_kv_mate(which):
            ref = kv_ref.at[place.me if which == 0 else place.behind[which - 1]]
            at = n_other + which
            return remote(ref, ref, kv_send.at[at], kv_recv.at[at], {"model": place.mate})

        save_kv = pltpu.make_async_copy(kv_stage, kv_ref.at[place.me], local.at[0])
        if start_layer:
            load_x = pltpu.make_async_copy(x_ref, h_ref.at[0], local.at[0])

        def load_tile(side, k):
            chunk, slot = k // n_data, lax.rem(k, n_data)
            src = (x_ref, par_ref)[side].at[chunk, slot]
            height, across = src.shape
            down_to, along = pl.multiple_of(chunk * height, height), pl.multiple_of(slot * across, across)
            return pltpu.make_async_copy(src, h_ref.at[side, pl.ds(down_to, height), pl.ds(along, across)], tile_sem.at[side, k])

        if start_layer:
            load_gain = pltpu.make_async_copy(gain_ref, gbuf.at[place.y], local.at[1])
            for which in range(3):
                c_gain(which).start()
        else:
            load_gain = pltpu.make_async_copy(gain_ref, gbuf, local.at[1])
        def send_slices(g):
            for half in range(2):
                w.up(g, half).start()
                w.down(g, half).start()

        load_gain.start()
        if start_layer:
            load_x.start()
        else:
            for side in range(2):

                @pl.loop(0, n_tiles)
                def _(k):
                    load_tile(side, k).start()

        if start_layer:
            send_slices(0)
            for g in range(n_group):
                for half in range(2):
                    w.neighbour_first(g, half).start()
                    w.load_own(g, half).start()
            for part_no in range(row_parts // 2):
                c_x(part_no).start()
        else:
            for g in range(n_group):
                for half in range(2):
                    w.load_own(g, half).start()
                for which in range(1, 4):
                    w.load_column(g, which).start()
                w.side_up(g).start()
                w.side_down(g).start()
                if g < 2:
                    w.far(g).start()
            for g in range(n_group):
                w.load_first(g).start()

        def ring_stage(g):
            for half in range(2):
                w.up(g, half).wait_recv()
                w.down(g, half).wait_recv()
            for half in range(2):
                w.forward(g, half).start()

        def column_stage(g):
            for half in range(2):
                w.load_own(g, half).wait()
            for which in range(1, 4):
                w.load_column(g, which).wait()
            w.mate(g).start()

        if start_layer:
            for which in range(3):
                c_gain(which).wait_recv()
        load_gain.wait()
        gain = jnp.concatenate([gbuf[k, layer:layer + 1, :] for k in range(n_data)], axis=1)
        if start_layer:
            save_gain = pltpu.make_async_copy(gbuf, gains_ref, local.at[1])
            save_gain.start()
        if start_layer:
            load_x.wait()
        else:

            @pl.loop(0, n_tiles)
            def _(k):
                load_tile(0, k).wait()

        def norm_rows(side, part_no):
            piece = pl.ds(part_no * row_part, row_part)
            h_ref[side, piece] = rms_norm(h_ref[side, piece], gain)

        @pl.loop(0, row_parts)
        def _(part_no):
            norm_rows(0, part_no)

        if start_layer:
            send_slices(1)
            ring_stage(0)
        else:
            column_stage(0)

        halfway, quarter = n_units // 2, n_units // 4

        def out_copy(slot, blk, side, g):
            def to_q():
                return pltpu.make_async_copy(stage.at[slot], q_ref.at[blk, side], out_sem.at[slot])

            def to_m():
                return pltpu.make_async_copy(stage.at[slot], m_ref.at[blk, side, g - 1], out_sem.at[slot])

            return to_q, to_m

        @pl.loop(0, n_units)
        def _(step):
            late = step - halfway
            if start_layer:
                opening, second = step < quarter, (step >= quarter) & (step < halfway)
                ahead = (step == 0) | ((lax.rem(step, 2) == 1) & (step < quarter - 1))
                open_g = jnp.where(ahead, (step + 1) // 2, jnp.where(step == quarter - 1, n_group - 1, step // 2 - 1))
                g = jnp.where(opening, open_g, jnp.where(second, (step - quarter) // 2, late // 4))
                open_blk = jnp.where(ahead, 0, 1)
                blk = jnp.where(opening, open_blk, jnp.where(second, lax.rem(step, 2), 2 + lax.rem(late, 4) // 2))
                side = jnp.where(opening, 0, jnp.where(second, 1, lax.rem(late, 2)))

                @pl.when(opening & (blk == 0))
                def _():
                    with jax.named_scope("a_ring"):
                        for half in range(2):
                            w.forward(g, half).wait_recv()

                        @pl.when(g + 2 < n_group)
                        def _():
                            send_slices(g + 2)

                        @pl.when(g + 1 < n_group)
                        def _():
                            ring_stage(g + 1)

                        @pl.when(g + 2 == n_group)
                        def _():
                            for k in range(n_group):
                                for half in range(2):
                                    w.neighbour_first(k, half).wait_recv()
                                w.side_up(k).start()
                                w.side_down(k).start()

                        @pl.when(g == 0)
                        def _():
                            w.far(0).start()

                        @pl.when(g > 0)
                        def _():
                            w.far(g).start()

                        @pl.when(g == 1)
                        def _():
                            for part_no in range(row_parts // 2, row_parts):
                                c_x(part_no).start()

                        for half in range(2):
                            w.load_own(g, half).wait()
                        w.mate(g).start()

                        @pl.when(g > 0)
                        def _():
                            w.take_mate(g - 1)

                @pl.when(step == quarter - 2)
                def _():
                    with jax.named_scope("a_take_last"):
                        w.take_mate(n_group - 1)

                @pl.when(opening & (blk == 1))
                def _():
                    with jax.named_scope("a_load_mate"):
                        w.load_mate(g).wait()

                @pl.when(step == quarter)
                def _():
                    with jax.named_scope("a_par"):
                        @pl.loop(0, row_parts)
                        def _(part_no):
                            c_x(part_no).wait_recv()
                            norm_rows(1, part_no)

                        out_next.neighbour_first(out_first_ref).start()
                        out_next.up().start()
                        out_next.down().start()
                        for k in range(n_group):
                            for half in range(2):
                                in_next.neighbour_first(k, half).start()
            else:
                g = jnp.where(late < 0, step, late) // 4
                blk = jnp.where(late < 0, 0, 2) + lax.rem(step, 4) // 2
                side = lax.rem(step, 2)

                @pl.when((late < 0) & (lax.rem(step, 4) == 0) & (g + 1 < n_group))
                def _():
                    with jax.named_scope("a_col"):
                        column_stage(g + 1)

                @pl.when(step == 1)
                def _():
                    with jax.named_scope("a_par1"):
                        @pl.loop(0, n_tiles)
                        def _(k):
                            load_tile(1, k).wait()

                        @pl.loop(0, row_parts)
                        def _(part_no):
                            norm_rows(1, part_no)

                @pl.when((late < 0) & (lax.rem(step, 4) == 1))
                def _():
                    with jax.named_scope("a_take_mate"):
                        w.take_mate(g)

                @pl.when((late < 0) & (lax.rem(step, 4) == 2))
                def _():
                    with jax.named_scope("a_wait_mate"):
                        w.load_mate(g).wait()

                @pl.when(step == n_units - 6)
                def _():
                    with jax.named_scope("a_next"):
                        out_next.up().wait_recv()
                        out_next.down().wait_recv()
                        out_next.forward().start()
                        out_next.forward_b().start()

            @pl.when(step == halfway - 2)
            def _():
                with jax.named_scope("a_pass0"):
                    w.pass_side(0)

            @pl.when(step == halfway + 1)
            def _():
                w.take_side(0)

            @pl.when((late > 1) & (lax.rem(late, 4) == 1))
            def _():
                w.take_side(g)

            @pl.when((late >= 0) & (lax.rem(late, 4) == 2))
            def _():
                with jax.named_scope("a_pass_side"):
                    @pl.when(g + 1 < n_group)
                    def _():
                        w.pass_side(g + 1)

                    @pl.when(g == 0)
                    def _():
                        w.load_side(0).wait()

                    @pl.when(g > 0)
                    def _():
                        w.load_side(g).wait()

            slot = lax.rem(step, 2)
            to_q, to_m = out_copy(slot, blk, side, g)

            @pl.when(step >= 2)
            def _():
                with jax.named_scope("a_outwait"):
                    to_q().wait()

            def columns(half):
                return wbuf[blk, g, :, half].reshape(d_model, c)

            @pl.when(g == 0)
            def _():
                with jax.named_scope("a_unit_q"):
                    q = jnp.dot(h_ref[side], columns(0), preferred_element_type=F32)
                    stage[slot] = q.astype(BF16)
                    to_q().start()

            @pl.when(g > 0)
            def _():
                with jax.named_scope("a_unit_m"):
                    h_val = h_ref[side]
                    gate = jnp.dot(h_val, columns(0), preferred_element_type=F32).astype(BF16).astype(F32)
                    raised = jnp.dot(h_val, columns(1), preferred_element_type=F32).astype(BF16).astype(F32)
                    stage[slot] = (gate * jax.nn.sigmoid(gate) * raised).astype(BF16)
                    to_m().start()

            @pl.when(step == 0)
            def _():
                kv_stage[...] = jnp.dot(h_ref[0], columns(1), preferred_element_type=F32).astype(BF16)
                save_kv.start()

            @pl.when(step == 1)
            def _():
                with jax.named_scope("a_kv1"):
                    save_kv.wait()
                    for which in range(n_other):
                        c_kv(which).start()
                    c_kv_mate(0).start()
                    if not start_layer:
                        for k in range(2, n_group):
                            w.far(k).start()

            if not start_layer:

                @pl.when(step == 8)
                def _():
                    out_next.up().start()
                    out_next.down().start()
                    out_next.neighbour_first(out_first_ref).start()

        with jax.named_scope("ta_kv"):
            for which in range(n_other):
                c_kv(which).wait_recv()
                c_kv_mate(1 + which).start()
        for which in range(n_other + 1):
            c_kv_mate(which).wait()
        for which in range(n_other):
            c_kv(which).wait_send()
        if start_layer:
            save_gain.wait()
            for which in range(3):
                c_gain(which).wait_send()
            for part_no in range(row_parts):
                c_x(part_no).wait_send()
            with jax.named_scope("ta_in"):
                for g in range(n_group):
                    for half in range(2):
                        in_next.neighbour_first(g, half).wait()
            with jax.named_scope("ta_out"):
                for copy in (out_next.up(), out_next.down()):
                    copy.wait()
        else:
            for copy in (out_next.forward(), out_next.forward_b()):
                copy.wait()
            for copy in (out_next.up(), out_next.down()):
                copy.wait_send()
        out_next.neighbour_first(out_first_ref).wait()
        for slot in range(2):
            pltpu.make_async_copy(stage.at[slot], q_ref.at[0, 0], out_sem.at[slot]).wait()

        for g in range(n_group):
            w.wait_sends(g)

    anywhere = pl.BlockSpec(memory_space=pl.ANY)
    out_shape = [
        jax.ShapeDtypeStruct((4, 2, rows, c), BF16),
        jax.ShapeDtypeStruct((4, 2, n_group - 1, rows, c), BF16),
        jax.ShapeDtypeStruct((n_model, rows, c), BF16),
        jax.ShapeDtypeStruct((2, n_group, n_data, 2, part, c), BF16),
    ]
    if start_layer:
        out_shape += [
            jax.ShapeDtypeStruct(gain_shape, F32),
            jax.ShapeDtypeStruct((depth, out_part), BF16),
            jax.ShapeDtypeStruct((1, n_data, depth, out_part), BF16),
            jax.ShapeDtypeStruct((n_group, 2, part, c), BF16),
        ]
    else:
        out_shape += [
            jax.ShapeDtypeStruct((depth, out_part), BF16),
            jax.ShapeDtypeStruct((1, n_data, depth, out_part), BF16),
        ]
    dma = pltpu.SemaphoreType.DMA
    args = (x_own, w_kv, w_in, w_out) + tuple(extra)
    return pl.pallas_call(
        kernel,
        out_shape=out_shape,
        in_specs=[anywhere] * len(args),
        out_specs=[anywhere] * len(out_shape),
        scratch_shapes=[
            pltpu.VMEM((4, n_group, n_data, 2, part, c), BF16),
            pltpu.VMEM((2, rows, d_model), BF16),
            pltpu.VMEM(gain_shape, F32),
            pltpu.VMEM((2, rows, c), BF16),
            pltpu.VMEM((rows, c), BF16),
            dma((SIDE_MATE + 1, 2 * n_group)), dma((SIDE_MATE + 1, 2 * n_group)), dma((8, n_group)),
            dma((FIRST + 1,)), dma((FIRST + 1,)), dma((4, 2 * n_group)), dma((4, 2 * n_group)),
            dma((row_parts,)), dma((row_parts,)), dma((3,)), dma((3,)),
            dma((n_model - 1,)), dma((n_model - 1,)), dma((3,)), dma((2,)), dma((2, n_tiles)),
        ],
        compiler_params=pltpu.CompilerParams(collective_id=2 * layer, has_side_effects=True, vmem_limit_bytes=VMEM_LIMIT),
        cost_estimate=pl.CostEstimate(flops=4 * rows * d_model * 4 * (c + 2 * ff), bytes_accessed=16 * rows * d_model, transcendentals=0),
        name=f"project_{layer}",
    )(*args)


def pick(step, values):
    found = jnp.int32(values[0])
    for at in range(1, len(values)):
        if values[at] != values[at - 1]:
            found = jnp.where(step >= at, jnp.int32(values[at]), found)
    return found


def attend_and_sum(layer, last, n_data, n_model, partner, neighbour, next_partner, lens, q, m, kv, x_own, w_in, w_out, w_kv, first, column):
    n_blocks, _, rows, c = q.shape
    n_mid = m.shape[2]
    ff = n_mid * c
    d_model = w_out.shape[2] * n_data
    tiled = x_own.ndim == 4
    depth, out_part = w_out.shape[1:]
    head_dim = c // 2
    n_batch = lens.shape[0]
    slab_len = rows // n_batch
    chunks = 4
    n_seq = n_batch // chunks
    crow = rows // chunks
    tiles = chunks * n_data
    heads = n_blocks * 2
    qrows = heads * slab_len
    key_rows = 2 * slab_len
    scale = head_dim ** -0.5 * 1.4426950408889634
    part = w_kv.shape[1]
    n_group = 1 + ff // c
    if layer == 0:
        order = [(0, 0), (1, 0), (2, 0), (0, 1), (1, 1), (2, 1), (0, 2), (1, 2), (2, 2)]
        order += [(3, 0), (3, 1), (3, 2), (0, 3), (1, 3), (2, 3), (3, 3)]
        opens = (0, 1, 2, 9)
        settles = {2: (0,), 3: (1,), 5: (2,), 7: (3,), 9: (4, 5), 11: (6,), 12: (7,), 14: (8,), 15: (9,)}
        side_step, far_step = 2, 11
    else:
        order = [(0, 0), (1, 0), (0, 1), (1, 1), (0, 2), (1, 2), (2, 0), (2, 1), (2, 2), (0, 3), (1, 3), (2, 3)]
        order += [(3, which) for which in range(4)]
        opens = (0, 1, 6, 12)
        settles = {2: (0,), 3: (1,), 6: (2,), 7: (3,), 8: (4,), 9: (5,), 10: (6,), 12: (7,), 13: (8,), 15: (9,)}
        side_step, far_step = 1, 8
    held = sum(len(some) for some in settles.values())
    whole_column = layer > 0

    def kernel(*refs):
        lens_ref, q_ref, m_ref, kv_ref, x_ref, wo_ref, first_ref = refs[:7]
        at = 7
        column_ref = refs[at]
        at += 1
        if not last:
            w_kv_ref, wi_ref = refs[at:at + 2]
            at += 2
        y_ref, pool_ref = refs[at:at + 2]
        at += 2
        if not last:
            par_ref, in_column_ref = refs[at:at + 2]
            at += 2
        (wbuf, obuf, kvb, mbuf, xb, zb, zr, z_stage, s_ref, mx_ref, sum_ref, acc_ref,
         send, recv, w_local, in_send, in_recv, z_send, z_recv, y_send, y_recv, y_save, x_sem, m_sem, local) = refs[at:]

        place = Place(n_data, n_model, partner, neighbour)
        place.meet()
        w = GatherOut(place, wbuf, wo_ref.at[layer], send, recv, w_local, first_ref, column_ref, pool_ref, whole_column)

        def tile_of(k):
            which = pick(k, [one for _, one in order])
            slot = jnp.where(which == 0, place.y, jnp.where(which == 1, place.down, jnp.where(which == 2, place.up, place.far)))
            return pick(k, [one for one, _ in order]), which, slot

        def whole(ref, chunk, slot):
            return ref.at[pl.ds(pl.multiple_of(chunk * crow, crow), crow), pl.ds(pl.multiple_of(slot * out_part, out_part), out_part)]

        def rows_of(chunk):
            return pl.ds(pl.multiple_of(chunk * crow, crow), crow)

        def load_q(chunk):
            return pltpu.make_async_copy(q_ref.at[:, :, rows_of(chunk)], obuf.at[:, :, rows_of(chunk)], local.at[0, chunk])

        def load_kv(chunk):
            return pltpu.make_async_copy(kv_ref.at[:, rows_of(chunk)], kvb.at[:, rows_of(chunk)], local.at[1, chunk])

        def load_m(k):
            chunk, _, _ = tile_of(k)
            slot = lax.rem(k, 2)
            return pltpu.make_async_copy(
                m_ref.at[:, :, :, pl.ds(pl.multiple_of(chunk * crow, crow), crow)], mbuf.at[slot], m_sem.at[slot]
            )

        def load_x(k):
            chunk, _, slot = tile_of(k)
            src = x_ref.at[chunk, slot] if tiled else whole(x_ref, chunk, slot)
            return pltpu.make_async_copy(src, xb.at[chunk, slot], x_sem.at[k])

        def c_z(k):
            chunk, _, slot = tile_of(k)
            return remote(z_stage.at[lax.rem(k, 4)], zr.at[chunk, slot], z_send.at[k], z_recv.at[k], {"model": place.partner})

        def c_y(k):
            chunk, _, slot = tile_of(k)
            target = {"model": next_partner(place.me)}
            return remote(xb.at[chunk, slot], par_ref.at[chunk, slot], y_send.at[k], y_recv.at[k], target)

        def save_y(k):
            chunk, _, slot = tile_of(k)
            dst = whole(y_ref, chunk, slot) if last else y_ref.at[chunk, slot]
            return pltpu.make_async_copy(xb.at[chunk, slot], dst, y_save.at[k])

        for chunk in range(chunks):
            load_q(chunk).start()
            load_kv(chunk).start()
        load_m(0).start()
        w.load_own().start()
        w.load_first().start()
        w.mate(0).start()
        w.side_mate(0).start()
        for which in range(1, 4 if whole_column else 3):
            w.load_column(which).start()
            w.mate(which).start()
        w.side_up().start()
        w.side_down().start()
        if whole_column:
            w.far().start()
        else:
            w.forward().start()
            w.forward_b().start()
        if not last:
            in_own = in_halves(layer + 1, w_kv_ref, wi_ref, c, ff)
            in_next = FetchIn(place, in_own, in_send, in_recv, column=in_column_ref)

        @pl.loop(0, tiles)
        def _(k):
            load_x(k).start()

        def attend_one(batch, side):
            slab = jnp.where(side == 0, place.me, place.partner)
            length = lens_ref[batch]
            n_key = slab // 2 + 1
            at_row = pl.ds(pl.multiple_of(batch * slab_len, slab_len), slab_len)
            parts = []
            for blk in range(n_blocks):
                for one in range(2):
                    parts.append(obuf[blk, side, at_row, one * head_dim:(one + 1) * head_dim])
            q_val = jnp.concatenate(parts, axis=0)
            row_pos = slab * slab_len + lax.rem(lax.broadcasted_iota(jnp.int32, (qrows, key_rows), 0), slab_len)
            key_pos = lax.broadcasted_iota(jnp.int32, (qrows, key_rows), 1)
            room = jnp.minimum(row_pos + 1, length) - key_pos
            mx_ref[...] = jnp.full_like(mx_ref, -1e30)

            def score(kb, carry):
                k = kvb[pl.ds(2 * kb, 2), at_row, :head_dim].reshape(key_rows, head_dim)
                s = lax.dot_general(q_val, k, (((1,), (1,)), ((), ())), preferred_element_type=F32) * scale
                s = jnp.where(room > kb * key_rows, s, -1e30)
                s_ref[kb] = s
                mx_ref[...] = jnp.maximum(mx_ref[...], jnp.maximum(s[:, :slab_len], s[:, slab_len:]))
                return carry

            lax.fori_loop(0, n_key, score, 0)
            top = jnp.max(mx_ref[...], axis=-1, keepdims=True)
            mx_ref[...] = jnp.broadcast_to(top, mx_ref.shape)
            sum_ref[...] = jnp.zeros_like(sum_ref)
            acc_ref[...] = jnp.zeros_like(acc_ref)

            def weigh(kb, carry):
                v = kvb[pl.ds(2 * kb, 2), at_row, head_dim:].reshape(key_rows, head_dim)
                top_b = mx_ref[...]
                e_lo = jnp.exp2(s_ref[kb, :, :slab_len] - top_b)
                e_hi = jnp.exp2(s_ref[kb, :, slab_len:] - top_b)
                sum_ref[...] += e_lo + e_hi
                e = jnp.concatenate([e_lo, e_hi], axis=1).astype(BF16)
                acc_ref[...] += jnp.dot(e, v, preferred_element_type=F32)
                return carry

            lax.fori_loop(0, n_key, weigh, 0)
            out = (acc_ref[...] / jnp.sum(sum_ref[...], axis=-1, keepdims=True)).astype(BF16)
            for blk in range(n_blocks):
                for one in range(2):
                    first_row = (blk * 2 + one) * slab_len
                    obuf[blk, side, at_row, one * head_dim:(one + 1) * head_dim] = out[first_row:first_row + slab_len]

        def settle(k):
            chunk, _, slot = tile_of(k)
            load_x(k).wait()
            c_z(k).wait_recv()
            z = zb[chunk, slot].astype(F32) + zr[chunk, slot].astype(F32)
            xb[chunk, slot] = (xb[chunk, slot].astype(F32) + z).astype(BF16)
            save_y(k).start()
            if not last:
                c_y(k).start()

        @pl.loop(0, tiles)
        def _(step):
            chunk, which, slot = tile_of(step)

            @pl.when(step + 1 < tiles)
            def _():
                load_m(step + 1).start()

            opening = functools.reduce(lambda one, other: one | other, [step == at for at in opens])

            @pl.when(opening)
            def _():
                with jax.named_scope("b_attn"):
                    load_q(chunk).wait()
                    load_kv(chunk).wait()

                    @pl.loop(0, 2 * n_seq)
                    def _(unit):
                        attend_one(chunk * n_seq + unit // 2, lax.rem(unit, 2))

            @pl.when(step == 0)
            def _():
                with jax.named_scope("b_w0"):
                    w.load_own().wait()
                    w.load_first().wait()
                    w.take(0)
                    w.load_mate(0).wait()
                    w.load_side(0).wait()

            @pl.when(step == side_step)
            def _():
                with jax.named_scope("b_side"):
                    if not whole_column:
                        w.forward().wait_recv()
                        w.forward_b().wait_recv()
                        w.far().start()
                        w.mate(3).start()
                    w.side_up().wait_recv()
                    w.side_mate(1).start()
                    w.side_down().wait_recv()
                    w.side_mate(2).start()

            @pl.when(step == side_step + 1)
            def _():
                with jax.named_scope("b_take"):
                    for one in (1, 2):
                        w.take(one)
                    for one in (1, 2):
                        w.load_column(one).wait()
                        w.load_mate(one).wait()
                        w.load_side(one).wait()

            @pl.when(step == far_step)
            def _():
                with jax.named_scope("b_far"):
                    w.far().wait_recv()
                    w.side_mate(3).start()

            @pl.when(step == far_step + 1)
            def _():
                with jax.named_scope("b_take3"):
                    w.take(3)
                    if whole_column:
                        w.load_column(3).wait()
                    w.load_mate(3).wait()
                    w.load_side(3).wait()

            if not last:
                for g, at in enumerate((3, 3, 4, 5, 6)[:n_group]):

                    @pl.when(step == at)
                    def _(g=g):
                        in_next.send_slices(g)

                for g, at in enumerate((9, 10, 12, 15)[:n_group]):

                    @pl.when(step == at)
                    def _(g=g):
                        with jax.named_scope("b_ring"):
                            in_next.ring_stage(g)

            @pl.when(step >= 4)
            def _():
                with jax.named_scope("b_zsend"):
                    c_z(step - 4).wait_send()

            with jax.named_scope("b_mwait"):
                load_m(step).wait()
            here = lax.rem(step, 2)
            rows_c = pl.ds(pl.multiple_of(chunk * crow, crow), crow)
            with jax.named_scope("b_dot"):
                total = None
                for blk in range(n_blocks):
                    mid = jnp.concatenate([mbuf[here, blk, :, k].reshape(2 * crow, c) for k in range(n_mid)], axis=1)
                    attn = obuf[blk, :, rows_c, :].reshape(2 * crow, c)
                    one = jnp.dot(mid, wbuf[blk, slot, c:, :], preferred_element_type=F32)
                    one = one + jnp.dot(attn, wbuf[blk, slot, :c, :], preferred_element_type=F32)
                    total = one if total is None else total + one
                z = total.astype(BF16)
                zb[chunk, slot] = z[:crow]
                z_stage[lax.rem(step, 4)] = z[crow:]
            c_z(step).start()

            for at, some in settles.items():

                @pl.when(step == at)
                def _(some=some):
                    for k in some:
                        with jax.named_scope("b_settle"):
                            settle(k)

        stages = list(range(4, n_group)) if not last else []
        for k in range(held, tiles):
            if stages and k - held >= 2:
                with jax.named_scope("t_ring"):
                    in_next.ring_stage(stages.pop(0))
            with jax.named_scope("t_settle"):
                settle(k)
        for g in stages:
            in_next.ring_stage(g)

        with jax.named_scope("t_save"):

            @pl.loop(0, tiles)
            def _(k):
                save_y(k).wait()

        if not last:
            with jax.named_scope("t_y"):

                @pl.loop(0, tiles)
                def _(k):
                    c_y(k).wait()

        @pl.loop(tiles - 4, tiles)
        def _(k):
            with jax.named_scope("b_tailz"):
                c_z(k).wait_send()

        made = [w.side_up(), w.side_down(), w.far()]
        made += [w.mate(which) for which in range(4)] + [w.side_mate(which) for which in range(4)]
        if not whole_column:
            made += [w.forward(), w.forward_b()]
        with jax.named_scope("t_w"):
            for copy in made:
                copy.wait_send()
        if not last:
            with jax.named_scope("t_in"):

                @pl.loop(0, n_group)
                def _(g):
                    for half in range(2):
                        in_next.forward(g, half).wait()
                        in_next.up(g, half).wait_send()
                        in_next.down(g, half).wait_send()

    anywhere = pl.BlockSpec(memory_space=pl.ANY)
    args = [lens, q, m, kv, x_own, w_out, first, column]
    if not last:
        args += [w_kv, w_in]
    tile = (chunks, n_data, crow, out_part)
    out_shape = [
        jax.ShapeDtypeStruct((rows, d_model) if last else tile, BF16),
        jax.ShapeDtypeStruct((2, n_data, depth, out_part), BF16),
    ]
    if not last:
        out_shape += [
            jax.ShapeDtypeStruct(tile, BF16),
            jax.ShapeDtypeStruct((n_group, n_data, 2, part, c), BF16),
        ]
    dma = pltpu.SemaphoreType.DMA
    return pl.pallas_call(
        kernel,
        out_shape=out_shape,
        in_specs=[pl.BlockSpec(memory_space=pltpu.SMEM)] + [anywhere] * (len(args) - 1),
        out_specs=[anywhere] * len(out_shape),
        scratch_shapes=[
            pltpu.VMEM((n_blocks, n_data, depth, out_part), BF16),
            pltpu.VMEM(q.shape, BF16),
            pltpu.VMEM(kv.shape, BF16),
            pltpu.VMEM((2, n_blocks, 2, n_mid, crow, c), BF16),
            pltpu.VMEM(tile, BF16),
            pltpu.VMEM(tile, BF16),
            pltpu.VMEM(tile, BF16),
            pltpu.VMEM((4, crow, out_part), BF16),
            pltpu.VMEM((n_model // 2, qrows, key_rows), F32),
            pltpu.VMEM((qrows, slab_len), F32),
            pltpu.VMEM((qrows, slab_len), F32),
            pltpu.VMEM((qrows, head_dim), F32),
            dma((SIDE_MATE + 7,)), dma((SIDE_MATE + 7,)), dma((13,)), dma((3, 2 * n_group)), dma((3, 2 * n_group)),
            dma((tiles,)), dma((tiles,)), dma((tiles,)), dma((tiles,)), dma((tiles,)), dma((tiles,)), dma((2,)), dma((2, chunks)),
        ],
        compiler_params=pltpu.CompilerParams(collective_id=2 * layer + 1, has_side_effects=True, vmem_limit_bytes=VMEM_LIMIT),
        cost_estimate=pl.CostEstimate(flops=4 * rows * n_blocks * depth * d_model, bytes_accessed=16 * rows * d_model, transcendentals=0),
        name=f"attend_and_sum_{layer}",
    )(*args)


def solution(mesh):
    batch_axes = ("rep", "data")
    n_data, n_model = mesh.shape["data"], mesh.shape["model"]
    n_chip = n_model // 2

    def near(x):
        return x + 1 - 2 * (x % 2)

    def across(x):
        return n_chip - 1 - x

    def on_chip(other):
        return lambda m: 2 * other(m // 2) + m % 2

    def local_step(x_loc, lens_loc, gamma_loc, w_in_loc, w_kv_loc, w_out_loc):
        n_batch, slab_len, d_model = x_loc.shape
        n_layers, part = gamma_loc.shape
        partners = [on_chip(near if layer % 2 == 0 else across) for layer in range(n_layers)]
        neighbours = [on_chip(across if layer % 2 == 0 else near) for layer in range(n_layers)]

        gain_rows = jnp.zeros((8, part), F32).at[:n_layers].set(gamma_loc.astype(F32))
        own = x_loc.reshape(n_batch * slab_len, d_model)
        for layer in range(n_layers):
            last = layer + 1 == n_layers
            following = min(layer + 1, n_layers - 1)
            if layer == 0:
                extra = (gain_rows,)
                q, m, kv, _, gains, out_first, out_column, in_first = project(
                    layer, n_data, n_model, partners[layer], neighbours[layer], neighbours[following],
                    own, w_kv_loc, w_in_loc, w_out_loc, extra,
                )
            else:
                extra = (other, gains, in_first, in_column)
                q, m, kv, _, out_first, out_column = project(
                    layer, n_data, n_model, partners[layer], neighbours[layer], neighbours[following],
                    own, w_kv_loc, w_in_loc, w_out_loc, extra,
                )
            outs = attend_and_sum(
                layer, last, n_data, n_model, partners[layer], neighbours[layer], partners[following],
                lens_loc, q, m, kv, own, w_in_loc, w_out_loc, w_kv_loc, out_first, out_column,
            )
            own = outs[0]
            if not last:
                other, in_column = outs[2:]
        return own.reshape(n_batch, slab_len, d_model)

    in_specs = (
        P(batch_axes, "model", None),
        P(batch_axes),
        P(None, "data"),
        P(None, "data", "model"),
        P(None, "data", None),
        P(None, "model", "data"),
    )
    return jax.shard_map(local_step, mesh=mesh, in_specs=in_specs, out_specs=P(batch_axes, "model", None), check_vma=False)
```

```python
import functools

import jax
import jax.numpy as jnp
from jax import lax
from jax.experimental import pallas as pl
from jax.experimental.pallas import tpu as pltpu
from jax.sharding import PartitionSpec as P

EPSILON = 1e-6
VMEM_LIMIT = 66_000_000
MESH = pl.DeviceIdType.MESH
BF16, F32 = jnp.bfloat16, jnp.float32

UP, DOWN, FORWARD, FORWARD_B, FIRST, SIDE_UP, SIDE_DOWN, FAR, MATE, SIDE_MATE = range(10)


def rms_norm(x_in, gain):
    x_f32 = x_in.astype(F32)
    inv_rms = lax.rsqrt(jnp.mean(x_f32 * x_f32, axis=-1, keepdims=True) + EPSILON)
    return (x_f32 * inv_rms * gain.astype(F32)).astype(BF16)


class Place:
    def __init__(self, n_data, n_model, partner, neighbour):
        self.n_data, self.n_model = n_data, n_model
        self.y = lax.axis_index("data")
        self.me = lax.axis_index("model")
        self.up = lax.rem(self.y + 1, n_data)
        self.down = lax.rem(self.y + n_data - 1, n_data)
        self.far = lax.rem(self.y + 2, n_data)
        self.slots = (self.y, self.down, self.up, self.far)
        self.mate = self.me + 1 - 2 * lax.rem(self.me, 2)
        self.partner, self.neighbour = partner(self.me), neighbour(self.me)
        n_other = n_model // 2 - 1
        self.ahead = [lax.rem(self.me + 2 * k, n_model) for k in range(1, n_other + 1)]
        self.behind = [lax.rem(self.me + n_model - 2 * k, n_model) for k in range(1, n_other + 1)]

    def meet(self):
        barrier = pltpu.get_barrier_semaphore()
        targets = [{"data": self.up}, {"data": self.down}, {"data": self.far}, {"model": self.mate}]
        targets += [{"model": m} for m in self.ahead]
        for target in targets:
            pl.semaphore_signal(barrier, inc=1, device_id=target, device_id_type=MESH)
        pl.semaphore_wait(barrier, len(targets))


def remote(src, dst, send, recv, target):
    return pltpu.make_async_remote_copy(
        src_ref=src, dst_ref=dst, send_sem=send, recv_sem=recv, device_id=target, device_id_type=MESH
    )


class GatherIn:
    def __init__(self, place, buf, pool, own, send, recv, local, first=None, column=None):
        self.place, self.buf, self.pool, self.own, self.first, self.column = place, buf, pool, own, first, column
        self.send, self.recv, self.local = send, recv, local

    def at(self, block, g, slot):
        return self.buf.at[block, g, slot]

    def _copy(self, src, dst, kind, at, target):
        return remote(src, dst, self.send.at[kind, at], self.recv.at[kind, at], target)

    def up(self, g, half):
        dst = self.at(0, g, self.place.y).at[half]
        return self._copy(self.own(g, half), dst, UP, 2 * g + half, {"data": self.place.up})

    def down(self, g, half):
        dst = self.at(0, g, self.place.y).at[half]
        return self._copy(self.own(g, half), dst, DOWN, 2 * g + half, {"data": self.place.down})

    def neighbour_first(self, g, half):
        dst = self.at(2, g, self.place.y).at[half]
        return self._copy(self.own(g, half), dst, FIRST, 2 * g + half, {"model": self.place.neighbour})

    def forward(self, g, half):
        ref = self.at(0, g, (self.place.down, self.place.up)[half]).at[half]
        target = (self.place.up, self.place.down)[half]
        return self._copy(ref, ref, FORWARD, 2 * g + half, {"data": target})

    def _needed(self, ref, g):
        return ref.at[0] if isinstance(g, int) and g == 0 else ref

    def _side(self, g, kind, target):
        src = self.at(2, g, self.place.y) if self.first is None else self.first.at[g]
        dst = self.at(2, g, self.place.y)
        return self._copy(self._needed(src, g), self._needed(dst, g), kind, g, {"data": target})

    def side_up(self, g):
        return self._side(g, SIDE_UP, self.place.up)

    def side_down(self, g):
        return self._side(g, SIDE_DOWN, self.place.down)

    def far(self, g):
        slot = self.place.far
        src = self.at(0, g, slot) if self.column is None else self.column.at[g, slot]
        dst = self.at(2, g, slot)
        return self._copy(self._needed(src, g), self._needed(dst, g), FAR, g, {"model": self.place.neighbour})

    def mate(self, g):
        return self._copy(self.buf.at[0, g], self.pool.at[0, g], MATE, g, {"model": self.place.mate})

    def side_mate(self, g):
        src, dst = self.buf.at[2, g], self.pool.at[1, g]
        if isinstance(g, int) and g == 0:
            src, dst = src.at[:, 0], dst.at[:, 0]
        return self._copy(src, dst, SIDE_MATE, g, {"model": self.place.mate})

    def load_mate(self, g):
        return pltpu.make_async_copy(self.pool.at[0, g], self.buf.at[1, g], self.local.at[6, g])

    def load_side(self, g):
        src, dst = self.pool.at[1, g], self.buf.at[3, g]
        if isinstance(g, int) and g == 0:
            src, dst = src.at[:, 0], dst.at[:, 0]
        return pltpu.make_async_copy(src, dst, self.local.at[7, g])

    def take_mate(self, g):
        self.mate(g).wait_recv()
        self.load_mate(g).start()

    def take_side(self, g):
        self.side_mate(g).wait_recv()
        self.load_side(g).start()

    def load_own(self, g, half):
        dst = self.at(0, g, self.place.y).at[half]
        return pltpu.make_async_copy(self.own(g, half), dst, self.local.at[half, g])

    def load_column(self, g, which):
        slot = self.place.slots[which]
        return pltpu.make_async_copy(self.column.at[g, slot], self.at(0, g, slot), self.local.at[1 + which, g])

    def load_first(self, g):
        return pltpu.make_async_copy(self.first.at[g], self.at(2, g, self.place.y), self.local.at[5, g])

    def pass_side(self, g):
        if self.first is not None:
            self.load_first(g).wait()
        self.side_up(g).wait_recv()
        self.side_down(g).wait_recv()
        self.far(g).wait_recv()
        self.side_mate(g).start()

    def wait_sends(self, g):
        made = [self.side_up(g), self.side_down(g), self.far(g), self.mate(g), self.side_mate(g)]
        if self.column is None:
            made += [copy(g, half) for copy in (self.up, self.down, self.forward) for half in range(2)]
        if self.first is None:
            made += [self.neighbour_first(g, half) for half in range(2)]
        for copy in made:
            copy.wait_send()


class FetchIn:
    def __init__(self, place, own, send, recv, neighbour=None, first=None, column=None):
        self.place, self.own, self.send, self.recv = place, own, send, recv
        self.neighbour, self.first, self.column = neighbour, first, column

    def _ring(self, g, half, kind, target):
        at = 2 * g + half
        dst = self.column.at[g, self.place.y, half]
        return remote(self.own(g, half), dst, self.send.at[kind, at], self.recv.at[kind, at], {"data": target})

    def up(self, g, half):
        return self._ring(g, half, 0, self.place.up)

    def down(self, g, half):
        return self._ring(g, half, 1, self.place.down)

    def forward(self, g, half):
        at = 2 * g + half
        ref = self.column.at[g, (self.place.down, self.place.up)[half], half]
        target = (self.place.up, self.place.down)[half]
        return remote(ref, ref, self.send.at[2, at], self.recv.at[2, at], {"data": target})

    def ring_stage(self, g):
        for half in range(2):
            self.up(g, half).wait_recv()
            self.down(g, half).wait_recv()
        for half in range(2):
            self.forward(g, half).start()

    def send_slices(self, g):
        for half in range(2):
            self.up(g, half).start()
            self.down(g, half).start()

    def neighbour_first(self, g, half):
        at = 2 * g + half
        dst = self.first.at[g, half]
        return remote(self.own(g, half), dst, self.send.at[3, at], self.recv.at[3, at], {"model": self.neighbour})


class GatherOut:
    def __init__(self, place, buf, own, send, recv, local=None, first=None, column=None, pool=None, whole_column=True):
        self.place, self.buf, self.own, self.first, self.column = place, buf, own, first, column
        self.far_held = column is not None and whole_column
        self.send, self.recv, self.local, self.pool = send, recv, local, pool

    def _copy(self, src, dst, kind, target):
        return remote(src, dst, self.send.at[kind], self.recv.at[kind], target)

    def up(self):
        return self._copy(self.own, self.buf.at[0, self.place.y], UP, {"data": self.place.up})

    def down(self):
        return self._copy(self.own, self.buf.at[0, self.place.y], DOWN, {"data": self.place.down})

    def _half(self, ref, second):
        size = ref.shape[0] // 2
        return ref.at[pl.ds(second * size, size)]

    def _forward(self, kind, slot, second, target):
        src = self.buf if self.column is None else self.column
        dst = self._half(self.buf.at[0, slot], second)
        return self._copy(self._half(src.at[0, slot], second), dst, kind, {"data": target})

    def forward(self):
        return self._forward(FORWARD, self.place.down, 0, self.place.up)

    def forward_b(self):
        return self._forward(FORWARD_B, self.place.up, 1, self.place.down)

    def neighbour_first(self, dst):
        return self._copy(self.own, dst, FIRST, {"model": self.place.neighbour})

    def side_up(self):
        return self._copy(self.first, self.buf.at[2, self.place.y], SIDE_UP, {"data": self.place.up})

    def side_down(self):
        return self._copy(self.first, self.buf.at[2, self.place.y], SIDE_DOWN, {"data": self.place.down})

    def far(self):
        slot = self.place.far
        src = self.column.at[0, slot] if self.far_held else self.buf.at[0, slot]
        return self._copy(src, self.buf.at[2, slot], FAR, {"model": self.place.neighbour})

    def mate(self, which):
        slot = self.place.slots[which]
        if which == 0:
            src = self.own
        else:
            src = self.column.at[0, slot] if which < 3 or self.far_held else self.buf.at[0, slot]
        return self._copy(src, self.pool.at[0, slot], MATE + 2 * which, {"model": self.place.mate})

    def side_mate(self, which):
        slot = self.place.slots[which]
        src = self.first if which == 0 else self.buf.at[2, slot]
        return self._copy(src, self.pool.at[1, slot], SIDE_MATE + 2 * which, {"model": self.place.mate})

    def load_mate(self, which):
        slot = self.place.slots[which]
        return pltpu.make_async_copy(self.pool.at[0, slot], self.buf.at[1, slot], self.local.at[5 + which])

    def load_side(self, which):
        slot = self.place.slots[which]
        return pltpu.make_async_copy(self.pool.at[1, slot], self.buf.at[3, slot], self.local.at[9 + which])

    def take(self, which):
        self.mate(which).wait_recv()
        self.load_mate(which).start()
        self.side_mate(which).wait_recv()
        self.load_side(which).start()

    def load_own(self):
        return pltpu.make_async_copy(self.own, self.buf.at[0, self.place.y], self.local.at[0])

    def load_column(self, which):
        slot = self.place.slots[which]
        return pltpu.make_async_copy(self.column.at[0, slot], self.buf.at[0, slot], self.local.at[which])

    def load_first(self):
        return pltpu.make_async_copy(self.first, self.buf.at[2, self.place.y], self.local.at[4])


def in_halves(layer, w_kv_ref, w_ref, c, ff):
    def own(g, half):
        if isinstance(g, int) and g == 0:
            return w_kv_ref.at[layer] if half else w_ref.at[layer, :, pl.ds(0, c)]
        return w_ref.at[layer, :, pl.ds(pl.multiple_of(g * c + half * ff, c), c)]

    return own


def project(layer, n_data, n_model, partner, neighbour, next_neighbour, x_own, w_kv, w_in, w_out, extra):
    start_layer = layer == 0
    part, c = w_kv.shape[1:]
    d_model = part * n_data
    rows = x_own.size // d_model
    depth, out_part = w_out.shape[1:]
    ff = depth - c
    n_group = 1 + ff // c
    n_units = 8 * n_group
    row_parts = 4
    row_part = rows // row_parts
    n_other = n_model // 2 - 1
    gain_shape = (n_data, 8, part)
    n_tiles = 1 if start_layer else x_own.shape[0] * x_own.shape[1]

    def kernel(*refs):
        x_ref, w_kv_ref, w_ref, wo_ref = refs[:4]
        if start_layer:
            gain_ref = refs[4]
            q_ref, m_ref, kv_ref, pool_ref, gains_ref, out_first_ref, out_column_ref, in_first_ref = refs[5:13]
            first_ref = column_ref = None
            rest = refs[13:]
        else:
            par_ref, gain_ref, first_ref, column_ref = refs[4:8]
            q_ref, m_ref, kv_ref, pool_ref, out_first_ref, out_column_ref = refs[8:14]
            rest = refs[14:]
        wbuf, h_ref, gbuf, stage, kv_stage, send, recv, w_local, next_send, next_recv, late_send, late_recv = rest[:12]
        x_send, x_recv, g_send, g_recv, kv_send, kv_recv, local, out_sem, tile_sem = rest[12:]

        place = Place(n_data, n_model, partner, neighbour)
        place.meet()
        in_own = in_halves(layer, w_kv_ref, w_ref, c, ff)
        w = GatherIn(place, wbuf, pool_ref, in_own, send, recv, w_local, first_ref, column_ref)
        out_next = GatherOut(place, out_column_ref, wo_ref.at[layer], next_send, next_recv)
        if start_layer:
            in_own_next = in_halves(layer + 1, w_kv_ref, w_ref, c, ff)
            in_next = FetchIn(place, in_own_next, late_send, late_recv, next_neighbour(place.me), in_first_ref)

        def c_x(part_no):
            piece = pl.ds(part_no * row_part, row_part)
            return remote(
                x_ref.at[piece], h_ref.at[1, piece], x_send.at[part_no], x_recv.at[part_no], {"model": place.partner}
            )

        def c_gain(which):
            target = {"data": (place.up, place.down, place.far)[which]}
            return remote(gain_ref, gbuf.at[place.y], g_send.at[which], g_recv.at[which], target)

        def c_kv(which):
            ref = kv_ref.at[place.me]
            return remote(ref, ref, kv_send.at[which], kv_recv.at[which], {"model": place.ahead[which]})

        def c_kv_mate(which):
            ref = kv_ref.at[place.me if which == 0 else place.behind[which - 1]]
            at = n_other + which
            return remote(ref, ref, kv_send.at[at], kv_recv.at[at], {"model": place.mate})

        save_kv = pltpu.make_async_copy(kv_stage, kv_ref.at[place.me], local.at[0])
        if start_layer:
            load_x = pltpu.make_async_copy(x_ref, h_ref.at[0], local.at[0])

        def load_tile(side, k):
            chunk, slot = k // n_data, lax.rem(k, n_data)
            src = (x_ref, par_ref)[side].at[chunk, slot]
            height, across = src.shape
            down_to, along = pl.multiple_of(chunk * height, height), pl.multiple_of(slot * across, across)
            return pltpu.make_async_copy(src, h_ref.at[side, pl.ds(down_to, height), pl.ds(along, across)], tile_sem.at[side, k])

        if start_layer:
            load_gain = pltpu.make_async_copy(gain_ref, gbuf.at[place.y], local.at[1])
            for which in range(3):
                c_gain(which).start()
        else:
            load_gain = pltpu.make_async_copy(gain_ref, gbuf, local.at[1])
        def send_slices(g):
            for half in range(2):
                w.up(g, half).start()
                w.down(g, half).start()

        load_gain.start()
        if start_layer:
            load_x.start()
        else:
            for side in range(2):

                @pl.loop(0, n_tiles)
                def _(k):
                    load_tile(side, k).start()

        if start_layer:
            send_slices(0)
            for g in range(n_group):
                for half in range(2):
                    w.neighbour_first(g, half).start()
                    w.load_own(g, half).start()
            for part_no in range(row_parts // 2):
                c_x(part_no).start()
        else:
            for g in range(n_group):
                for half in range(2):
                    w.load_own(g, half).start()
                for which in range(1, 4):
                    w.load_column(g, which).start()
                w.side_up(g).start()
                w.side_down(g).start()
                if g < 2:
                    w.far(g).start()
            for g in range(n_group):
                w.load_first(g).start()

        def ring_stage(g):
            for half in range(2):
                w.up(g, half).wait_recv()
                w.down(g, half).wait_recv()
            for half in range(2):
                w.forward(g, half).start()

        def column_stage(g):
            for half in range(2):
                w.load_own(g, half).wait()
            for which in range(1, 4):
                w.load_column(g, which).wait()
            w.mate(g).start()

        if start_layer:
            for which in range(3):
                c_gain(which).wait_recv()
        load_gain.wait()
        gain = jnp.concatenate([gbuf[k, layer:layer + 1, :] for k in range(n_data)], axis=1)
        if start_layer:
            save_gain = pltpu.make_async_copy(gbuf, gains_ref, local.at[1])
            save_gain.start()
        if start_layer:
            load_x.wait()
        else:

            @pl.loop(0, n_tiles)
            def _(k):
                load_tile(0, k).wait()

        def norm_rows(side, part_no):
            piece = pl.ds(part_no * row_part, row_part)
            h_ref[side, piece] = rms_norm(h_ref[side, piece], gain)

        @pl.loop(0, row_parts)
        def _(part_no):
            norm_rows(0, part_no)

        if start_layer:
            send_slices(1)
            ring_stage(0)
        else:
            column_stage(0)

        halfway, quarter = n_units // 2, n_units // 4

        def out_copy(slot, blk, side, g):
            def to_q():
                return pltpu.make_async_copy(stage.at[slot], q_ref.at[blk, side], out_sem.at[slot])

            def to_m():
                return pltpu.make_async_copy(stage.at[slot], m_ref.at[blk, side, g - 1], out_sem.at[slot])

            return to_q, to_m

        @pl.loop(0, n_units)
        def _(step):
            late = step - halfway
            if start_layer:
                opening, second = step < quarter, (step >= quarter) & (step < halfway)
                ahead = (step == 0) | ((lax.rem(step, 2) == 1) & (step < quarter - 1))
                open_g = jnp.where(ahead, (step + 1) // 2, jnp.where(step == quarter - 1, n_group - 1, step // 2 - 1))
                g = jnp.where(opening, open_g, jnp.where(second, (step - quarter) // 2, late // 4))
                open_blk = jnp.where(ahead, 0, 1)
                blk = jnp.where(opening, open_blk, jnp.where(second, lax.rem(step, 2), 2 + lax.rem(late, 4) // 2))
                side = jnp.where(opening, 0, jnp.where(second, 1, lax.rem(late, 2)))

                @pl.when(opening & (blk == 0))
                def _():
                    for half in range(2):
                        w.forward(g, half).wait_recv()

                    @pl.when(g + 2 < n_group)
                    def _():
                        send_slices(g + 2)

                    @pl.when(g + 1 < n_group)
                    def _():
                        ring_stage(g + 1)

                    @pl.when(g + 2 == n_group)
                    def _():
                        for k in range(n_group):
                            for half in range(2):
                                w.neighbour_first(k, half).wait_recv()
                            w.side_up(k).start()
                            w.side_down(k).start()

                    @pl.when(g == 0)
                    def _():
                        w.far(0).start()

                    @pl.when(g > 0)
                    def _():
                        w.far(g).start()

                    @pl.when(g == 1)
                    def _():
                        for part_no in range(row_parts // 2, row_parts):
                            c_x(part_no).start()

                    for half in range(2):
                        w.load_own(g, half).wait()
                    w.mate(g).start()

                    @pl.when(g > 0)
                    def _():
                        w.take_mate(g - 1)

                @pl.when(step == quarter - 2)
                def _():
                    w.take_mate(n_group - 1)

                @pl.when(opening & (blk == 1))
                def _():
                    w.load_mate(g).wait()

                @pl.when(step == quarter)
                def _():
                    @pl.loop(0, row_parts)
                    def _(part_no):
                        c_x(part_no).wait_recv()
                        norm_rows(1, part_no)

                    out_next.neighbour_first(out_first_ref).start()
                    out_next.up().start()
                    out_next.down().start()
                    for k in range(n_group):
                        for half in range(2):
                            in_next.neighbour_first(k, half).start()
            else:
                g = jnp.where(late < 0, step, late) // 4
                blk = jnp.where(late < 0, 0, 2) + lax.rem(step, 4) // 2
                side = lax.rem(step, 2)

                @pl.when((late < 0) & (lax.rem(step, 4) == 0) & (g + 1 < n_group))
                def _():
                    column_stage(g + 1)

                @pl.when(step == 1)
                def _():
                    @pl.loop(0, n_tiles)
                    def _(k):
                        load_tile(1, k).wait()

                    @pl.loop(0, row_parts)
                    def _(part_no):
                        norm_rows(1, part_no)

                @pl.when((late < 0) & (lax.rem(step, 4) == 1))
                def _():
                    w.take_mate(g)

                @pl.when((late < 0) & (lax.rem(step, 4) == 2))
                def _():
                    w.load_mate(g).wait()

                @pl.when(step == n_units - 6)
                def _():
                    out_next.up().wait_recv()
                    out_next.down().wait_recv()
                    out_next.forward().start()
                    out_next.forward_b().start()

            @pl.when(step == halfway - 2)
            def _():
                w.pass_side(0)

            @pl.when(step == halfway + 1)
            def _():
                w.take_side(0)

            @pl.when((late > 1) & (lax.rem(late, 4) == 1))
            def _():
                w.take_side(g)

            @pl.when((late >= 0) & (lax.rem(late, 4) == 2))
            def _():
                @pl.when(g + 1 < n_group)
                def _():
                    w.pass_side(g + 1)

                @pl.when(g == 0)
                def _():
                    w.load_side(0).wait()

                @pl.when(g > 0)
                def _():
                    w.load_side(g).wait()

            slot = lax.rem(step, 2)
            to_q, to_m = out_copy(slot, blk, side, g)

            @pl.when(step >= 2)
            def _():
                to_q().wait()

            def columns(half):
                return wbuf[blk, g, :, half].reshape(d_model, c)

            @pl.when(g == 0)
            def _():
                q = jnp.dot(h_ref[side], columns(0), preferred_element_type=F32)
                stage[slot] = q.astype(BF16)
                to_q().start()

            @pl.when(g > 0)
            def _():
                h_val = h_ref[side]
                gate = jnp.dot(h_val, columns(0), preferred_element_type=F32).astype(BF16).astype(F32)
                raised = jnp.dot(h_val, columns(1), preferred_element_type=F32).astype(BF16).astype(F32)
                stage[slot] = (gate * jax.nn.sigmoid(gate) * raised).astype(BF16)
                to_m().start()

            @pl.when(step == 0)
            def _():
                kv_stage[...] = jnp.dot(h_ref[0], columns(1), preferred_element_type=F32).astype(BF16)
                save_kv.start()

            @pl.when(step == 1)
            def _():
                save_kv.wait()
                for which in range(n_other):
                    c_kv(which).start()
                c_kv_mate(0).start()
                if not start_layer:
                    for k in range(2, n_group):
                        w.far(k).start()

            @pl.when(step == n_units - 4)
            def _():
                for which in range(n_other):
                    c_kv(which).wait_recv()
                    c_kv_mate(1 + which).start()

            if not start_layer:

                @pl.when(step == 8)
                def _():
                    out_next.up().start()
                    out_next.down().start()
                    out_next.neighbour_first(out_first_ref).start()
        for which in range(n_other + 1):
            c_kv_mate(which).wait()
        for which in range(n_other):
            c_kv(which).wait_send()
        if start_layer:
            save_gain.wait()
            for which in range(3):
                c_gain(which).wait_send()
            for part_no in range(row_parts):
                c_x(part_no).wait_send()
            for g in range(n_group):
                for half in range(2):
                    in_next.neighbour_first(g, half).wait()
            for copy in (out_next.up(), out_next.down()):
                copy.wait()
        else:
            for copy in (out_next.forward(), out_next.forward_b()):
                copy.wait()
            for copy in (out_next.up(), out_next.down()):
                copy.wait_send()
        out_next.neighbour_first(out_first_ref).wait()
        for slot in range(2):
            pltpu.make_async_copy(stage.at[slot], q_ref.at[0, 0], out_sem.at[slot]).wait()

        for g in range(n_group):
            w.wait_sends(g)

    anywhere = pl.BlockSpec(memory_space=pl.ANY)
    out_shape = [
        jax.ShapeDtypeStruct((4, 2, rows, c), BF16),
        jax.ShapeDtypeStruct((4, 2, n_group - 1, rows, c), BF16),
        jax.ShapeDtypeStruct((n_model, rows, c), BF16),
        jax.ShapeDtypeStruct((2, n_group, n_data, 2, part, c), BF16),
    ]
    if start_layer:
        out_shape += [
            jax.ShapeDtypeStruct(gain_shape, F32),
            jax.ShapeDtypeStruct((depth, out_part), BF16),
            jax.ShapeDtypeStruct((1, n_data, depth, out_part), BF16),
            jax.ShapeDtypeStruct((n_group, 2, part, c), BF16),
        ]
    else:
        out_shape += [
            jax.ShapeDtypeStruct((depth, out_part), BF16),
            jax.ShapeDtypeStruct((1, n_data, depth, out_part), BF16),
        ]
    dma = pltpu.SemaphoreType.DMA
    args = (x_own, w_kv, w_in, w_out) + tuple(extra)
    return pl.pallas_call(
        kernel,
        out_shape=out_shape,
        in_specs=[anywhere] * len(args),
        out_specs=[anywhere] * len(out_shape),
        scratch_shapes=[
            pltpu.VMEM((4, n_group, n_data, 2, part, c), BF16),
            pltpu.VMEM((2, rows, d_model), BF16),
            pltpu.VMEM(gain_shape, F32),
            pltpu.VMEM((2, rows, c), BF16),
            pltpu.VMEM((rows, c), BF16),
            dma((SIDE_MATE + 1, 2 * n_group)), dma((SIDE_MATE + 1, 2 * n_group)), dma((8, n_group)),
            dma((FIRST + 1,)), dma((FIRST + 1,)), dma((4, 2 * n_group)), dma((4, 2 * n_group)),
            dma((row_parts,)), dma((row_parts,)), dma((3,)), dma((3,)),
            dma((n_model - 1,)), dma((n_model - 1,)), dma((3,)), dma((2,)), dma((2, n_tiles)),
        ],
        compiler_params=pltpu.CompilerParams(collective_id=2 * layer, has_side_effects=True, vmem_limit_bytes=VMEM_LIMIT),
        cost_estimate=pl.CostEstimate(flops=4 * rows * d_model * 4 * (c + 2 * ff), bytes_accessed=16 * rows * d_model, transcendentals=0),
        name=f"project_{layer}",
    )(*args)


def pick(step, values):
    found = jnp.int32(values[0])
    for at in range(1, len(values)):
        if values[at] != values[at - 1]:
            found = jnp.where(step >= at, jnp.int32(values[at]), found)
    return found


def attend_and_sum(layer, last, n_data, n_model, partner, neighbour, next_partner, lens, q, m, kv, x_own, w_in, w_out, w_kv, first, column):
    n_blocks, _, rows, c = q.shape
    n_mid = m.shape[2]
    ff = n_mid * c
    d_model = w_out.shape[2] * n_data
    tiled = x_own.ndim == 4
    depth, out_part = w_out.shape[1:]
    head_dim = c // 2
    n_batch = lens.shape[0]
    slab_len = rows // n_batch
    chunks = 4
    n_seq = n_batch // chunks
    crow = rows // chunks
    tiles = chunks * n_data
    heads = n_blocks * 2
    qrows = heads * slab_len
    key_rows = 2 * slab_len
    scale = head_dim ** -0.5 * 1.4426950408889634
    part = w_kv.shape[1]
    n_group = 1 + ff // c
    if layer == 0:
        order = [(0, 0), (1, 0), (2, 0), (0, 1), (1, 1), (2, 1), (0, 2), (1, 2), (2, 2)]
        order += [(3, 0), (3, 1), (3, 2), (0, 3), (1, 3), (2, 3), (3, 3)]
        opens = (0, 1, 2, 9)
        side_step, far_step = 2, 11
    else:
        order = [(0, 0), (1, 0), (0, 1), (1, 1), (0, 2), (1, 2), (2, 0), (2, 1), (2, 2), (0, 3), (1, 3), (2, 3)]
        order += [(3, which) for which in range(4)]
        opens = (0, 1, 6, 12)
        side_step, far_step = 1, 8
    flying = 3
    settles = {2: (0,), 3: (1,)}
    for at in range(5, tiles):
        settles[at] = (at - flying,)
    held = sum(len(some) for some in settles.values())
    whole_column = layer > 0

    def kernel(*refs):
        lens_ref, q_ref, m_ref, kv_ref, x_ref, wo_ref, first_ref = refs[:7]
        at = 7
        column_ref = refs[at]
        at += 1
        if not last:
            w_kv_ref, wi_ref = refs[at:at + 2]
            at += 2
        y_ref, pool_ref = refs[at:at + 2]
        at += 2
        if not last:
            par_ref, in_column_ref = refs[at:at + 2]
            at += 2
        (wbuf, obuf, kvb, mbuf, xb, zb, zr, z_stage, s_ref, mx_ref, sum_ref, acc_ref,
         send, recv, w_local, in_send, in_recv, z_send, z_recv, y_send, y_recv, y_save, x_sem, m_sem, local) = refs[at:]

        place = Place(n_data, n_model, partner, neighbour)
        place.meet()
        w = GatherOut(place, wbuf, wo_ref.at[layer], send, recv, w_local, first_ref, column_ref, pool_ref, whole_column)

        def tile_of(k):
            which = pick(k, [one for _, one in order])
            slot = jnp.where(which == 0, place.y, jnp.where(which == 1, place.down, jnp.where(which == 2, place.up, place.far)))
            return pick(k, [one for one, _ in order]), which, slot

        def whole(ref, chunk, slot):
            return ref.at[pl.ds(pl.multiple_of(chunk * crow, crow), crow), pl.ds(pl.multiple_of(slot * out_part, out_part), out_part)]

        def rows_of(chunk):
            return pl.ds(pl.multiple_of(chunk * crow, crow), crow)

        def load_q(chunk):
            return pltpu.make_async_copy(q_ref.at[:, :, rows_of(chunk)], obuf.at[:, :, rows_of(chunk)], local.at[0, chunk])

        def load_kv(chunk):
            return pltpu.make_async_copy(kv_ref.at[:, rows_of(chunk)], kvb.at[:, rows_of(chunk)], local.at[1, chunk])

        def load_m(k):
            chunk, _, _ = tile_of(k)
            slot = lax.rem(k, 2)
            return pltpu.make_async_copy(
                m_ref.at[:, :, :, pl.ds(pl.multiple_of(chunk * crow, crow), crow)], mbuf.at[slot], m_sem.at[slot]
            )

        def load_x(k):
            chunk, _, slot = tile_of(k)
            src = x_ref.at[chunk, slot] if tiled else whole(x_ref, chunk, slot)
            return pltpu.make_async_copy(src, xb.at[chunk, slot], x_sem.at[k])

        def c_z(k):
            chunk, _, slot = tile_of(k)
            return remote(z_stage.at[lax.rem(k, 4)], zr.at[chunk, slot], z_send.at[k], z_recv.at[k], {"model": place.partner})

        def c_y(k):
            chunk, _, slot = tile_of(k)
            target = {"model": next_partner(place.me)}
            return remote(xb.at[chunk, slot], par_ref.at[chunk, slot], y_send.at[k], y_recv.at[k], target)

        def save_y(k):
            chunk, _, slot = tile_of(k)
            dst = whole(y_ref, chunk, slot) if last else y_ref.at[chunk, slot]
            return pltpu.make_async_copy(xb.at[chunk, slot], dst, y_save.at[k])

        for chunk in range(chunks):
            load_q(chunk).start()
            load_kv(chunk).start()
        load_m(0).start()
        w.load_own().start()
        w.load_first().start()
        w.mate(0).start()
        w.side_mate(0).start()
        for which in range(1, 4 if whole_column else 3):
            w.load_column(which).start()
            w.mate(which).start()
        w.side_up().start()
        w.side_down().start()
        if whole_column:
            w.far().start()
        else:
            w.forward().start()
            w.forward_b().start()
        if not last:
            in_own = in_halves(layer + 1, w_kv_ref, wi_ref, c, ff)
            in_next = FetchIn(place, in_own, in_send, in_recv, column=in_column_ref)

        @pl.loop(0, tiles)
        def _(k):
            load_x(k).start()

        def attend_one(batch, side):
            slab = jnp.where(side == 0, place.me, place.partner)
            length = lens_ref[batch]
            n_key = slab // 2 + 1
            at_row = pl.ds(pl.multiple_of(batch * slab_len, slab_len), slab_len)
            parts = []
            for blk in range(n_blocks):
                for one in range(2):
                    parts.append(obuf[blk, side, at_row, one * head_dim:(one + 1) * head_dim])
            q_val = jnp.concatenate(parts, axis=0)
            row_pos = slab * slab_len + lax.rem(lax.broadcasted_iota(jnp.int32, (qrows, key_rows), 0), slab_len)
            key_pos = lax.broadcasted_iota(jnp.int32, (qrows, key_rows), 1)
            room = jnp.minimum(row_pos + 1, length) - key_pos
            mx_ref[...] = jnp.full_like(mx_ref, -1e30)

            def score(kb, carry):
                k = kvb[pl.ds(2 * kb, 2), at_row, :head_dim].reshape(key_rows, head_dim)
                s = lax.dot_general(q_val, k, (((1,), (1,)), ((), ())), preferred_element_type=F32) * scale
                s = jnp.where(room > kb * key_rows, s, -1e30)
                s_ref[kb] = s
                mx_ref[...] = jnp.maximum(mx_ref[...], jnp.maximum(s[:, :slab_len], s[:, slab_len:]))
                return carry

            lax.fori_loop(0, n_key, score, 0)
            top = jnp.max(mx_ref[...], axis=-1, keepdims=True)
            mx_ref[...] = jnp.broadcast_to(top, mx_ref.shape)
            sum_ref[...] = jnp.zeros_like(sum_ref)
            acc_ref[...] = jnp.zeros_like(acc_ref)

            def weigh(kb, carry):
                v = kvb[pl.ds(2 * kb, 2), at_row, head_dim:].reshape(key_rows, head_dim)
                top_b = mx_ref[...]
                e_lo = jnp.exp2(s_ref[kb, :, :slab_len] - top_b)
                e_hi = jnp.exp2(s_ref[kb, :, slab_len:] - top_b)
                sum_ref[...] += e_lo + e_hi
                e = jnp.concatenate([e_lo, e_hi], axis=1).astype(BF16)
                acc_ref[...] += jnp.dot(e, v, preferred_element_type=F32)
                return carry

            lax.fori_loop(0, n_key, weigh, 0)
            out = (acc_ref[...] / jnp.sum(sum_ref[...], axis=-1, keepdims=True)).astype(BF16)
            for blk in range(n_blocks):
                for one in range(2):
                    first_row = (blk * 2 + one) * slab_len
                    obuf[blk, side, at_row, one * head_dim:(one + 1) * head_dim] = out[first_row:first_row + slab_len]

        def settle(k):
            chunk, _, slot = tile_of(k)
            load_x(k).wait()
            c_z(k).wait_recv()
            z = zb[chunk, slot].astype(F32) + zr[chunk, slot].astype(F32)
            xb[chunk, slot] = (xb[chunk, slot].astype(F32) + z).astype(BF16)
            save_y(k).start()
            if not last:
                c_y(k).start()

        @pl.loop(0, tiles)
        def _(step):
            chunk, which, slot = tile_of(step)

            @pl.when(step + 1 < tiles)
            def _():
                load_m(step + 1).start()

            opening = functools.reduce(lambda one, other: one | other, [step == at for at in opens])

            @pl.when(opening)
            def _():
                load_q(chunk).wait()
                load_kv(chunk).wait()

                @pl.loop(0, 2 * n_seq)
                def _(unit):
                    attend_one(chunk * n_seq + unit // 2, lax.rem(unit, 2))

            @pl.when(step == 0)
            def _():
                w.load_own().wait()
                w.load_first().wait()
                w.take(0)
                w.load_mate(0).wait()
                w.load_side(0).wait()

            @pl.when(step == side_step)
            def _():
                w.side_up().wait_recv()
                w.side_mate(1).start()
                w.side_down().wait_recv()
                w.side_mate(2).start()

            @pl.when(step == side_step + 1)
            def _():
                for one in (1, 2):
                    w.take(one)
                for one in (1, 2):
                    w.load_column(one).wait()
                    w.load_mate(one).wait()
                    w.load_side(one).wait()

            if not whole_column:

                @pl.when(step == side_step + 2)
                def _():
                    w.forward().wait_recv()
                    w.forward_b().wait_recv()
                    w.far().start()
                    w.mate(3).start()

            @pl.when(step == far_step)
            def _():
                w.far().wait_recv()
                w.side_mate(3).start()

            @pl.when(step == far_step + 1)
            def _():
                w.take(3)
                if whole_column:
                    w.load_column(3).wait()
                w.load_mate(3).wait()
                w.load_side(3).wait()

            if not last:
                for g, at in enumerate((3, 3, 4, 5, 6)[:n_group]):

                    @pl.when(step == at)
                    def _(g=g):
                        in_next.send_slices(g)

                for g, at in enumerate((9, 10, 12, 15)[:n_group]):

                    @pl.when(step == at)
                    def _(g=g):
                        in_next.ring_stage(g)

            @pl.when(step >= flying)
            def _():
                c_z(step - flying).wait_send()

            load_m(step).wait()
            here = lax.rem(step, 2)
            rows_c = pl.ds(pl.multiple_of(chunk * crow, crow), crow)
            total = None
            for blk in range(n_blocks):
                mid = jnp.concatenate([mbuf[here, blk, :, k].reshape(2 * crow, c) for k in range(n_mid)], axis=1)
                attn = obuf[blk, :, rows_c, :].reshape(2 * crow, c)
                one = jnp.dot(mid, wbuf[blk, slot, c:, :], preferred_element_type=F32)
                one = one + jnp.dot(attn, wbuf[blk, slot, :c, :], preferred_element_type=F32)
                total = one if total is None else total + one
            z = total.astype(BF16)
            zb[chunk, slot] = z[:crow]
            z_stage[lax.rem(step, 4)] = z[crow:]
            c_z(step).start()

            for at, some in settles.items():

                @pl.when(step == at)
                def _(some=some):
                    for k in some:
                        settle(k)

        stages = list(range(4, n_group)) if not last else []
        for k in range(held, tiles):
            if stages and k - held >= 2:
                in_next.ring_stage(stages.pop(0))
            settle(k)
        for g in stages:
            in_next.ring_stage(g)

        @pl.loop(0, tiles)
        def _(k):
            save_y(k).wait()
            if not last:
                c_y(k).wait()

        @pl.loop(tiles - flying, tiles)
        def _(k):
            c_z(k).wait_send()

        made = [w.side_up(), w.side_down(), w.far()]
        made += [w.mate(which) for which in range(4)] + [w.side_mate(which) for which in range(4)]
        if not whole_column:
            made += [w.forward(), w.forward_b()]
        for copy in made:
            copy.wait_send()
        if not last:

            @pl.loop(0, n_group)
            def _(g):
                for half in range(2):
                    in_next.forward(g, half).wait()
                    in_next.up(g, half).wait_send()
                    in_next.down(g, half).wait_send()

    anywhere = pl.BlockSpec(memory_space=pl.ANY)
    args = [lens, q, m, kv, x_own, w_out, first, column]
    if not last:
        args += [w_kv, w_in]
    tile = (chunks, n_data, crow, out_part)
    out_shape = [
        jax.ShapeDtypeStruct((rows, d_model) if last else tile, BF16),
        jax.ShapeDtypeStruct((2, n_data, depth, out_part), BF16),
    ]
    if not last:
        out_shape += [
            jax.ShapeDtypeStruct(tile, BF16),
            jax.ShapeDtypeStruct((n_group, n_data, 2, part, c), BF16),
        ]
    dma = pltpu.SemaphoreType.DMA
    return pl.pallas_call(
        kernel,
        out_shape=out_shape,
        in_specs=[pl.BlockSpec(memory_space=pltpu.SMEM)] + [anywhere] * (len(args) - 1),
        out_specs=[anywhere] * len(out_shape),
        scratch_shapes=[
            pltpu.VMEM((n_blocks, n_data, depth, out_part), BF16),
            pltpu.VMEM(q.shape, BF16),
            pltpu.VMEM(kv.shape, BF16),
            pltpu.VMEM((2, n_blocks, 2, n_mid, crow, c), BF16),
            pltpu.VMEM(tile, BF16),
            pltpu.VMEM(tile, BF16),
            pltpu.VMEM(tile, BF16),
            pltpu.VMEM((4, crow, out_part), BF16),
            pltpu.VMEM((n_model // 2, qrows, key_rows), F32),
            pltpu.VMEM((qrows, slab_len), F32),
            pltpu.VMEM((qrows, slab_len), F32),
            pltpu.VMEM((qrows, head_dim), F32),
            dma((SIDE_MATE + 7,)), dma((SIDE_MATE + 7,)), dma((13,)), dma((3, 2 * n_group)), dma((3, 2 * n_group)),
            dma((tiles,)), dma((tiles,)), dma((tiles,)), dma((tiles,)), dma((tiles,)), dma((tiles,)), dma((2,)), dma((2, chunks)),
        ],
        compiler_params=pltpu.CompilerParams(collective_id=2 * layer + 1, has_side_effects=True, vmem_limit_bytes=VMEM_LIMIT),
        cost_estimate=pl.CostEstimate(flops=4 * rows * n_blocks * depth * d_model, bytes_accessed=16 * rows * d_model, transcendentals=0),
        name=f"attend_and_sum_{layer}",
    )(*args)


def solution(mesh):
    batch_axes = ("rep", "data")
    n_data, n_model = mesh.shape["data"], mesh.shape["model"]
    n_chip = n_model // 2

    def near(x):
        return x + 1 - 2 * (x % 2)

    def across(x):
        return n_chip - 1 - x

    def on_chip(other):
        return lambda m: 2 * other(m // 2) + m % 2

    def local_step(x_loc, lens_loc, gamma_loc, w_in_loc, w_kv_loc, w_out_loc):
        n_batch, slab_len, d_model = x_loc.shape
        n_layers, part = gamma_loc.shape
        partners = [on_chip(near if layer % 2 == 0 else across) for layer in range(n_layers)]
        neighbours = [on_chip(across if layer % 2 == 0 else near) for layer in range(n_layers)]

        gain_rows = jnp.zeros((8, part), F32).at[:n_layers].set(gamma_loc.astype(F32))
        own = x_loc.reshape(n_batch * slab_len, d_model)
        for layer in range(n_layers):
            last = layer + 1 == n_layers
            following = min(layer + 1, n_layers - 1)
            if layer == 0:
                extra = (gain_rows,)
                q, m, kv, _, gains, out_first, out_column, in_first = project(
                    layer, n_data, n_model, partners[layer], neighbours[layer], neighbours[following],
                    own, w_kv_loc, w_in_loc, w_out_loc, extra,
                )
            else:
                extra = (other, gains, in_first, in_column)
                q, m, kv, _, out_first, out_column = project(
                    layer, n_data, n_model, partners[layer], neighbours[layer], neighbours[following],
                    own, w_kv_loc, w_in_loc, w_out_loc, extra,
                )
            outs = attend_and_sum(
                layer, last, n_data, n_model, partners[layer], neighbours[layer], partners[following],
                lens_loc, q, m, kv, own, w_in_loc, w_out_loc, w_kv_loc, out_first, out_column,
            )
            own = outs[0]
            if not last:
                other, in_column = outs[2:]
        return own.reshape(n_batch, slab_len, d_model)

    in_specs = (
        P(batch_axes, "model", None),
        P(batch_axes),
        P(None, "data"),
        P(None, "data", "model"),
        P(None, "data", None),
        P(None, "model", "data"),
    )
    return jax.shard_map(local_step, mesh=mesh, in_specs=in_specs, out_specs=P(batch_axes, "model", None), check_vma=False)
```

```python
import functools

import jax
import jax.numpy as jnp
from jax import lax
from jax.experimental import pallas as pl
from jax.experimental.pallas import tpu as pltpu
from jax.sharding import PartitionSpec as P

EPSILON = 1e-6
VMEM_LIMIT = 66_000_000
MESH = pl.DeviceIdType.MESH
BF16, F32 = jnp.bfloat16, jnp.float32

UP, DOWN, FORWARD, FORWARD_B, FIRST, SIDE_UP, SIDE_DOWN, FAR, MATE, SIDE_MATE = range(10)


def rms_norm(x_in, gain):
    x_f32 = x_in.astype(F32)
    inv_rms = lax.rsqrt(jnp.mean(x_f32 * x_f32, axis=-1, keepdims=True) + EPSILON)
    return (x_f32 * inv_rms * gain.astype(F32)).astype(BF16)


class Place:
    def __init__(self, n_data, n_model, partner, neighbour):
        self.n_data, self.n_model = n_data, n_model
        self.y = lax.axis_index("data")
        self.me = lax.axis_index("model")
        self.up = lax.rem(self.y + 1, n_data)
        self.down = lax.rem(self.y + n_data - 1, n_data)
        self.far = lax.rem(self.y + 2, n_data)
        self.slots = (self.y, self.down, self.up, self.far)
        self.mate = self.me + 1 - 2 * lax.rem(self.me, 2)
        self.partner, self.neighbour = partner(self.me), neighbour(self.me)
        n_other = n_model // 2 - 1
        self.ahead = [lax.rem(self.me + 2 * k, n_model) for k in range(1, n_other + 1)]
        self.behind = [lax.rem(self.me + n_model - 2 * k, n_model) for k in range(1, n_other + 1)]

    def meet(self):
        barrier = pltpu.get_barrier_semaphore()
        targets = [{"data": self.up}, {"data": self.down}, {"data": self.far}, {"model": self.mate}]
        targets += [{"model": m} for m in self.ahead]
        for target in targets:
            pl.semaphore_signal(barrier, inc=1, device_id=target, device_id_type=MESH)
        pl.semaphore_wait(barrier, len(targets))


def remote(src, dst, send, recv, target):
    return pltpu.make_async_remote_copy(
        src_ref=src, dst_ref=dst, send_sem=send, recv_sem=recv, device_id=target, device_id_type=MESH
    )


class GatherIn:
    def __init__(self, place, buf, pool, own, send, recv, local, first=None, column=None):
        self.place, self.buf, self.pool, self.own, self.first, self.column = place, buf, pool, own, first, column
        self.send, self.recv, self.local = send, recv, local

    def at(self, block, g, slot):
        return self.buf.at[block, g, slot]

    def _copy(self, src, dst, kind, at, target):
        return remote(src, dst, self.send.at[kind, at], self.recv.at[kind, at], target)

    def up(self, g, half):
        dst = self.at(0, g, self.place.y).at[half]
        return self._copy(self.own(g, half), dst, UP, 2 * g + half, {"data": self.place.up})

    def down(self, g, half):
        dst = self.at(0, g, self.place.y).at[half]
        return self._copy(self.own(g, half), dst, DOWN, 2 * g + half, {"data": self.place.down})

    def neighbour_first(self, g, half):
        dst = self.at(2, g, self.place.y).at[half]
        return self._copy(self.own(g, half), dst, FIRST, 2 * g + half, {"model": self.place.neighbour})

    def forward(self, g, half):
        ref = self.at(0, g, (self.place.down, self.place.up)[half]).at[half]
        target = (self.place.up, self.place.down)[half]
        return self._copy(ref, ref, FORWARD, 2 * g + half, {"data": target})

    def _needed(self, ref, g):
        return ref.at[0] if isinstance(g, int) and g == 0 else ref

    def _side(self, g, kind, target):
        src = self.at(2, g, self.place.y) if self.first is None else self.first.at[g]
        dst = self.at(2, g, self.place.y)
        return self._copy(self._needed(src, g), self._needed(dst, g), kind, g, {"data": target})

    def side_up(self, g):
        return self._side(g, SIDE_UP, self.place.up)

    def side_down(self, g):
        return self._side(g, SIDE_DOWN, self.place.down)

    def far(self, g):
        slot = self.place.far
        src = self.at(0, g, slot) if self.column is None else self.column.at[g, slot]
        dst = self.at(2, g, slot)
        return self._copy(self._needed(src, g), self._needed(dst, g), FAR, g, {"model": self.place.neighbour})

    def mate(self, g):
        return self._copy(self.buf.at[0, g], self.pool.at[0, g], MATE, g, {"model": self.place.mate})

    def side_mate(self, g):
        src, dst = self.buf.at[2, g], self.pool.at[1, g]
        if isinstance(g, int) and g == 0:
            src, dst = src.at[:, 0], dst.at[:, 0]
        return self._copy(src, dst, SIDE_MATE, g, {"model": self.place.mate})

    def load_mate(self, g):
        return pltpu.make_async_copy(self.pool.at[0, g], self.buf.at[1, g], self.local.at[6, g])

    def load_side(self, g):
        src, dst = self.pool.at[1, g], self.buf.at[3, g]
        if isinstance(g, int) and g == 0:
            src, dst = src.at[:, 0], dst.at[:, 0]
        return pltpu.make_async_copy(src, dst, self.local.at[7, g])

    def take_mate(self, g):
        self.mate(g).wait_recv()
        self.load_mate(g).start()

    def take_side(self, g):
        self.side_mate(g).wait_recv()
        self.load_side(g).start()

    def load_own(self, g, half):
        dst = self.at(0, g, self.place.y).at[half]
        return pltpu.make_async_copy(self.own(g, half), dst, self.local.at[half, g])

    def load_column(self, g, which):
        slot = self.place.slots[which]
        return pltpu.make_async_copy(self.column.at[g, slot], self.at(0, g, slot), self.local.at[1 + which, g])

    def load_first(self, g):
        return pltpu.make_async_copy(self.first.at[g], self.at(2, g, self.place.y), self.local.at[5, g])

    def pass_side(self, g):
        if self.first is not None:
            self.load_first(g).wait()
        self.side_up(g).wait_recv()
        self.side_down(g).wait_recv()
        self.far(g).wait_recv()
        self.side_mate(g).start()

    def wait_sends(self, g):
        made = [self.side_up(g), self.side_down(g), self.far(g), self.mate(g), self.side_mate(g)]
        if self.column is None:
            made += [copy(g, half) for copy in (self.up, self.down, self.forward) for half in range(2)]
        if self.first is None:
            made += [self.neighbour_first(g, half) for half in range(2)]
        for copy in made:
            copy.wait_send()


class FetchIn:
    def __init__(self, place, own, send, recv, neighbour=None, first=None, column=None):
        self.place, self.own, self.send, self.recv = place, own, send, recv
        self.neighbour, self.first, self.column = neighbour, first, column

    def _ring(self, g, half, kind, target):
        at = 2 * g + half
        dst = self.column.at[g, self.place.y, half]
        return remote(self.own(g, half), dst, self.send.at[kind, at], self.recv.at[kind, at], {"data": target})

    def up(self, g, half):
        return self._ring(g, half, 0, self.place.up)

    def down(self, g, half):
        return self._ring(g, half, 1, self.place.down)

    def forward(self, g, half):
        at = 2 * g + half
        ref = self.column.at[g, (self.place.down, self.place.up)[half], half]
        target = (self.place.up, self.place.down)[half]
        return remote(ref, ref, self.send.at[2, at], self.recv.at[2, at], {"data": target})

    def ring_stage(self, g):
        for half in range(2):
            self.up(g, half).wait_recv()
            self.down(g, half).wait_recv()
        for half in range(2):
            self.forward(g, half).start()

    def send_slices(self, g):
        for half in range(2):
            self.up(g, half).start()
            self.down(g, half).start()

    def neighbour_first(self, g, half):
        at = 2 * g + half
        dst = self.first.at[g, half]
        return remote(self.own(g, half), dst, self.send.at[3, at], self.recv.at[3, at], {"model": self.neighbour})


class GatherOut:
    def __init__(self, place, buf, own, send, recv, local=None, first=None, column=None, pool=None, whole_column=True):
        self.place, self.buf, self.own, self.first, self.column = place, buf, own, first, column
        self.far_held = column is not None and whole_column
        self.send, self.recv, self.local, self.pool = send, recv, local, pool

    def _copy(self, src, dst, kind, target):
        return remote(src, dst, self.send.at[kind], self.recv.at[kind], target)

    def up(self):
        return self._copy(self.own, self.buf.at[0, self.place.y], UP, {"data": self.place.up})

    def down(self):
        return self._copy(self.own, self.buf.at[0, self.place.y], DOWN, {"data": self.place.down})

    def _half(self, ref, second):
        size = ref.shape[0] // 2
        return ref.at[pl.ds(second * size, size)]

    def _forward(self, kind, slot, second, target):
        src = self.buf if self.column is None else self.column
        dst = self._half(self.buf.at[0, slot], second)
        return self._copy(self._half(src.at[0, slot], second), dst, kind, {"data": target})

    def forward(self):
        return self._forward(FORWARD, self.place.down, 0, self.place.up)

    def forward_b(self):
        return self._forward(FORWARD_B, self.place.up, 1, self.place.down)

    def neighbour_first(self, dst):
        return self._copy(self.own, dst, FIRST, {"model": self.place.neighbour})

    def side_up(self):
        return self._copy(self.first, self.buf.at[2, self.place.y], SIDE_UP, {"data": self.place.up})

    def side_down(self):
        return self._copy(self.first, self.buf.at[2, self.place.y], SIDE_DOWN, {"data": self.place.down})

    def far(self):
        slot = self.place.far
        src = self.column.at[0, slot] if self.far_held else self.buf.at[0, slot]
        return self._copy(src, self.buf.at[2, slot], FAR, {"model": self.place.neighbour})

    def mate(self, which):
        slot = self.place.slots[which]
        if which == 0:
            src = self.own
        else:
            src = self.column.at[0, slot] if which < 3 or self.far_held else self.buf.at[0, slot]
        return self._copy(src, self.pool.at[0, slot], MATE + 2 * which, {"model": self.place.mate})

    def side_mate(self, which):
        slot = self.place.slots[which]
        src = self.first if which == 0 else self.buf.at[2, slot]
        return self._copy(src, self.pool.at[1, slot], SIDE_MATE + 2 * which, {"model": self.place.mate})

    def load_mate(self, which):
        slot = self.place.slots[which]
        return pltpu.make_async_copy(self.pool.at[0, slot], self.buf.at[1, slot], self.local.at[5 + which])

    def load_side(self, which):
        slot = self.place.slots[which]
        return pltpu.make_async_copy(self.pool.at[1, slot], self.buf.at[3, slot], self.local.at[9 + which])

    def take(self, which):
        self.mate(which).wait_recv()
        self.load_mate(which).start()
        self.side_mate(which).wait_recv()
        self.load_side(which).start()

    def load_own(self):
        return pltpu.make_async_copy(self.own, self.buf.at[0, self.place.y], self.local.at[0])

    def load_column(self, which):
        slot = self.place.slots[which]
        return pltpu.make_async_copy(self.column.at[0, slot], self.buf.at[0, slot], self.local.at[which])

    def load_first(self):
        return pltpu.make_async_copy(self.first, self.buf.at[2, self.place.y], self.local.at[4])


def in_halves(layer, w_kv_ref, w_ref, c, ff):
    def own(g, half):
        if isinstance(g, int) and g == 0:
            return w_kv_ref.at[layer] if half else w_ref.at[layer, :, pl.ds(0, c)]
        return w_ref.at[layer, :, pl.ds(pl.multiple_of(g * c + half * ff, c), c)]

    return own


def project(layer, n_data, n_model, partner, neighbour, next_neighbour, x_own, w_kv, w_in, w_out, extra):
    start_layer = layer == 0
    part, c = w_kv.shape[1:]
    d_model = part * n_data
    rows = x_own.size // d_model
    depth, out_part = w_out.shape[1:]
    ff = depth - c
    n_group = 1 + ff // c
    n_units = 8 * n_group
    row_parts = 4
    row_part = rows // row_parts
    n_other = n_model // 2 - 1
    gain_shape = (n_data, 8, part)
    n_tiles = 1 if start_layer else x_own.shape[0] * x_own.shape[1]

    def kernel(*refs):
        x_ref, w_kv_ref, w_ref, wo_ref = refs[:4]
        if start_layer:
            gain_ref = refs[4]
            q_ref, m_ref, kv_ref, pool_ref, gains_ref, out_first_ref, out_column_ref, in_first_ref = refs[5:13]
            first_ref = column_ref = None
            rest = refs[13:]
        else:
            par_ref, gain_ref, first_ref, column_ref = refs[4:8]
            q_ref, m_ref, kv_ref, pool_ref, out_first_ref, out_column_ref = refs[8:14]
            rest = refs[14:]
        wbuf, h_ref, gbuf, stage, kv_stage, send, recv, w_local, next_send, next_recv, late_send, late_recv = rest[:12]
        x_send, x_recv, g_send, g_recv, kv_send, kv_recv, local, out_sem, tile_sem = rest[12:]

        place = Place(n_data, n_model, partner, neighbour)
        place.meet()
        in_own = in_halves(layer, w_kv_ref, w_ref, c, ff)
        w = GatherIn(place, wbuf, pool_ref, in_own, send, recv, w_local, first_ref, column_ref)
        out_next = GatherOut(place, out_column_ref, wo_ref.at[layer], next_send, next_recv)
        if start_layer:
            in_own_next = in_halves(layer + 1, w_kv_ref, w_ref, c, ff)
            in_next = FetchIn(place, in_own_next, late_send, late_recv, next_neighbour(place.me), in_first_ref)

        def c_x(part_no):
            piece = pl.ds(part_no * row_part, row_part)
            return remote(
                x_ref.at[piece], h_ref.at[1, piece], x_send.at[part_no], x_recv.at[part_no], {"model": place.partner}
            )

        def c_gain(which):
            target = {"data": (place.up, place.down, place.far)[which]}
            return remote(gain_ref, gbuf.at[place.y], g_send.at[which], g_recv.at[which], target)

        def c_kv(which):
            ref = kv_ref.at[place.me]
            return remote(ref, ref, kv_send.at[which], kv_recv.at[which], {"model": place.ahead[which]})

        def c_kv_mate(which):
            ref = kv_ref.at[place.me if which == 0 else place.behind[which - 1]]
            at = n_other + which
            return remote(ref, ref, kv_send.at[at], kv_recv.at[at], {"model": place.mate})

        save_kv = pltpu.make_async_copy(kv_stage, kv_ref.at[place.me], local.at[0])
        if start_layer:
            load_x = pltpu.make_async_copy(x_ref, h_ref.at[0], local.at[0])

        def load_tile(side, k):
            chunk, slot = k // n_data, lax.rem(k, n_data)
            src = (x_ref, par_ref)[side].at[chunk, slot]
            height, across = src.shape
            down_to, along = pl.multiple_of(chunk * height, height), pl.multiple_of(slot * across, across)
            return pltpu.make_async_copy(src, h_ref.at[side, pl.ds(down_to, height), pl.ds(along, across)], tile_sem.at[side, k])

        if start_layer:
            load_gain = pltpu.make_async_copy(gain_ref, gbuf.at[place.y], local.at[1])
            for which in range(3):
                c_gain(which).start()
        else:
            load_gain = pltpu.make_async_copy(gain_ref, gbuf, local.at[1])
        def send_slices(g):
            for half in range(2):
                w.up(g, half).start()
                w.down(g, half).start()

        load_gain.start()
        if start_layer:
            load_x.start()
        else:
            for side in range(2):

                @pl.loop(0, n_tiles)
                def _(k):
                    load_tile(side, k).start()

        if start_layer:
            send_slices(0)
            for g in range(n_group):
                for half in range(2):
                    w.neighbour_first(g, half).start()
                    w.load_own(g, half).start()
            for part_no in range(row_parts // 2):
                c_x(part_no).start()
        else:
            for g in range(n_group):
                for half in range(2):
                    w.load_own(g, half).start()
                for which in range(1, 4):
                    w.load_column(g, which).start()
                w.side_up(g).start()
                w.side_down(g).start()
                if g < 2:
                    w.far(g).start()
            for g in range(n_group):
                w.load_first(g).start()

        def ring_stage(g):
            for half in range(2):
                w.up(g, half).wait_recv()
                w.down(g, half).wait_recv()
            for half in range(2):
                w.forward(g, half).start()

        def column_stage(g):
            for half in range(2):
                w.load_own(g, half).wait()
            for which in range(1, 4):
                w.load_column(g, which).wait()
            w.mate(g).start()

        if start_layer:
            for which in range(3):
                c_gain(which).wait_recv()
        load_gain.wait()
        gain = jnp.concatenate([gbuf[k, layer:layer + 1, :] for k in range(n_data)], axis=1)
        if start_layer:
            save_gain = pltpu.make_async_copy(gbuf, gains_ref, local.at[1])
            save_gain.start()
        if start_layer:
            load_x.wait()
        else:

            @pl.loop(0, n_tiles)
            def _(k):
                load_tile(0, k).wait()

        def norm_rows(side, part_no):
            piece = pl.ds(part_no * row_part, row_part)
            h_ref[side, piece] = rms_norm(h_ref[side, piece], gain)

        @pl.loop(0, row_parts)
        def _(part_no):
            norm_rows(0, part_no)

        if start_layer:
            send_slices(1)
            ring_stage(0)
        else:
            column_stage(0)

        halfway, quarter = n_units // 2, n_units // 4

        def out_copy(slot, blk, side, g):
            def to_q():
                return pltpu.make_async_copy(stage.at[slot], q_ref.at[blk, side], out_sem.at[slot])

            def to_m():
                return pltpu.make_async_copy(stage.at[slot], m_ref.at[blk, side, g - 1], out_sem.at[slot])

            return to_q, to_m

        @pl.loop(0, n_units)
        def _(step):
            late = step - halfway
            if start_layer:
                opening, second = step < quarter, (step >= quarter) & (step < halfway)
                ahead = (step == 0) | ((lax.rem(step, 2) == 1) & (step < quarter - 1))
                open_g = jnp.where(ahead, (step + 1) // 2, jnp.where(step == quarter - 1, n_group - 1, step // 2 - 1))
                g = jnp.where(opening, open_g, jnp.where(second, (step - quarter) // 2, late // 4))
                open_blk = jnp.where(ahead, 0, 1)
                blk = jnp.where(opening, open_blk, jnp.where(second, lax.rem(step, 2), 2 + lax.rem(late, 4) // 2))
                side = jnp.where(opening, 0, jnp.where(second, 1, lax.rem(late, 2)))

                @pl.when(opening & (blk == 0))
                def _():
                    for half in range(2):
                        w.forward(g, half).wait_recv()

                    @pl.when(g + 2 < n_group)
                    def _():
                        send_slices(g + 2)

                    @pl.when(g + 1 < n_group)
                    def _():
                        ring_stage(g + 1)

                    @pl.when(g + 2 == n_group)
                    def _():
                        for k in range(n_group):
                            for half in range(2):
                                w.neighbour_first(k, half).wait_recv()
                            w.side_up(k).start()
                            w.side_down(k).start()

                    @pl.when(g == 0)
                    def _():
                        w.far(0).start()

                    @pl.when(g > 0)
                    def _():
                        w.far(g).start()

                    @pl.when(g == 1)
                    def _():
                        for part_no in range(row_parts // 2, row_parts):
                            c_x(part_no).start()

                    for half in range(2):
                        w.load_own(g, half).wait()
                    w.mate(g).start()

                    @pl.when(g > 0)
                    def _():
                        w.take_mate(g - 1)

                @pl.when(step == quarter - 2)
                def _():
                    w.take_mate(n_group - 1)

                @pl.when(opening & (blk == 1))
                def _():
                    w.load_mate(g).wait()

                @pl.when(step == quarter)
                def _():
                    @pl.loop(0, row_parts)
                    def _(part_no):
                        c_x(part_no).wait_recv()
                        norm_rows(1, part_no)

                    out_next.neighbour_first(out_first_ref).start()
                    out_next.up().start()
                    out_next.down().start()
                    for k in range(n_group):
                        for half in range(2):
                            in_next.neighbour_first(k, half).start()
            else:
                g = jnp.where(late < 0, step, late) // 4
                blk = jnp.where(late < 0, 0, 2) + lax.rem(step, 4) // 2
                side = lax.rem(step, 2)

                @pl.when((late < 0) & (lax.rem(step, 4) == 0) & (g + 1 < n_group))
                def _():
                    column_stage(g + 1)

                @pl.when(step == 1)
                def _():
                    @pl.loop(0, n_tiles)
                    def _(k):
                        load_tile(1, k).wait()

                    @pl.loop(0, row_parts)
                    def _(part_no):
                        norm_rows(1, part_no)

                @pl.when((late < 0) & (lax.rem(step, 4) == 1))
                def _():
                    w.take_mate(g)

                @pl.when((late < 0) & (lax.rem(step, 4) == 2))
                def _():
                    w.load_mate(g).wait()

                @pl.when(step == n_units - 6)
                def _():
                    out_next.up().wait_recv()
                    out_next.down().wait_recv()
                    out_next.forward().start()
                    out_next.forward_b().start()

            @pl.when(step == halfway - 2)
            def _():
                w.pass_side(0)

            @pl.when(step == halfway + 1)
            def _():
                w.take_side(0)

            @pl.when((late > 1) & (lax.rem(late, 4) == 1))
            def _():
                w.take_side(g)

            @pl.when((late >= 0) & (lax.rem(late, 4) == 2))
            def _():
                @pl.when(g + 1 < n_group)
                def _():
                    w.pass_side(g + 1)

                @pl.when(g == 0)
                def _():
                    w.load_side(0).wait()

                @pl.when(g > 0)
                def _():
                    w.load_side(g).wait()

            slot = lax.rem(step, 2)
            to_q, to_m = out_copy(slot, blk, side, g)

            @pl.when(step >= 2)
            def _():
                to_q().wait()

            def columns(half):
                return wbuf[blk, g, :, half].reshape(d_model, c)

            @pl.when(g == 0)
            def _():
                q = jnp.dot(h_ref[side], columns(0), preferred_element_type=F32)
                stage[slot] = q.astype(BF16)
                to_q().start()

            @pl.when(g > 0)
            def _():
                h_val = h_ref[side]
                gate = jnp.dot(h_val, columns(0), preferred_element_type=F32).astype(BF16).astype(F32)
                raised = jnp.dot(h_val, columns(1), preferred_element_type=F32).astype(BF16).astype(F32)
                stage[slot] = (gate * jax.nn.sigmoid(gate) * raised).astype(BF16)
                to_m().start()

            @pl.when(step == 0)
            def _():
                kv_stage[...] = jnp.dot(h_ref[0], columns(1), preferred_element_type=F32).astype(BF16)
                save_kv.start()

            @pl.when(step == 1)
            def _():
                save_kv.wait()
                for which in range(n_other):
                    c_kv(which).start()
                c_kv_mate(0).start()
                if not start_layer:
                    for k in range(2, n_group):
                        w.far(k).start()

            @pl.when(step == n_units - 4)
            def _():
                for which in range(n_other):
                    c_kv(which).wait_recv()
                    c_kv_mate(1 + which).start()

            if not start_layer:

                @pl.when(step == 8)
                def _():
                    out_next.up().start()
                    out_next.down().start()
                    out_next.neighbour_first(out_first_ref).start()
        for which in range(n_other + 1):
            c_kv_mate(which).wait()
        for which in range(n_other):
            c_kv(which).wait_send()
        if start_layer:
            save_gain.wait()
            for which in range(3):
                c_gain(which).wait_send()
            for part_no in range(row_parts):
                c_x(part_no).wait_send()
            for g in range(n_group):
                for half in range(2):
                    in_next.neighbour_first(g, half).wait()
            for copy in (out_next.up(), out_next.down()):
                copy.wait()
        else:
            for copy in (out_next.forward(), out_next.forward_b()):
                copy.wait()
            for copy in (out_next.up(), out_next.down()):
                copy.wait_send()
        out_next.neighbour_first(out_first_ref).wait()
        for slot in range(2):
            pltpu.make_async_copy(stage.at[slot], q_ref.at[0, 0], out_sem.at[slot]).wait()

        for g in range(n_group):
            w.wait_sends(g)

    anywhere = pl.BlockSpec(memory_space=pl.ANY)
    out_shape = [
        jax.ShapeDtypeStruct((4, 2, rows, c), BF16),
        jax.ShapeDtypeStruct((4, 2, n_group - 1, rows, c), BF16),
        jax.ShapeDtypeStruct((n_model, rows, c), BF16),
        jax.ShapeDtypeStruct((2, n_group, n_data, 2, part, c), BF16),
    ]
    if start_layer:
        out_shape += [
            jax.ShapeDtypeStruct(gain_shape, F32),
            jax.ShapeDtypeStruct((depth, out_part), BF16),
            jax.ShapeDtypeStruct((1, n_data, depth, out_part), BF16),
            jax.ShapeDtypeStruct((n_group, 2, part, c), BF16),
        ]
    else:
        out_shape += [
            jax.ShapeDtypeStruct((depth, out_part), BF16),
            jax.ShapeDtypeStruct((1, n_data, depth, out_part), BF16),
        ]
    dma = pltpu.SemaphoreType.DMA
    args = (x_own, w_kv, w_in, w_out) + tuple(extra)
    return pl.pallas_call(
        kernel,
        out_shape=out_shape,
        in_specs=[anywhere] * len(args),
        out_specs=[anywhere] * len(out_shape),
        scratch_shapes=[
            pltpu.VMEM((4, n_group, n_data, 2, part, c), BF16),
            pltpu.VMEM((2, rows, d_model), BF16),
            pltpu.VMEM(gain_shape, F32),
            pltpu.VMEM((2, rows, c), BF16),
            pltpu.VMEM((rows, c), BF16),
            dma((SIDE_MATE + 1, 2 * n_group)), dma((SIDE_MATE + 1, 2 * n_group)), dma((8, n_group)),
            dma((FIRST + 1,)), dma((FIRST + 1,)), dma((4, 2 * n_group)), dma((4, 2 * n_group)),
            dma((row_parts,)), dma((row_parts,)), dma((3,)), dma((3,)),
            dma((n_model - 1,)), dma((n_model - 1,)), dma((3,)), dma((2,)), dma((2, n_tiles)),
        ],
        compiler_params=pltpu.CompilerParams(collective_id=2 * layer, has_side_effects=True, vmem_limit_bytes=VMEM_LIMIT),
        cost_estimate=pl.CostEstimate(flops=4 * rows * d_model * 4 * (c + 2 * ff), bytes_accessed=16 * rows * d_model, transcendentals=0),
        name=f"project_{layer}",
    )(*args)


def pick(step, values):
    found = jnp.int32(values[0])
    for at in range(1, len(values)):
        if values[at] != values[at - 1]:
            found = jnp.where(step >= at, jnp.int32(values[at]), found)
    return found


def attend_and_sum(layer, last, n_data, n_model, partner, neighbour, next_partner, lens, q, m, kv, x_own, w_in, w_out, w_kv, first, column):
    n_blocks, _, rows, c = q.shape
    n_mid = m.shape[2]
    ff = n_mid * c
    d_model = w_out.shape[2] * n_data
    tiled = x_own.ndim == 4
    depth, out_part = w_out.shape[1:]
    head_dim = c // 2
    n_batch = lens.shape[0]
    slab_len = rows // n_batch
    chunks = 4
    n_seq = n_batch // chunks
    crow = rows // chunks
    tiles = chunks * n_data
    heads = n_blocks * 2
    qrows = heads * slab_len
    key_rows = 2 * slab_len
    scale = head_dim ** -0.5 * 1.4426950408889634
    part = w_kv.shape[1]
    n_group = 1 + ff // c
    if layer == 0:
        order = [(0, 0), (1, 0), (2, 0), (0, 1), (1, 1), (2, 1), (0, 2), (1, 2), (2, 2)]
        order += [(3, 0), (3, 1), (3, 2), (0, 3), (1, 3), (2, 3), (3, 3)]
        opens = (0, 1, 2, 9)
        side_step, far_step = 2, 11
    else:
        order = [(0, 0), (1, 0), (0, 1), (1, 1), (0, 2), (1, 2), (2, 0), (2, 1), (2, 2), (0, 3), (1, 3), (2, 3)]
        order += [(3, which) for which in range(4)]
        opens = (0, 1, 6, 12)
        side_step, far_step = 1, 8
    flying = 3
    settles = {2: (0,), 3: (1,)}
    for at in range(5, tiles):
        settles[at] = (at - flying,)
    held = sum(len(some) for some in settles.values())
    whole_column = layer > 0

    def kernel(*refs):
        lens_ref, q_ref, m_ref, kv_ref, x_ref, wo_ref, first_ref = refs[:7]
        at = 7
        column_ref = refs[at]
        at += 1
        if not last:
            w_kv_ref, wi_ref = refs[at:at + 2]
            at += 2
        y_ref, pool_ref = refs[at:at + 2]
        at += 2
        if not last:
            par_ref, in_column_ref = refs[at:at + 2]
            at += 2
        (wbuf, obuf, kvb, mbuf, xb, zb, zr, z_stage, s_ref, mx_ref, sum_ref, acc_ref,
         send, recv, w_local, in_send, in_recv, z_send, z_recv, y_send, y_recv, y_save, x_sem, m_sem, local) = refs[at:]

        place = Place(n_data, n_model, partner, neighbour)
        place.meet()
        w = GatherOut(place, wbuf, wo_ref.at[layer], send, recv, w_local, first_ref, column_ref, pool_ref, whole_column)

        def tile_of(k):
            which = pick(k, [one for _, one in order])
            slot = jnp.where(which == 0, place.y, jnp.where(which == 1, place.down, jnp.where(which == 2, place.up, place.far)))
            return pick(k, [one for one, _ in order]), which, slot

        def whole(ref, chunk, slot):
            return ref.at[pl.ds(pl.multiple_of(chunk * crow, crow), crow), pl.ds(pl.multiple_of(slot * out_part, out_part), out_part)]

        def rows_of(chunk):
            return pl.ds(pl.multiple_of(chunk * crow, crow), crow)

        def load_q(chunk):
            return pltpu.make_async_copy(q_ref.at[:, :, rows_of(chunk)], obuf.at[:, :, rows_of(chunk)], local.at[0, chunk])

        def load_kv(chunk):
            return pltpu.make_async_copy(kv_ref.at[:, rows_of(chunk)], kvb.at[:, rows_of(chunk)], local.at[1, chunk])

        def load_m(k):
            chunk, _, _ = tile_of(k)
            slot = lax.rem(k, 2)
            return pltpu.make_async_copy(
                m_ref.at[:, :, :, pl.ds(pl.multiple_of(chunk * crow, crow), crow)], mbuf.at[slot], m_sem.at[slot]
            )

        def load_x(k):
            chunk, _, slot = tile_of(k)
            src = x_ref.at[chunk, slot] if tiled else whole(x_ref, chunk, slot)
            return pltpu.make_async_copy(src, xb.at[chunk, slot], x_sem.at[k])

        def c_z(k):
            chunk, _, slot = tile_of(k)
            return remote(z_stage.at[lax.rem(k, 4)], zr.at[chunk, slot], z_send.at[k], z_recv.at[k], {"model": place.partner})

        def c_y(k):
            chunk, _, slot = tile_of(k)
            target = {"model": next_partner(place.me)}
            return remote(xb.at[chunk, slot], par_ref.at[chunk, slot], y_send.at[k], y_recv.at[k], target)

        def save_y(k):
            chunk, _, slot = tile_of(k)
            dst = whole(y_ref, chunk, slot) if last else y_ref.at[chunk, slot]
            return pltpu.make_async_copy(xb.at[chunk, slot], dst, y_save.at[k])

        for chunk in range(chunks):
            load_q(chunk).start()
            load_kv(chunk).start()
        load_m(0).start()
        w.load_own().start()
        w.load_first().start()
        w.mate(0).start()
        w.side_mate(0).start()
        for which in range(1, 4 if whole_column else 3):
            w.load_column(which).start()
            w.mate(which).start()
        if whole_column:
            w.far().start()
        else:
            w.forward().start()
            w.forward_b().start()
        w.side_up().start()
        w.side_down().start()
        if not last:
            in_own = in_halves(layer + 1, w_kv_ref, wi_ref, c, ff)
            in_next = FetchIn(place, in_own, in_send, in_recv, column=in_column_ref)

        @pl.loop(0, tiles)
        def _(k):
            load_x(k).start()

        def attend_one(batch, side):
            slab = jnp.where(side == 0, place.me, place.partner)
            length = lens_ref[batch]
            n_key = slab // 2 + 1
            at_row = pl.ds(pl.multiple_of(batch * slab_len, slab_len), slab_len)
            parts = []
            for blk in range(n_blocks):
                for one in range(2):
                    parts.append(obuf[blk, side, at_row, one * head_dim:(one + 1) * head_dim])
            q_val = jnp.concatenate(parts, axis=0)
            row_pos = slab * slab_len + lax.rem(lax.broadcasted_iota(jnp.int32, (qrows, key_rows), 0), slab_len)
            key_pos = lax.broadcasted_iota(jnp.int32, (qrows, key_rows), 1)
            room = jnp.minimum(row_pos + 1, length) - key_pos
            mx_ref[...] = jnp.full_like(mx_ref, -1e30)

            def score(kb, carry):
                k = kvb[pl.ds(2 * kb, 2), at_row, :head_dim].reshape(key_rows, head_dim)
                s = lax.dot_general(q_val, k, (((1,), (1,)), ((), ())), preferred_element_type=F32) * scale
                s = jnp.where(room > kb * key_rows, s, -1e30)
                s_ref[kb] = s
                mx_ref[...] = jnp.maximum(mx_ref[...], jnp.maximum(s[:, :slab_len], s[:, slab_len:]))
                return carry

            lax.fori_loop(0, n_key, score, 0)
            top = jnp.max(mx_ref[...], axis=-1, keepdims=True)
            mx_ref[...] = jnp.broadcast_to(top, mx_ref.shape)
            sum_ref[...] = jnp.zeros_like(sum_ref)
            acc_ref[...] = jnp.zeros_like(acc_ref)

            def weigh(kb, carry):
                v = kvb[pl.ds(2 * kb, 2), at_row, head_dim:].reshape(key_rows, head_dim)
                top_b = mx_ref[...]
                e_lo = jnp.exp2(s_ref[kb, :, :slab_len] - top_b)
                e_hi = jnp.exp2(s_ref[kb, :, slab_len:] - top_b)
                sum_ref[...] += e_lo + e_hi
                e = jnp.concatenate([e_lo, e_hi], axis=1).astype(BF16)
                acc_ref[...] += jnp.dot(e, v, preferred_element_type=F32)
                return carry

            lax.fori_loop(0, n_key, weigh, 0)
            out = (acc_ref[...] / jnp.sum(sum_ref[...], axis=-1, keepdims=True)).astype(BF16)
            for blk in range(n_blocks):
                for one in range(2):
                    first_row = (blk * 2 + one) * slab_len
                    obuf[blk, side, at_row, one * head_dim:(one + 1) * head_dim] = out[first_row:first_row + slab_len]

        def settle(k):
            chunk, _, slot = tile_of(k)
            load_x(k).wait()
            c_z(k).wait_recv()
            z = zb[chunk, slot].astype(F32) + zr[chunk, slot].astype(F32)
            xb[chunk, slot] = (xb[chunk, slot].astype(F32) + z).astype(BF16)
            save_y(k).start()
            if not last:
                c_y(k).start()

        @pl.loop(0, tiles)
        def _(step):
            chunk, which, slot = tile_of(step)

            @pl.when(step + 1 < tiles)
            def _():
                load_m(step + 1).start()

            opening = functools.reduce(lambda one, other: one | other, [step == at for at in opens])

            @pl.when(opening)
            def _():
                load_q(chunk).wait()
                load_kv(chunk).wait()

                @pl.loop(0, 2 * n_seq)
                def _(unit):
                    attend_one(chunk * n_seq + unit // 2, lax.rem(unit, 2))

            @pl.when(step == 0)
            def _():
                w.load_own().wait()
                w.load_first().wait()
                w.take(0)
                w.load_mate(0).wait()
                w.load_side(0).wait()

            @pl.when(step == side_step)
            def _():
                w.side_up().wait_recv()
                w.side_mate(1).start()
                w.side_down().wait_recv()
                w.side_mate(2).start()

            @pl.when(step == side_step + 1)
            def _():
                for one in (1, 2):
                    w.take(one)
                for one in (1, 2):
                    w.load_column(one).wait()
                    w.load_mate(one).wait()
                    w.load_side(one).wait()

            if not whole_column:

                @pl.when(step == side_step - 1)
                def _():
                    w.forward().wait_recv()
                    w.forward_b().wait_recv()
                    w.far().start()
                    w.mate(3).start()

            @pl.when(step == far_step)
            def _():
                w.far().wait_recv()
                w.side_mate(3).start()

            @pl.when(step == far_step + 1)
            def _():
                w.take(3)
                if whole_column:
                    w.load_column(3).wait()
                w.load_mate(3).wait()
                w.load_side(3).wait()

            if not last:
                for g, at in enumerate((3, 3, 4, 5, 6)[:n_group]):

                    @pl.when(step == at)
                    def _(g=g):
                        in_next.send_slices(g)

                for g, at in enumerate((9, 10, 12, 15)[:n_group]):

                    @pl.when(step == at)
                    def _(g=g):
                        in_next.ring_stage(g)

            @pl.when(step >= flying)
            def _():
                c_z(step - flying).wait_send()

            load_m(step).wait()
            here = lax.rem(step, 2)
            rows_c = pl.ds(pl.multiple_of(chunk * crow, crow), crow)
            total = None
            for blk in range(n_blocks):
                mid = jnp.concatenate([mbuf[here, blk, :, k].reshape(2 * crow, c) for k in range(n_mid)], axis=1)
                attn = obuf[blk, :, rows_c, :].reshape(2 * crow, c)
                one = jnp.dot(mid, wbuf[blk, slot, c:, :], preferred_element_type=F32)
                one = one + jnp.dot(attn, wbuf[blk, slot, :c, :], preferred_element_type=F32)
                total = one if total is None else total + one
            z = total.astype(BF16)
            zb[chunk, slot] = z[:crow]
            z_stage[lax.rem(step, 4)] = z[crow:]
            c_z(step).start()

            for at, some in settles.items():

                @pl.when(step == at)
                def _(some=some):
                    for k in some:
                        settle(k)

        stages = list(range(4, n_group)) if not last else []
        for k in range(held, tiles):
            if stages and k - held >= 2:
                in_next.ring_stage(stages.pop(0))
            settle(k)
        for g in stages:
            in_next.ring_stage(g)

        @pl.loop(0, tiles)
        def _(k):
            save_y(k).wait()
            if not last:
                c_y(k).wait()

        @pl.loop(tiles - flying, tiles)
        def _(k):
            c_z(k).wait_send()

        made = [w.side_up(), w.side_down(), w.far()]
        made += [w.mate(which) for which in range(4)] + [w.side_mate(which) for which in range(4)]
        if not whole_column:
            made += [w.forward(), w.forward_b()]
        for copy in made:
            copy.wait_send()
        if not last:

            @pl.loop(0, n_group)
            def _(g):
                for half in range(2):
                    in_next.forward(g, half).wait()
                    in_next.up(g, half).wait_send()
                    in_next.down(g, half).wait_send()

    anywhere = pl.BlockSpec(memory_space=pl.ANY)
    args = [lens, q, m, kv, x_own, w_out, first, column]
    if not last:
        args += [w_kv, w_in]
    tile = (chunks, n_data, crow, out_part)
    out_shape = [
        jax.ShapeDtypeStruct((rows, d_model) if last else tile, BF16),
        jax.ShapeDtypeStruct((2, n_data, depth, out_part), BF16),
    ]
    if not last:
        out_shape += [
            jax.ShapeDtypeStruct(tile, BF16),
            jax.ShapeDtypeStruct((n_group, n_data, 2, part, c), BF16),
        ]
    dma = pltpu.SemaphoreType.DMA
    return pl.pallas_call(
        kernel,
        out_shape=out_shape,
        in_specs=[pl.BlockSpec(memory_space=pltpu.SMEM)] + [anywhere] * (len(args) - 1),
        out_specs=[anywhere] * len(out_shape),
        scratch_shapes=[
            pltpu.VMEM((n_blocks, n_data, depth, out_part), BF16),
            pltpu.VMEM(q.shape, BF16),
            pltpu.VMEM(kv.shape, BF16),
            pltpu.VMEM((2, n_blocks, 2, n_mid, crow, c), BF16),
            pltpu.VMEM(tile, BF16),
            pltpu.VMEM(tile, BF16),
            pltpu.VMEM(tile, BF16),
            pltpu.VMEM((4, crow, out_part), BF16),
            pltpu.VMEM((n_model // 2, qrows, key_rows), F32),
            pltpu.VMEM((qrows, slab_len), F32),
            pltpu.VMEM((qrows, slab_len), F32),
            pltpu.VMEM((qrows, head_dim), F32),
            dma((SIDE_MATE + 7,)), dma((SIDE_MATE + 7,)), dma((13,)), dma((3, 2 * n_group)), dma((3, 2 * n_group)),
            dma((tiles,)), dma((tiles,)), dma((tiles,)), dma((tiles,)), dma((tiles,)), dma((tiles,)), dma((2,)), dma((2, chunks)),
        ],
        compiler_params=pltpu.CompilerParams(collective_id=2 * layer + 1, has_side_effects=True, vmem_limit_bytes=VMEM_LIMIT),
        cost_estimate=pl.CostEstimate(flops=4 * rows * n_blocks * depth * d_model, bytes_accessed=16 * rows * d_model, transcendentals=0),
        name=f"attend_and_sum_{layer}",
    )(*args)


def solution(mesh):
    batch_axes = ("rep", "data")
    n_data, n_model = mesh.shape["data"], mesh.shape["model"]
    n_chip = n_model // 2

    def near(x):
        return x + 1 - 2 * (x % 2)

    def across(x):
        return n_chip - 1 - x

    def on_chip(other):
        return lambda m: 2 * other(m // 2) + m % 2

    def local_step(x_loc, lens_loc, gamma_loc, w_in_loc, w_kv_loc, w_out_loc):
        n_batch, slab_len, d_model = x_loc.shape
        n_layers, part = gamma_loc.shape
        partners = [on_chip(near if layer % 2 == 0 else across) for layer in range(n_layers)]
        neighbours = [on_chip(across if layer % 2 == 0 else near) for layer in range(n_layers)]

        gain_rows = jnp.zeros((8, part), F32).at[:n_layers].set(gamma_loc.astype(F32))
        own = x_loc.reshape(n_batch * slab_len, d_model)
        for layer in range(n_layers):
            last = layer + 1 == n_layers
            following = min(layer + 1, n_layers - 1)
            if layer == 0:
                extra = (gain_rows,)
                q, m, kv, _, gains, out_first, out_column, in_first = project(
                    layer, n_data, n_model, partners[layer], neighbours[layer], neighbours[following],
                    own, w_kv_loc, w_in_loc, w_out_loc, extra,
                )
            else:
                extra = (other, gains, in_first, in_column)
                q, m, kv, _, out_first, out_column = project(
                    layer, n_data, n_model, partners[layer], neighbours[layer], neighbours[following],
                    own, w_kv_loc, w_in_loc, w_out_loc, extra,
                )
            outs = attend_and_sum(
                layer, last, n_data, n_model, partners[layer], neighbours[layer], partners[following],
                lens_loc, q, m, kv, own, w_in_loc, w_out_loc, w_kv_loc, out_first, out_column,
            )
            own = outs[0]
            if not last:
                other, in_column = outs[2:]
        return own.reshape(n_batch, slab_len, d_model)

    in_specs = (
        P(batch_axes, "model", None),
        P(batch_axes),
        P(None, "data"),
        P(None, "data", "model"),
        P(None, "data", None),
        P(None, "model", "data"),
    )
    return jax.shard_map(local_step, mesh=mesh, in_specs=in_specs, out_specs=P(batch_axes, "model", None), check_vma=False)
```
